256 devices in a mesh: rows: 32 (over x_lo, z, core), freq: 8 (over y, x_hi).
Axes of the slice: x: 4 (x_hi: 2, x_lo: 2; x = x_hi * 2 + x_lo), y: 4, z: 8, core: 2. Of those that a mesh axis runs over, the one named last changes fastest.
Arguments:
- design: float32 [256, 65536], P('rows'), may hold values from 0.05 to 0.95
- passive: int32 [256, 65536], P('rows'), may hold values 0 or 1
- state: bfloat16 [2, 8, 256, 65536], P(None, 'freq', 'rows'), may hold values from -36 to 36
- adjoint: bfloat16 [2, 8, 256, 65536], P(None, 'freq', 'rows'), may hold values from -36 to 36
- omega_sq: float32 [8], replicated, may hold values from 0.05 to 2
- assign: int32 [8], P('freq'), may hold values from 0 to 7, each once
Outputs:
- gradient: float32 [256, 65536], P('rows')
The draws below stay inside these ranges and needn't reach their ends.
Inputs may be any that keep to these rules, and one draw needn't show every extreme that they name: `assign`: each of 0 .. 7 appears once.
All inputs are finite; a program needn't handle non-finite values. No bound on the sum of `passive` on one device may be relied on, other than what follows from the above.
Results may differ from the reference program's by a relative error of at most 0.0003.
Values may be sent and summed in bfloat16 or wider, within the bound.
No kernel may reach another device: no remote copies, remote signals or barrier semaphores. Data moves between devices by JAX's collectives and lax.ppermute only.
A program may use at most 128 MiB of HBM per device.

```python
import math
import jax
import jax.numpy as jnp
from jax import lax

NC = 65536
RADIUS = 8
NR = 256
NF = 8


def field_draw(key, salt):
    base_key, col_key = jax.random.split(jax.random.fold_in(key, salt))
    rows = jnp.arange(NR, dtype=jnp.float32) / max(NR - 1, 1)
    col_scale = jnp.exp(math.log(3.0) * jax.random.uniform(col_key, (NC,), jnp.float32))
    values = jnp.clip(jax.random.normal(base_key, (2, NF, NR, NC), jnp.float32), -4.0, 4.0)
    row_scale = jnp.exp(math.log(3.0) * rows)
    return (values * row_scale[None, None, :, None] * col_scale).astype(jnp.bfloat16)


def draw_state(key, part):
    return field_draw(key, 11)


def draw_adjoint(key, part):
    return field_draw(key, 23)


def draw_design(key, part):
    wave_key, phase_key, noise_key = jax.random.split(jax.random.fold_in(key, 31), 3)
    waves = jax.random.uniform(wave_key, (2,), jnp.float32, 1.0, 4.0)
    phases = jax.random.uniform(phase_key, (2,), jnp.float32, 0.0, 2.0 * math.pi)
    rows = jnp.arange(NR, dtype=jnp.float32) / NR
    cols = jnp.arange(NC, dtype=jnp.float32) / NC
    amplitude = 0.3
    rough = 0.15
    smooth = jnp.sin(2.0 * math.pi * waves[0] * rows + phases[0])[:, None] * jnp.cos(2.0 * math.pi * waves[1] * cols + phases[1])[None, :]
    noise = jax.random.uniform(noise_key, (NR, NC), jnp.float32, -rough, rough)
    return 0.5 + amplitude * smooth + noise


def set_ends(values, own_key, smallest, largest):
    shape = values.shape
    place = [jax.random.randint(jax.random.fold_in(own_key, axis), (), 0, shape[axis]) for axis in range(len(shape))]
    values = values.at[tuple(place)].set(smallest)
    longest = shape.index(max(shape))
    place[longest] = (place[longest] + 1) % shape[longest]
    return values.at[tuple(place)].set(largest)


def setup_inputs(seed: int = 0) -> dict:
    keys = jax.random.split(jax.random.key(seed), 7)
    return {
        "design": draw_design(jax.random.fold_in(keys[6], 71), 0),
        "passive": set_ends((jax.random.randint(keys[1], (NR, NC), 0, 8) < 1).astype(jnp.int32), jax.random.fold_in(keys[1], 1), 0, 1),
        "state": draw_state(jax.random.fold_in(keys[6], 71), 0),
        "adjoint": draw_adjoint(jax.random.fold_in(keys[6], 71), 0),
        "omega_sq": jnp.clip(jnp.exp(jax.random.uniform(keys[4], (NF,), jnp.float32, math.log(0.05), math.log(2.0))), 0.05, 2.0),
        "assign": jax.random.permutation(keys[5], NF).astype(jnp.int32),
    }


sharpness = 8.0
threshold = 0.5
exponent = 3.0
soft_floor = 0.001
loss_factor = 0.2
epsilon = 1e-06
stiff_table = [[4.0 / 6, -1.0 / 6, -1.0 / 6, -2.0 / 6], [-1.0 / 6, 4.0 / 6, -2.0 / 6, -1.0 / 6], [-1.0 / 6, -2.0 / 6, 4.0 / 6, -1.0 / 6], [-2.0 / 6, -1.0 / 6, -1.0 / 6, 4.0 / 6]]
mass_table = [[4.0 / 36, 2.0 / 36, 2.0 / 36, 1.0 / 36], [2.0 / 36, 4.0 / 36, 1.0 / 36, 2.0 / 36], [2.0 / 36, 1.0 / 36, 4.0 / 36, 2.0 / 36], [1.0 / 36, 2.0 / 36, 2.0 / 36, 4.0 / 36]]

def tap_list():
    return [float(RADIUS + 1 - abs(offset)) for offset in range(-RADIUS, RADIUS + 1)]

def row_pass(padded, count):
    taps = tap_list()
    total = taps[0] * padded[0:count]
    for offset in range(1, 2 * RADIUS + 1):
        total = total + taps[offset] * padded[offset:offset + count]
    return total

def col_pass(field):
    taps = tap_list()
    count = field.shape[1]
    padded = jnp.pad(field, ((0, 0), (RADIUS, RADIUS)))
    total = taps[0] * padded[:, 0:count]
    for offset in range(1, 2 * RADIUS + 1):
        total = total + taps[offset] * padded[:, offset:offset + count]
    return total

def edge_sums(start, count, whole):
    positions = start + jnp.arange(count, dtype=jnp.int32)
    total = jnp.zeros((count,), jnp.float32)
    for offset in range(-RADIUS, RADIUS + 1):
        inside = ((positions + offset >= 0) & (positions + offset < whole)).astype(jnp.float32)
        total = total + float(RADIUS + 1 - abs(offset)) * inside
    return total

def project(tilde, passive):
    bottom = jnp.tanh(sharpness * threshold) + jnp.tanh(sharpness * (1.0 - threshold))
    steep = jnp.tanh(sharpness * (tilde - threshold))
    value = (jnp.tanh(sharpness * threshold) + steep) / bottom
    slope = sharpness * (1.0 - steep * steep) / bottom
    solid = passive > 0
    density = jnp.where(solid, 1.0, value)
    slope = jnp.where(solid, 0.0, slope)
    stiffness = exponent * density * density * (1.0 - soft_floor)
    return (stiffness, slope)

def bilinear(table, left, right):
    total = None
    for row_pos in range(4):
        inner = table[row_pos][0] * right[0]
        for col_pos in range(1, 4):
            inner = inner + table[row_pos][col_pos] * right[col_pos]
        term = left[row_pos] * inner
        total = term if total is None else total + term
    return total

def corners(nodes, below):
    stacked = jnp.concatenate([nodes, below], axis=0)
    right_col = jnp.zeros((stacked.shape[0], 1), stacked.dtype)
    shifted = jnp.concatenate([stacked[:, 1:], right_col], axis=1)
    return (stacked[:-1], shifted[:-1], stacked[1:], shifted[1:])

def element_terms(fields, fields_below, duals, duals_below, stiffness, omega):
    state_real = corners(fields[0], fields_below[0])
    state_imag = corners(fields[1], fields_below[1])
    adjoint_real = corners(duals[0], duals_below[0])
    adjoint_imag = corners(duals[1], duals_below[1])
    elastic = bilinear(stiff_table, adjoint_real, state_real) - bilinear(stiff_table, adjoint_imag, state_imag)
    damped = bilinear(stiff_table, adjoint_real, state_imag) + bilinear(stiff_table, adjoint_imag, state_real)
    inertia = bilinear(mass_table, adjoint_real, state_real) - bilinear(mass_table, adjoint_imag, state_imag)
    return stiffness * (elastic - loss_factor * damped) - omega * inertia

def reference(design, passive, state, adjoint, omega_sq, assign):
    weight_sum = edge_sums(0, NR, NR)[:, None] * edge_sums(0, NC, NC)[None, :]
    padded = jnp.pad(design, ((RADIUS, RADIUS), (0, 0)))
    tilde = col_pass(row_pass(padded, NR)) / weight_sum
    stiffness, slope = project(tilde, passive)
    factor = slope / weight_sum
    below = jnp.zeros((2, 1, NC), jnp.float32)

    def step(total, slot):
        fields = lax.dynamic_index_in_dim(state, slot, 1, keepdims=False).astype(jnp.float32)
        duals = lax.dynamic_index_in_dim(adjoint, slot, 1, keepdims=False).astype(jnp.float32)
        omega = omega_sq[assign[slot].astype(jnp.int32)]
        return (total + element_terms(fields, below, duals, below, stiffness, omega), None)
    summed, unused = lax.scan(step, jnp.zeros((NR, NC), jnp.float32), jnp.arange(NF, dtype=jnp.int32))
    spread = summed * factor
    back = col_pass(row_pass(jnp.pad(spread, ((RADIUS, RADIUS), (0, 0))), NR))
    total = jnp.sum(back * back)
    return back * lax.rsqrt(total / (NR * NC) + epsilon)
```

```python
import functools

import jax
import jax.numpy as jnp
from jax import lax
from jax.experimental import pallas as pl
from jax.experimental.pallas import tpu as pltpu
from jax.sharding import PartitionSpec as P

RADIUS = 8
LANES = 128
SHARPNESS = 8.0
THRESHOLD = 0.5
EXPONENT = 3.0
SOFT_FLOOR = 0.001
LOSS = 0.2
EPSILON = 1e-06
TANH_HALF = 0.999329299739067
DESIGN_STEPS = 32767.0
CODE_STEPS = 32700.0

f32 = jnp.float32
i16 = jnp.int16


def params(megabytes):
    return pltpu.CompilerParams(vmem_limit_bytes=megabytes * 1024 * 1024)


def vmem(count):
    return [pl.BlockSpec(memory_space=pltpu.VMEM)] * count


def cost(flops, moved):
    return pl.CostEstimate(flops=flops, bytes_accessed=moved, transcendentals=0)


def cols(index, width):
    return pl.ds(pl.multiple_of(index * width, width), width)


def row_ids(width):
    return lax.broadcasted_iota(jnp.int32, (8, width), 0)


def rows_up(block, count, ids):
    return jnp.where(ids < 8 - count, pltpu.roll(block, 8 - count, 0), 0.0)


def rows_down(block, count, ids):
    return jnp.where(ids >= count, pltpu.roll(block, count, 0), 0.0)


def row_filter(above, here, below):
    ids = row_ids(here.shape[1])
    upper = above - here
    lower = below - here
    for _ in range(2):
        for count in (1, 2, 4):
            upper = upper + rows_up(upper, count, ids)
            lower = lower + rows_down(lower, count, ids)
    total = here
    for count in (1, 2, 4):
        total = total + pltpu.roll(total, count, 0)
    return upper + lower + here + 10.0 * total


def cols_left(block, count):
    return pltpu.roll(block, block.shape[1] - count, 1)


def col_filter(block):
    for _ in range(2):
        first = block
        for count in (1, 2, 4):
            block = block + cols_left(block, count)
        block = block + cols_left(first, 8)
    return block


def moved_right(carry, block):
    joined = jnp.concatenate([carry, block], axis=1)
    return pltpu.roll(joined, RADIUS, 1)[:, LANES:]


def decode_scale(code):
    return jnp.exp2(code.astype(jnp.int32).astype(f32) * (1.0 / 256)) * (1.0 / CODE_STEPS)


def scale_code(largest):
    level = jnp.floor(jnp.log(jnp.maximum(largest, 1e-30)) * (256 * 1.4426950408889634)) + 1.0
    return level


def to_i16(values):
    return jnp.floor(values + 0.5).astype(jnp.int32).astype(i16)


def wide(tile, width):
    return jnp.concatenate([tile] * (width // LANES), axis=1)


def folded_max(block):
    parts = [block[:, i : i + LANES] for i in range(0, block.shape[1], LANES)]
    while len(parts) > 1:
        parts = [jnp.maximum(a, b) for a, b in zip(parts[::2], parts[1::2])]
    return parts[0]


def encode(source, target, count, width):
    largest = lax.fori_loop(
        0,
        count // width,
        lambda c, m: jnp.maximum(m, folded_max(jnp.abs(source[:, cols(c, width)]))),
        jnp.zeros((8, LANES), f32),
    )
    level = scale_code(largest)
    code = level.astype(jnp.int32).astype(i16)
    target[:, count : count + LANES] = code
    inverse = wide(1.0 / decode_scale(code), width)

    def step(c, none):
        target[:, cols(c, width)] = to_i16(source[:, cols(c, width)] * inverse)
        return none

    lax.fori_loop(0, count // width, step, 0)


def prepare_kernel(design, state, adjoint, edge, code, *, width):
    ids = row_ids(width)

    def step(c, none):
        at = cols(c, width)
        first = state[0, 0, :, at].astype(f32)
        rows = [state[1, 0, :, at], adjoint[0, 0, :, at], adjoint[1, 0, :, at]]
        for place, row in enumerate(rows):
            first = jnp.where(ids == place + 1, pltpu.roll(row.astype(f32), place + 1, 0), first)
        edge[:, at] = first[:4].astype(jnp.bfloat16)
        code[:, at] = to_i16(design[:, at] * DESIGN_STEPS)
        return none

    lax.fori_loop(0, design.shape[1] // width, step, 0)


def element_kernel(omega_sq, assign, state, adjoint, edge, elastic, inertia, *, width):
    omega = omega_sq[assign[0]]
    ids = row_ids(width)
    count = elastic.shape[1] // width
    whole = width + LANES

    def shifted(block, carry):
        return cols_left(jnp.concatenate([block, carry], axis=1), 1)[:, :width]

    def step(c, carries):
        at = cols(count - 1 - c, width)
        edges = edge[:, at].astype(f32)
        fields = [state[0, 0, :, at], state[1, 0, :, at], adjoint[0, 0, :, at], adjoint[1, 0, :, at]]
        kept = []
        parts = []
        for place, field in enumerate(fields):
            here = field.astype(f32)
            row = jnp.broadcast_to(edges[place : place + 1], here.shape)
            below = jnp.where(ids == 7, row, pltpu.roll(here, 7, 0))
            plus = here + below
            minus = here - below
            kept += [plus[:, :LANES], minus[:, :LANES]]
            plus_next = shifted(plus, carries[2 * place])
            minus_next = shifted(minus, carries[2 * place + 1])
            parts.append((plus + plus_next, plus - plus_next, minus + minus_next, minus - minus_next))
        sr, si, ar, ai = parts
        same = [ar[k] * sr[k] - ai[k] * si[k] for k in range(4)]
        cross = [ar[k] * si[k] + ai[k] * sr[k] for k in range(1, 4)]
        same_mixed = same[1] + same[2]
        cross_mixed = cross[0] + cross[1]
        stiff = 1.5 * (same_mixed - LOSS * cross_mixed) + (same[3] - LOSS * cross[2])
        mass = 2.25 * same[0] + 0.75 * same_mixed + 0.25 * same[3]
        elastic[:, at] = stiff * (EXPONENT * (1.0 - SOFT_FLOOR) / 6.0)
        inertia[:, at] = mass * (omega * (1.0 / 36.0))
        return tuple(kept)

    lax.fori_loop(0, count, step, tuple(jnp.zeros((8, LANES), f32) for _ in range(8)))


def partial_kernel(place, design, above, below, passive, elastic, inertia, inverse, *refs, width):
    outs, (rowed, spread, blocks) = refs[:-3], refs[-3:]
    count = design.shape[1] // width
    peers = len(outs)
    piece = design.shape[1] // peers
    zeros = jnp.zeros((8, LANES), f32)

    def filter_rows(c, carry):
        at = cols(c, width)
        upper = above[:, at].astype(jnp.int32).astype(f32) * (1.0 / DESIGN_STEPS)
        lower = below[:, at].astype(jnp.int32).astype(f32) * (1.0 / DESIGN_STEPS)
        block = row_filter(upper, design[:, at], lower)
        rowed[:, at] = moved_right(carry, block)
        return block[:, width - LANES :]

    last = lax.fori_loop(0, count, filter_rows, zeros)
    rowed[:, count * width :] = moved_right(last, zeros)

    def scale(c, carry):
        at = cols(c, width)
        window = rowed[:, pl.ds(pl.multiple_of(c * width, width), width + LANES)]
        weights = inverse[:, at]
        tilde = col_filter(window)[:, :width] * weights
        steep = jnp.tanh(SHARPNESS * (tilde - THRESHOLD))
        solid = passive[:, at] > 0
        density = jnp.where(solid, 1.0, (TANH_HALF + steep) * (0.5 / TANH_HALF))
        slope = jnp.where(solid, 0.0, (1.0 - steep * steep) * (SHARPNESS * 0.5 / TANH_HALF))
        block = (density * density * elastic[:, at] - inertia[:, at]) * (slope * weights)
        spread[:, at] = moved_right(carry, block)
        return block[:, width - LANES :]

    last = lax.fori_loop(0, count, scale, zeros)
    spread[:, count * width :] = moved_right(last, zeros)

    for shift in range(peers):
        start = lax.rem(place[0] + shift, peers) * piece

        def filter_cols(c, none):
            at = pl.ds(pl.multiple_of(start + c * width, width), width + LANES)
            blocks[:, cols(c, width)] = col_filter(spread[:, at])[:, :width]
            return none

        lax.fori_loop(0, piece // width, filter_cols, 0)
        encode(blocks, outs[shift], piece, width)


def sum_kernel(*refs, width):
    coded, out = refs[:-1], refs[-1]
    piece = out.shape[1]
    scales = [decode_scale(ref[:, piece:]) for ref in coded]

    def step(c, none):
        at = cols(c, width)
        total = None
        for ref, scale in zip(coded, scales):
            term = ref[:, at].astype(jnp.int32).astype(f32) * wide(scale, width)
            total = term if total is None else total + term
        out[:, at] = total
        return none

    lax.fori_loop(0, piece // width, step, 0)


def back_kernel(above, here, below, out, blocks, *, width):
    piece = here.shape[1]

    def step(c, none):
        at = cols(c, width)
        blocks[:, at] = row_filter(above[:, at], here[:, at], below[:, at])
        return none

    lax.fori_loop(0, piece // width, step, 0)
    encode(blocks, out, piece, width)


def decode_kernel(place, *refs, width):
    coded, out, squares = refs[:-2], refs[-2], refs[-1]
    peers = len(coded)
    piece = out.shape[1] // peers
    total = jnp.zeros((8, LANES), f32)
    for shift, ref in enumerate(coded):
        start = lax.rem(place[0] + peers - shift, peers) * piece
        scale = wide(decode_scale(ref[:, piece:]), width)

        def step(c, total):
            block = ref[:, cols(c, width)].astype(jnp.int32).astype(f32) * scale
            out[:, pl.ds(pl.multiple_of(start + c * width, width), width)] = block
            square = block * block
            parts = [square[:, i : i + LANES] for i in range(0, width, LANES)]
            while len(parts) > 1:
                parts = [a + b for a, b in zip(parts[::2], parts[1::2])]
            return total + parts[0]

        total = lax.fori_loop(0, piece // width, step, total)
    squares[...] = jnp.broadcast_to(total[None], squares.shape)


def scale_kernel(back, squares, out, *, width, elements):
    mean = jnp.sum(jnp.sum(squares[...], axis=0), keepdims=True) * (1.0 / elements) + EPSILON
    root = lax.rsqrt(mean)
    root = root * (1.5 - 0.5 * mean * root * root)

    def step(c, none):
        at = cols(c, width)
        out[:, at] = back[:, at] * root
        return none

    lax.fori_loop(0, out.shape[1] // width, step, 0)


def edge_weights(positions, whole):
    near = jnp.maximum(RADIUS - positions, 0)
    far = jnp.maximum(RADIUS - (whole - 1 - positions), 0)
    missing = near * (near + 1) // 2 + far * (far + 1) // 2
    return ((RADIUS + 1) ** 2 - missing).astype(f32)


def shards(design, passive, state, adjoint, omega_sq, assign):
    slab_rows, width = design.shape
    rows = lax.axis_size("rows")
    peers = lax.axis_size("freq")
    whole_rows = slab_rows * rows
    piece = width // peers
    up = [(i, i + 1) for i in range(rows - 1)]
    down = [(target, source) for source, target in up]
    place = lax.axis_index("freq").astype(jnp.int32).reshape(1)
    smem = pl.BlockSpec(memory_space=pltpu.SMEM)

    edge, code = pl.pallas_call(
        functools.partial(prepare_kernel, width=512),
        out_shape=[
            jax.ShapeDtypeStruct((4, width), jnp.bfloat16),
            jax.ShapeDtypeStruct((slab_rows, width), i16),
        ],
        in_specs=vmem(3),
        out_specs=vmem(2),
        compiler_params=params(16),
        name="prepare",
    )(design, state, adjoint)
    edge_below = lax.ppermute(edge, "rows", down)
    code_below = lax.ppermute(code, "rows", down)
    code_above = lax.ppermute(code, "rows", up)

    top = lax.axis_index("rows") * slab_rows
    inverse = 1.0 / (
        edge_weights(top + jnp.arange(slab_rows, dtype=jnp.int32), whole_rows)[:, None]
        * edge_weights(jnp.arange(width, dtype=jnp.int32), width)[None, :]
    )

    slab = jax.ShapeDtypeStruct((slab_rows, width), f32)
    elastic, inertia = pl.pallas_call(
        functools.partial(element_kernel, width=256),
        out_shape=[slab, slab],
        in_specs=[smem, smem] + vmem(3),
        out_specs=vmem(2),
        compiler_params=params(20),
        cost_estimate=cost(80 * slab_rows * width, 8 * 1024 * 1024),
        name="element",
    )(omega_sq, assign, state, adjoint, edge_below)

    coded_piece = jax.ShapeDtypeStruct((slab_rows, piece + LANES), i16)
    sent = pl.pallas_call(
        functools.partial(partial_kernel, width=1024),
        out_shape=[coded_piece] * peers,
        in_specs=[smem] + vmem(7),
        out_specs=vmem(peers),
        scratch_shapes=[
            pltpu.VMEM((slab_rows, width + LANES), f32),
            pltpu.VMEM((slab_rows, width + LANES), f32),
            pltpu.VMEM((slab_rows, piece), f32),
        ],
        compiler_params=params(32),
        cost_estimate=cost(150 * slab_rows * width, 14 * 1024 * 1024),
        name="partial",
    )(place, design, code_above, code_below, passive, elastic, inertia, inverse)

    received = [sent[0]]
    for shift in range(1, peers):
        route = [(i, (i + shift) % peers) for i in range(peers)]
        received.append(lax.ppermute(sent[shift], "freq", route))

    spread = pl.pallas_call(
        functools.partial(sum_kernel, width=1024),
        out_shape=jax.ShapeDtypeStruct((slab_rows, piece), f32),
        in_specs=vmem(peers),
        out_specs=vmem(1)[0],
        compiler_params=params(8),
        name="total",
    )(*received)
    spread_below = lax.ppermute(spread, "rows", down)
    spread_above = lax.ppermute(spread, "rows", up)

    result = pl.pallas_call(
        functools.partial(back_kernel, width=1024),
        out_shape=coded_piece,
        in_specs=vmem(3),
        out_specs=vmem(1)[0],
        scratch_shapes=[pltpu.VMEM((slab_rows, piece), f32)],
        compiler_params=params(8),
        name="back",
    )(spread_above, spread, spread_below)

    pieces = [result]
    for shift in range(1, peers):
        route = [(i, (i + shift) % peers) for i in range(peers)]
        pieces.append(lax.ppermute(result, "freq", route))

    back, squares = pl.pallas_call(
        functools.partial(decode_kernel, width=1024),
        out_shape=[slab, jax.ShapeDtypeStruct((rows, 8, LANES), f32)],
        in_specs=[smem] + vmem(peers),
        out_specs=vmem(2),
        compiler_params=params(16),
        name="decode",
    )(place, *pieces)
    squares = lax.all_to_all(squares, "rows", 0, 0, tiled=True)

    return pl.pallas_call(
        functools.partial(scale_kernel, width=1024, elements=float(whole_rows * width)),
        out_shape=slab,
        in_specs=vmem(2),
        out_specs=vmem(1)[0],
        compiler_params=params(16),
        name="scale",
    )(back, squares)


def solution(mesh):
    return jax.shard_map(
        shards,
        mesh=mesh,
        in_specs=(
            P("rows", None),
            P("rows", None),
            P(None, "freq", "rows", None),
            P(None, "freq", "rows", None),
            P(),
            P("freq"),
        ),
        out_specs=P("rows", None),
        check_vma=False,
    )
```

```python
import functools

import jax
import jax.numpy as jnp
from jax import lax
from jax.experimental import pallas as pl
from jax.experimental.pallas import tpu as pltpu
from jax.sharding import PartitionSpec as P


RADIUS = 8
LANES = 128
SHARPNESS = 8.0
THRESHOLD = 0.5
EXPONENT = 3.0
SOFT_FLOOR = 0.001
LOSS = 0.2
EPSILON = 1e-06
TANH_HALF = 0.999329299739067
DESIGN_STEPS = 32767.0
CODE_STEPS = 32700.0

f32 = jnp.float32
i16 = jnp.int16


def params(megabytes):
    return pltpu.CompilerParams(vmem_limit_bytes=megabytes * 1024 * 1024)


def vmem(count):
    return [pl.BlockSpec(memory_space=pltpu.VMEM)] * count


def cost(flops, moved):
    return pl.CostEstimate(flops=flops, bytes_accessed=moved, transcendentals=0)


def cols(index, width):
    return pl.ds(pl.multiple_of(index * width, width), width)


def row_ids(width):
    return lax.broadcasted_iota(jnp.int32, (8, width), 0)


def rows_up(block, count, ids):
    return jnp.where(ids < 8 - count, pltpu.roll(block, 8 - count, 0), 0.0)


def rows_down(block, count, ids):
    return jnp.where(ids >= count, pltpu.roll(block, count, 0), 0.0)


def row_filter(above, here, below):
    ids = row_ids(here.shape[1])
    upper = above - here
    lower = below - here
    for _ in range(2):
        for count in (1, 2, 4):
            upper = upper + rows_up(upper, count, ids)
            lower = lower + rows_down(lower, count, ids)
    total = here
    for count in (1, 2, 4):
        total = total + pltpu.roll(total, count, 0)
    return upper + lower + here + 10.0 * total


def moved(block, count):
    width = block.shape[1]
    return pltpu.roll(block, (width - count) % width, 1)


def col_filter(block):
    for step in (1, 3):
        near = moved(block, step) + moved(block, -step)
        far = moved(block, 2 * step) + moved(block, -2 * step)
        block = 3.0 * block + 2.0 * near + far
    return block


def padded_cols(index, width):
    return pl.ds(pl.multiple_of(index * width, LANES), width + 2 * LANES)


def inner_cols(index, width):
    return pl.ds(pl.multiple_of(index * width + LANES, LANES), width)


def clear_ends(ref):
    count = ref.shape[1]
    ref[:, :LANES] = jnp.zeros((8, LANES), f32)
    ref[:, count - LANES :] = jnp.zeros((8, LANES), f32)


def decode_scale(code):
    return jnp.exp2(code.astype(jnp.int32).astype(f32) * (1.0 / 256)) * (1.0 / CODE_STEPS)


def scale_code(largest):
    level = jnp.floor(jnp.log(jnp.maximum(largest, 1e-30)) * (256 * 1.4426950408889634)) + 1.0
    return level


def to_i16(values):
    return jnp.round(values).astype(jnp.int32).astype(i16)


def wide(tile, width):
    return jnp.concatenate([tile] * (width // LANES), axis=1)


def folded_max(block):
    parts = [block[:, i : i + LANES] for i in range(0, block.shape[1], LANES)]
    while len(parts) > 1:
        parts = [jnp.maximum(a, b) for a, b in zip(parts[::2], parts[1::2])]
    return parts[0]


def encode(source, largest, target, width):
    count = source.shape[1]
    code = scale_code(largest).astype(jnp.int32).astype(i16)
    target[:, count : count + LANES] = code
    inverse = wide(1.0 / decode_scale(code), width)

    def step(c, none):
        target[:, cols(c, width)] = to_i16(source[:, cols(c, width)] * inverse)
        return none

    lax.fori_loop(0, count // width, step, 0)


def edge_kernel(state, adjoint, edge, *, width):
    ids = row_ids(width)

    def step(c, none):
        at = cols(c, width)
        first = state[0, 0, :, at].astype(f32)
        rows = [state[1, 0, :, at], adjoint[0, 0, :, at], adjoint[1, 0, :, at]]
        for place, row in enumerate(rows):
            first = jnp.where(ids == place + 1, pltpu.roll(row.astype(f32), place + 1, 0), first)
        edge[:, at] = first[:4].astype(jnp.bfloat16)
        return none

    lax.fori_loop(0, edge.shape[1] // width, step, 0)


def element_kernel(omega_sq, assign, state, adjoint, edge, elastic, inertia, *, width):
    omega = omega_sq[assign[0]]
    ids = row_ids(width)
    count = elastic.shape[1] // width

    def shifted(block, carry):
        return moved(jnp.concatenate([block, carry], axis=1), 1)[:, :width]

    def step(c, carries):
        at = cols(count - 1 - c, width)
        edges = edge[:, at].astype(f32)
        edges_next = shifted(edges, carries[4])
        edges_plus = edges + edges_next
        edges_minus = edges - edges_next
        fields = [state[0, 0, :, at], state[1, 0, :, at], adjoint[0, 0, :, at], adjoint[1, 0, :, at]]
        kept = []
        parts = []
        for place, field in enumerate(fields):
            here = field.astype(f32)
            kept.append(here[:, :LANES])
            following = shifted(here, carries[place])
            plus = here + following
            minus = here - following

            def below(block, edge_rows):
                row = jnp.broadcast_to(edge_rows[place : place + 1], block.shape)
                return jnp.where(ids == 7, row, pltpu.roll(block, 7, 0))

            plus_below = below(plus, edges_plus)
            minus_below = below(minus, edges_minus)
            parts.append((plus + plus_below, minus + minus_below, plus - plus_below, minus - minus_below))
        kept.append(edges[:, :LANES])
        sr, si, ar, ai = parts
        same = [ar[k] * sr[k] - ai[k] * si[k] for k in range(4)]
        cross = [ar[k] * si[k] + ai[k] * sr[k] for k in range(1, 4)]
        same_mixed = same[1] + same[2]
        cross_mixed = cross[0] + cross[1]
        stiff = 1.5 * (same_mixed - LOSS * cross_mixed) + (same[3] - LOSS * cross[2])
        mass = 2.25 * same[0] + 0.75 * same_mixed + 0.25 * same[3]
        elastic[:, at] = stiff * (EXPONENT * (1.0 - SOFT_FLOOR) / 6.0)
        inertia[:, at] = mass * (omega * (1.0 / 36.0))
        return tuple(kept)

    zeros = jnp.zeros((8, LANES), f32)
    lax.fori_loop(0, count, step, (zeros, zeros, zeros, zeros, zeros[:4]))


def partial_kernel(place, design, above, below, passive, elastic, inertia, inverse, *refs):
    outs, (rowed, spread, blocks) = refs[:-3], refs[-3:]
    peers = len(outs)
    piece = design.shape[1] // peers
    narrow = 2048
    clear_ends(rowed)
    clear_ends(spread)

    def filter_rows(c, none):
        at = cols(c, narrow)
        upper = above[:, at].astype(jnp.int32).astype(f32) * (1.0 / DESIGN_STEPS)
        lower = below[:, at].astype(jnp.int32).astype(f32) * (1.0 / DESIGN_STEPS)
        rowed[:, inner_cols(c, narrow)] = row_filter(upper, design[:, at], lower)
        return none

    lax.fori_loop(0, design.shape[1] // narrow, filter_rows, 0)

    def scale(c, none):
        at = cols(c, piece)
        weights = inverse[:, at]
        tilde = col_filter(rowed[:, padded_cols(c, piece)])[:, LANES : LANES + piece] * weights
        steep = jnp.tanh(SHARPNESS * (tilde - THRESHOLD))
        solid = passive[:, at] > 0
        density = jnp.where(solid, 1.0, (TANH_HALF + steep) * (0.5 / TANH_HALF))
        slope = jnp.where(solid, 0.0, (1.0 - steep * steep) * (SHARPNESS * 0.5 / TANH_HALF))
        block = (density * density * elastic[:, at] - inertia[:, at]) * (slope * weights)
        spread[:, inner_cols(c, piece)] = block
        return none

    lax.fori_loop(0, peers, scale, 0)

    for shift in range(peers):
        source = lax.rem(place[0] + shift, peers)
        block = col_filter(spread[:, padded_cols(source, piece)])[:, LANES : LANES + piece]
        blocks[...] = block
        encode(blocks, folded_max(jnp.abs(block)), outs[shift], narrow)


def sum_kernel(*refs, width):
    coded, out = refs[:-1], refs[-1]
    piece = out.shape[1]
    scales = [decode_scale(ref[:, piece:]) for ref in coded]

    def step(c, none):
        at = cols(c, width)
        total = None
        for ref, scale in zip(coded, scales):
            term = ref[:, at].astype(jnp.int32).astype(f32) * wide(scale, width)
            total = term if total is None else total + term
        out[:, at] = total
        return none

    lax.fori_loop(0, piece // width, step, 0)


def back_kernel(above, here, below, out, blocks, *, width):
    piece = here.shape[1]

    def step(c, largest):
        at = cols(c, width)
        block = row_filter(above[:, at], here[:, at], below[:, at])
        blocks[:, at] = block
        return jnp.maximum(largest, folded_max(jnp.abs(block)))

    largest = lax.fori_loop(0, piece // width, step, jnp.zeros((8, LANES), f32))
    encode(blocks, largest, out, width)


def decode_kernel(place, *refs, width):
    coded, out, squares = refs[:-2], refs[-2], refs[-1]
    peers = len(coded)
    piece = out.shape[1] // peers
    total = jnp.zeros((8, LANES), f32)
    for shift, ref in enumerate(coded):
        start = lax.rem(place[0] + peers - shift, peers) * piece
        scale = wide(decode_scale(ref[:, piece:]), width)

        def step(c, total):
            block = ref[:, cols(c, width)].astype(jnp.int32).astype(f32) * scale
            out[:, pl.ds(pl.multiple_of(start + c * width, width), width)] = block
            square = block * block
            parts = [square[:, i : i + LANES] for i in range(0, width, LANES)]
            while len(parts) > 1:
                parts = [a + b for a, b in zip(parts[::2], parts[1::2])]
            return total + parts[0]

        total = lax.fori_loop(0, piece // width, step, total)
    squares[...] = jnp.broadcast_to(total[None], squares.shape)


def scale_kernel(back, squares, out, *, width, elements):
    mean = jnp.sum(jnp.sum(squares[...], axis=0), keepdims=True) * (1.0 / elements) + EPSILON
    root = lax.rsqrt(mean)
    root = root * (1.5 - 0.5 * mean * root * root)

    def step(c, none):
        at = cols(c, width)
        out[:, at] = back[:, at] * root
        return none

    lax.fori_loop(0, out.shape[1] // width, step, 0)


def edge_weights(positions, whole):
    near = jnp.maximum(RADIUS - positions, 0)
    far = jnp.maximum(RADIUS - (whole - 1 - positions), 0)
    missing = near * (near + 1) // 2 + far * (far + 1) // 2
    return ((RADIUS + 1) ** 2 - missing).astype(f32)


def layer(design, passive, state, adjoint, omega_sq, assign):
    slab_rows, width = design.shape
    rows = lax.axis_size("rows")
    peers = lax.axis_size("freq")
    whole_rows = slab_rows * rows
    piece = width // peers
    up = [(i, i + 1) for i in range(rows - 1)]
    down = [(target, source) for source, target in up]
    place = lax.axis_index("freq").astype(jnp.int32).reshape(1)
    smem = pl.BlockSpec(memory_space=pltpu.SMEM)

    edge_width = 8192
    field_block = pl.BlockSpec((2, 1, slab_rows, edge_width), lambda c: (0, 0, 0, c))
    edge = pl.pallas_call(
        functools.partial(edge_kernel, width=1024),
        grid=(width // edge_width,),
        out_shape=jax.ShapeDtypeStruct((4, width), jnp.bfloat16),
        in_specs=[field_block, field_block],
        out_specs=pl.BlockSpec((4, edge_width), lambda c: (0, c)),
        compiler_params=params(8),
        cost_estimate=cost(8 * slab_rows * width, 4 * 1024 * 1024),
        name="edge",
    )(state, adjoint)
    edge_below = lax.ppermute(edge, "rows", down)
    code = jnp.round(design * DESIGN_STEPS).astype(i16)
    code_below = lax.ppermute(code, "rows", down)
    code_above = lax.ppermute(code, "rows", up)

    top = lax.axis_index("rows") * slab_rows
    inverse = 1.0 / (
        edge_weights(top + jnp.arange(slab_rows, dtype=jnp.int32), whole_rows)[:, None]
        * edge_weights(jnp.arange(width, dtype=jnp.int32), width)[None, :]
    )

    slab = jax.ShapeDtypeStruct((slab_rows, width), f32)
    elastic, inertia = pl.pallas_call(
        functools.partial(element_kernel, width=2048),
        out_shape=[slab, slab],
        in_specs=[smem, smem] + vmem(3),
        out_specs=vmem(2),
        compiler_params=params(20),
        cost_estimate=cost(80 * slab_rows * width, 8 * 1024 * 1024),
        name="element",
    )(omega_sq, assign, state, adjoint, edge_below)

    coded_piece = jax.ShapeDtypeStruct((slab_rows, piece + LANES), i16)
    sent = pl.pallas_call(
        partial_kernel,
        out_shape=[coded_piece] * peers,
        in_specs=[smem] + vmem(7),
        out_specs=vmem(peers),
        scratch_shapes=[
            pltpu.VMEM((slab_rows, width + 2 * LANES), f32),
            pltpu.VMEM((slab_rows, width + 2 * LANES), f32),
            pltpu.VMEM((slab_rows, piece), f32),
        ],
        compiler_params=params(32),
        cost_estimate=cost(150 * slab_rows * width, 14 * 1024 * 1024),
        name="partial",
    )(place, design, code_above, code_below, passive, elastic, inertia, inverse)

    received = [sent[0]]
    for shift in range(1, peers):
        route = [(i, (i + shift) % peers) for i in range(peers)]
        received.append(lax.ppermute(sent[shift], "freq", route))

    spread = pl.pallas_call(
        functools.partial(sum_kernel, width=1024),
        out_shape=jax.ShapeDtypeStruct((slab_rows, piece), f32),
        in_specs=vmem(peers),
        out_specs=vmem(1)[0],
        compiler_params=params(8),
        name="total",
    )(*received)
    spread_below = lax.ppermute(spread, "rows", down)
    spread_above = lax.ppermute(spread, "rows", up)

    result = pl.pallas_call(
        functools.partial(back_kernel, width=1024),
        out_shape=coded_piece,
        in_specs=vmem(3),
        out_specs=vmem(1)[0],
        scratch_shapes=[pltpu.VMEM((slab_rows, piece), f32)],
        compiler_params=params(8),
        name="back",
    )(spread_above, spread, spread_below)

    pieces = [result]
    for shift in range(1, peers):
        route = [(i, (i + shift) % peers) for i in range(peers)]
        pieces.append(lax.ppermute(result, "freq", route))

    back, squares = pl.pallas_call(
        functools.partial(decode_kernel, width=1024),
        out_shape=[slab, jax.ShapeDtypeStruct((rows, 8, LANES), f32)],
        in_specs=[smem] + vmem(peers),
        out_specs=vmem(2),
        compiler_params=params(16),
        name="decode",
    )(place, *pieces)
    squares = lax.all_to_all(squares, "rows", 0, 0, tiled=True)

    return pl.pallas_call(
        functools.partial(scale_kernel, width=1024, elements=float(whole_rows * width)),
        out_shape=slab,
        in_specs=vmem(2),
        out_specs=vmem(1)[0],
        compiler_params=params(16),
        name="scale",
    )(back, squares)


def solution(mesh):
    return jax.shard_map(
        layer,
        mesh=mesh,
        in_specs=(
            P("rows", None),
            P("rows", None),
            P(None, "freq", "rows", None),
            P(None, "freq", "rows", None),
            P(),
            P("freq"),
        ),
        out_specs=P("rows", None),
        check_vma=False,
    )
```

```python
import functools

import jax
import jax.numpy as jnp
from jax import lax
from jax.experimental import pallas as pl
from jax.experimental.pallas import tpu as pltpu
from jax.sharding import PartitionSpec as P


RADIUS = 8
LANES = 128
SHARPNESS = 8.0
THRESHOLD = 0.5
EXPONENT = 3.0
SOFT_FLOOR = 0.001
LOSS = 0.2
EPSILON = 1e-06
TANH_HALF = 0.999329299739067
DESIGN_STEPS = 32767.0
CODE_STEPS = 32700.0

f32 = jnp.float32
i16 = jnp.int16


def params(megabytes):
    return pltpu.CompilerParams(vmem_limit_bytes=megabytes * 1024 * 1024)


def vmem(count):
    return [pl.BlockSpec(memory_space=pltpu.VMEM)] * count


def cost(flops, moved):
    return pl.CostEstimate(flops=flops, bytes_accessed=moved, transcendentals=0)


def cols(index, width):
    return pl.ds(pl.multiple_of(index * width, width), width)


def row_ids(width):
    return lax.broadcasted_iota(jnp.int32, (8, width), 0)


def rows_up(block, count, ids):
    return jnp.where(ids < 8 - count, pltpu.roll(block, 8 - count, 0), 0.0)


def rows_down(block, count, ids):
    return jnp.where(ids >= count, pltpu.roll(block, count, 0), 0.0)


def row_filter(above, here, below):
    ids = row_ids(here.shape[1])
    upper = above - here
    lower = below - here
    for _ in range(2):
        for count in (1, 2, 4):
            upper = upper + rows_up(upper, count, ids)
            lower = lower + rows_down(lower, count, ids)
    total = here
    for count in (1, 2, 4):
        total = total + pltpu.roll(total, count, 0)
    return upper + lower + here + 10.0 * total


def moved(block, count):
    width = block.shape[1]
    return pltpu.roll(block, (width - count) % width, 1)


def col_filter(block):
    for step in (1, 3):
        near = moved(block, step) + moved(block, -step)
        far = moved(block, 2 * step) + moved(block, -2 * step)
        block = 3.0 * block + 2.0 * near + far
    return block


def padded_cols(index, width):
    return pl.ds(pl.multiple_of(index * width, LANES), width + 2 * LANES)


def inner_cols(index, width):
    return pl.ds(pl.multiple_of(index * width + LANES, LANES), width)


def clear_ends(ref):
    count = ref.shape[1]
    ref[:, :LANES] = jnp.zeros((8, LANES), f32)
    ref[:, count - LANES :] = jnp.zeros((8, LANES), f32)


def decode_scale(code):
    return jnp.exp2(code.astype(jnp.int32).astype(f32) * (1.0 / 256)) * (1.0 / CODE_STEPS)


def scale_code(largest):
    level = jnp.floor(jnp.log(jnp.maximum(largest, 1e-30)) * (256 * 1.4426950408889634)) + 1.0
    return level


def to_i16(values):
    return jnp.round(values).astype(jnp.int32).astype(i16)


def wide(tile, width):
    return jnp.concatenate([tile] * (width // LANES), axis=1)


def folded_max(block):
    parts = [block[:, i : i + LANES] for i in range(0, block.shape[1], LANES)]
    while len(parts) > 1:
        parts = [jnp.maximum(a, b) for a, b in zip(parts[::2], parts[1::2])]
    return parts[0]


def encode(source, largest, targets, width):
    count = source.shape[1]
    code = scale_code(largest).astype(jnp.int32).astype(i16)
    for target in targets:
        target[:, count : count + LANES] = code
    inverse = wide(1.0 / decode_scale(code), width)

    def step(c, none):
        values = to_i16(source[:, cols(c, width)] * inverse)
        for target in targets:
            target[:, cols(c, width)] = values
        return none

    lax.fori_loop(0, count // width, step, 0)


def field_copies(sources, kept, arrived, stage, span):
    at = pl.ds(stage * span, span)
    whole = lambda ref: (slice(None),) * (len(ref.shape) - 1) + (at,)
    return [
        pltpu.make_async_copy(source.at[whole(source)], target.at[whole(target)], arrived.at[stage, place])
        for place, (source, target) in enumerate(zip(sources, kept))
    ]


def edge_kernel(state_far, adjoint_far, edge, state, adjoint, arrived, *, width, stages):
    ids = row_ids(width)
    span = edge.shape[1] // stages
    copies = functools.partial(
        field_copies, (state_far, adjoint_far), (state, adjoint), arrived, span=span
    )
    for stage in range(stages):
        for copy in copies(stage):
            copy.start()

    for stage in range(stages):
        for copy in copies(stage):
            copy.wait()

        def step(c, none):
            at = cols(stage * (span // width) + c, width)
            first = state[0, 0, :, at].astype(f32)
            rows = [state[1, 0, :, at], adjoint[0, 0, :, at], adjoint[1, 0, :, at]]
            for place, row in enumerate(rows):
                first = jnp.where(ids == place + 1, pltpu.roll(row.astype(f32), place + 1, 0), first)
            edge[:, at] = first[:4].astype(jnp.bfloat16)
            return none

        lax.fori_loop(0, span // width, step, 0)


def element_kernel(
    omega_sq,
    assign,
    state_far,
    adjoint_far,
    edge_far,
    elastic_far,
    inertia_far,
    state,
    adjoint,
    edge,
    elastic,
    inertia,
    arrived,
    left,
    *,
    width,
    stages,
):
    omega = omega_sq[assign[0]]
    ids = row_ids(width)
    span = elastic.shape[1] // stages
    count = span // width
    copies = functools.partial(
        field_copies, (state_far, adjoint_far, edge_far), (state, adjoint, edge), arrived, span=span
    )
    for stage in reversed(range(stages)):
        for copy in copies(stage):
            copy.start()

    def shifted(block, carry):
        return moved(jnp.concatenate([block, carry], axis=1), 1)[:, :width]

    def step(stage, c, carries):
        at = cols((stage + 1) * count - 1 - c, width)
        edges = edge[:, at].astype(f32)
        fields = [state[0, 0, :, at], state[1, 0, :, at], adjoint[0, 0, :, at], adjoint[1, 0, :, at]]
        kept = []
        parts = []
        for place, field in enumerate(fields):
            here = field.astype(f32)
            row = jnp.broadcast_to(edges[place : place + 1], here.shape)
            below = jnp.where(ids == 7, row, pltpu.roll(here, 7, 0))
            plus = here + below
            minus = here - below
            kept += [plus[:, :LANES], minus[:, :LANES]]
            plus_next = shifted(plus, carries[2 * place])
            minus_next = shifted(minus, carries[2 * place + 1])
            parts.append((plus + plus_next, plus - plus_next, minus + minus_next, minus - minus_next))
        sr, si, ar, ai = parts
        same = [ar[k] * sr[k] - ai[k] * si[k] for k in range(4)]
        cross = [ar[k] * si[k] + ai[k] * sr[k] for k in range(1, 4)]
        same_mixed = same[1] + same[2]
        cross_mixed = cross[0] + cross[1]
        stiff = 1.5 * (same_mixed - LOSS * cross_mixed) + (same[3] - LOSS * cross[2])
        mass = 2.25 * same[0] + 0.75 * same_mixed + 0.25 * same[3]
        elastic[:, at] = stiff * (EXPONENT * (1.0 - SOFT_FLOOR) / 6.0)
        inertia[:, at] = mass * (omega * (1.0 / 36.0))
        return tuple(kept)

    def results(stage):
        at = pl.ds(stage * span, span)
        return [
            pltpu.make_async_copy(source.at[:, at], target.at[:, at], left.at[stage, place])
            for place, (source, target) in enumerate(((elastic, elastic_far), (inertia, inertia_far)))
        ]

    carries = (jnp.zeros((8, LANES), f32),) * 8
    for stage in reversed(range(stages)):
        for copy in copies(stage):
            copy.wait()
        carries = lax.fori_loop(0, count, functools.partial(step, stage), carries)
        for copy in results(stage):
            copy.start()
    for stage in reversed(range(stages)):
        for copy in results(stage):
            copy.wait()


def partial_kernel(*refs, stages):
    sources, out_far, kept = refs[:7], refs[7], refs[8:15]
    rowed, spread, blocks, out, arrived, left = refs[15:]
    design, above, below, passive, elastic, inertia, inverse = kept
    peers = out.shape[0]
    piece = design.shape[1] // peers
    narrow = 2048
    span = design.shape[1] // stages

    def early(stage):
        at = pl.ds(stage * span, span)
        return [
            pltpu.make_async_copy(sources[k].at[:, at], kept[k].at[:, at], arrived.at[stage, k])
            for k in range(3)
        ]

    late = [pltpu.make_async_copy(sources[k], kept[k], arrived.at[0, k]) for k in range(3, 7)]
    for stage in range(stages):
        for copy in early(stage):
            copy.start()
    for copy in late:
        copy.start()
    clear_ends(rowed)
    clear_ends(spread)

    def filter_rows(c, none):
        at = cols(c, narrow)
        upper = above[:, at].astype(jnp.int32).astype(f32) * (1.0 / DESIGN_STEPS)
        lower = below[:, at].astype(jnp.int32).astype(f32) * (1.0 / DESIGN_STEPS)
        rowed[:, inner_cols(c, narrow)] = row_filter(upper, design[:, at], lower)
        return none

    for stage in range(stages):
        for copy in early(stage):
            copy.wait()
        first = stage * (span // narrow)
        lax.fori_loop(first, first + span // narrow, filter_rows, 0)
    for copy in late:
        copy.wait()

    def scale(c, none):
        at = cols(c, piece)
        weights = inverse[:, at]
        tilde = col_filter(rowed[:, padded_cols(c, piece)])[:, LANES : LANES + piece] * weights
        steep = jnp.tanh(SHARPNESS * (tilde - THRESHOLD))
        solid = passive[:, at] > 0
        density = jnp.where(solid, 1.0, (TANH_HALF + steep) * (0.5 / TANH_HALF))
        slope = jnp.where(solid, 0.0, (1.0 - steep * steep) * (SHARPNESS * 0.5 / TANH_HALF))
        block = (density * density * elastic[:, at] - inertia[:, at]) * (slope * weights)
        spread[:, inner_cols(c, piece)] = block
        return none

    lax.fori_loop(0, peers, scale, 0)

    def send(peer, none):
        block = col_filter(spread[:, padded_cols(peer, piece)])[:, LANES : LANES + piece]
        blocks[...] = block
        encode(blocks, folded_max(jnp.abs(block)), [out.at[peer]], narrow)
        pltpu.make_async_copy(out.at[peer], out_far.at[peer], left.at[peer]).start()
        return none

    lax.fori_loop(0, peers, send, 0)
    for peer in range(peers):
        pltpu.make_async_copy(out.at[peer], out_far.at[peer], left.at[peer]).wait()


def sum_kernel(coded, out, *, width):
    peers, piece = coded.shape[0], out.shape[1]
    scales = [wide(decode_scale(coded[peer, :, piece:]), width) for peer in range(peers)]

    def step(c, none):
        at = cols(c, width)
        total = None
        for peer in range(peers):
            term = coded[peer, :, at].astype(jnp.int32).astype(f32) * scales[peer]
            total = term if total is None else total + term
        out[:, at] = total
        return none

    lax.fori_loop(0, piece // width, step, 0)


def back_kernel(above, here, below, out, blocks, *, width):
    piece = here.shape[1]

    def step(c, largest):
        at = cols(c, width)
        block = row_filter(above[:, at], here[:, at], below[:, at])
        blocks[:, at] = block
        return jnp.maximum(largest, folded_max(jnp.abs(block)))

    largest = lax.fori_loop(0, piece // width, step, jnp.zeros((8, LANES), f32))
    encode(blocks, largest, [out.at[peer] for peer in range(out.shape[0])], width)


def decode_kernel(coded, out, squares, *, width):
    peers = coded.shape[0]
    piece = out.shape[1] // peers
    total = jnp.zeros((8, LANES), f32)
    for peer in range(peers):
        scale = wide(decode_scale(coded[peer, :, piece:]), width)

        def step(c, total):
            block = coded[peer, :, cols(c, width)].astype(jnp.int32).astype(f32) * scale
            out[:, cols(peer * (piece // width) + c, width)] = block
            square = block * block
            parts = [square[:, i : i + LANES] for i in range(0, width, LANES)]
            while len(parts) > 1:
                parts = [a + b for a, b in zip(parts[::2], parts[1::2])]
            return total + parts[0]

        total = lax.fori_loop(0, piece // width, step, total)
    squares[...] = jnp.broadcast_to(total[None], squares.shape)


def scale_kernel(back, squares, out, *, width, elements):
    mean = jnp.sum(jnp.sum(squares[...], axis=0), keepdims=True) * (1.0 / elements) + EPSILON
    root = lax.rsqrt(mean)
    root = root * (1.5 - 0.5 * mean * root * root)

    def step(c, none):
        at = cols(c, width)
        out[:, at] = back[:, at] * root
        return none

    lax.fori_loop(0, out.shape[1] // width, step, 0)


def edge_weights(positions, whole):
    near = jnp.maximum(RADIUS - positions, 0)
    far = jnp.maximum(RADIUS - (whole - 1 - positions), 0)
    missing = near * (near + 1) // 2 + far * (far + 1) // 2
    return ((RADIUS + 1) ** 2 - missing).astype(f32)


def layer(design, passive, state, adjoint, omega_sq, assign):
    slab_rows, width = design.shape
    rows = lax.axis_size("rows")
    peers = lax.axis_size("freq")
    whole_rows = slab_rows * rows
    piece = width // peers
    up = [(i, i + 1) for i in range(rows - 1)]
    down = [(target, source) for source, target in up]
    smem = pl.BlockSpec(memory_space=pltpu.SMEM)

    in_place = pl.BlockSpec(memory_space=pltpu.HBM)
    stages = 4
    field_scratch = [
        pltpu.VMEM(state.shape, state.dtype),
        pltpu.VMEM(adjoint.shape, adjoint.dtype),
        pltpu.SemaphoreType.DMA((stages, 2)),
    ]
    edge = pl.pallas_call(
        functools.partial(edge_kernel, width=2048, stages=stages),
        out_shape=jax.ShapeDtypeStruct((4, width), jnp.bfloat16),
        in_specs=[in_place, in_place],
        out_specs=vmem(1)[0],
        scratch_shapes=field_scratch,
        compiler_params=params(63),
        cost_estimate=cost(8 * slab_rows * width, 4 * 1024 * 1024),
        name="edge",
    )(state, adjoint)
    edge_below = lax.ppermute(edge, "rows", down)
    code = jnp.round(design * DESIGN_STEPS).astype(i16)
    code_below = lax.ppermute(code, "rows", down)
    code_above = lax.ppermute(code, "rows", up)

    top = lax.axis_index("rows") * slab_rows
    inverse = 1.0 / (
        edge_weights(top + jnp.arange(slab_rows, dtype=jnp.int32), whole_rows)[:, None]
        * edge_weights(jnp.arange(width, dtype=jnp.int32), width)[None, :]
    )

    slab = jax.ShapeDtypeStruct((slab_rows, width), f32)
    elastic, inertia = pl.pallas_call(
        functools.partial(element_kernel, width=2048, stages=stages),
        out_shape=[slab, slab],
        in_specs=[smem, smem] + [in_place] * 3,
        out_specs=[in_place, in_place],
        scratch_shapes=field_scratch[:2]
        + [pltpu.VMEM(edge.shape, edge.dtype)]
        + [pltpu.VMEM((slab_rows, width), f32)] * 2
        + [pltpu.SemaphoreType.DMA((stages, 3)), pltpu.SemaphoreType.DMA((stages, 2))],
        compiler_params=params(63),
        cost_estimate=cost(80 * slab_rows * width, 8 * 1024 * 1024),
        name="element",
    )(omega_sq, assign, state, adjoint, edge_below)

    coded = jax.ShapeDtypeStruct((peers, slab_rows, piece + LANES), i16)
    operands = (design, code_above, code_below, passive, elastic, inertia, inverse)
    sent = pl.pallas_call(
        functools.partial(partial_kernel, stages=stages),
        out_shape=coded,
        in_specs=[in_place] * len(operands),
        out_specs=in_place,
        scratch_shapes=[pltpu.VMEM(operand.shape, operand.dtype) for operand in operands]
        + [
            pltpu.VMEM((slab_rows, width + 2 * LANES), f32),
            pltpu.VMEM((slab_rows, width + 2 * LANES), f32),
            pltpu.VMEM((slab_rows, piece), f32),
            pltpu.VMEM(coded.shape, coded.dtype),
            pltpu.SemaphoreType.DMA((stages, len(operands))),
            pltpu.SemaphoreType.DMA((peers,)),
        ],
        compiler_params=params(63),
        cost_estimate=cost(150 * slab_rows * width, 14 * 1024 * 1024),
        name="partial",
    )(*operands)

    received = lax.all_to_all(sent, "freq", 0, 0, tiled=True)

    spread = pl.pallas_call(
        functools.partial(sum_kernel, width=1024),
        out_shape=jax.ShapeDtypeStruct((slab_rows, piece), f32),
        in_specs=vmem(1),
        out_specs=vmem(1)[0],
        compiler_params=params(8),
        name="total",
    )(received)
    spread_below = lax.ppermute(spread, "rows", down)
    spread_above = lax.ppermute(spread, "rows", up)

    result = pl.pallas_call(
        functools.partial(back_kernel, width=1024),
        out_shape=coded,
        in_specs=vmem(3),
        out_specs=vmem(1)[0],
        scratch_shapes=[pltpu.VMEM((slab_rows, piece), f32)],
        compiler_params=params(8),
        name="back",
    )(spread_above, spread, spread_below)

    pieces = lax.all_to_all(result, "freq", 0, 0, tiled=True)

    back, squares = pl.pallas_call(
        functools.partial(decode_kernel, width=1024),
        out_shape=[slab, jax.ShapeDtypeStruct((rows, 8, LANES), f32)],
        in_specs=vmem(1),
        out_specs=vmem(2),
        compiler_params=params(16),
        name="decode",
    )(pieces)
    squares = lax.all_to_all(squares, "rows", 0, 0, tiled=True)

    out_width = 16384
    out_block = pl.BlockSpec((slab_rows, out_width), lambda c: (0, c))
    return pl.pallas_call(
        functools.partial(scale_kernel, width=2048, elements=float(whole_rows * width)),
        grid=(width // out_width,),
        out_shape=slab,
        in_specs=[out_block, pl.BlockSpec((rows, 8, LANES), lambda c: (0, 0, 0))],
        out_specs=out_block,
        compiler_params=params(16),
        name="scale",
    )(back, squares)


def solution(mesh):
    return jax.shard_map(
        layer,
        mesh=mesh,
        in_specs=(
            P("rows", None),
            P("rows", None),
            P(None, "freq", "rows", None),
            P(None, "freq", "rows", None),
            P(),
            P("freq"),
        ),
        out_specs=P("rows", None),
        check_vma=False,
    )
```

```python
import functools

import jax
import jax.numpy as jnp
from jax import lax
from jax.experimental import pallas as pl
from jax.experimental.pallas import tpu as pltpu
from jax.sharding import PartitionSpec as P


RADIUS = 8
LANES = 128
SHARPNESS = 8.0
THRESHOLD = 0.5
EXPONENT = 3.0
SOFT_FLOOR = 0.001
LOSS = 0.2
EPSILON = 1e-06
TANH_HALF = 0.999329299739067
DESIGN_STEPS = 32767.0
CODE_STEPS = 32700.0

f32 = jnp.float32
i16 = jnp.int16


def params(megabytes):
    return pltpu.CompilerParams(vmem_limit_bytes=megabytes * 1024 * 1024)


def vmem(count):
    return [pl.BlockSpec(memory_space=pltpu.VMEM)] * count


def cost(flops, moved):
    return pl.CostEstimate(flops=flops, bytes_accessed=moved, transcendentals=0)


def cols(index, width):
    return pl.ds(pl.multiple_of(index * width, width), width)


def row_ids(width):
    return lax.broadcasted_iota(jnp.int32, (8, width), 0)


def rows_up(block, count, ids):
    return jnp.where(ids < 8 - count, pltpu.roll(block, 8 - count, 0), 0.0)


def rows_down(block, count, ids):
    return jnp.where(ids >= count, pltpu.roll(block, count, 0), 0.0)


def row_filter(above, here, below):
    ids = row_ids(here.shape[1])
    upper = above - here
    lower = below - here
    for _ in range(2):
        for count in (1, 2, 4):
            upper = upper + rows_up(upper, count, ids)
            lower = lower + rows_down(lower, count, ids)
    total = here
    for count in (1, 2, 4):
        total = total + pltpu.roll(total, count, 0)
    return upper + lower + here + 10.0 * total


def moved(block, count):
    width = block.shape[1]
    return pltpu.roll(block, (width - count) % width, 1)


def col_filter(block):
    for step in (1, 3):
        near = moved(block, step) + moved(block, -step)
        far = moved(block, 2 * step) + moved(block, -2 * step)
        block = 3.0 * block + 2.0 * near + far
    return block


def padded_cols(index, width):
    return pl.ds(pl.multiple_of(index * width, LANES), width + 2 * LANES)


def inner_cols(index, width):
    return pl.ds(pl.multiple_of(index * width + LANES, LANES), width)


def clear_ends(ref):
    count = ref.shape[1]
    ref[:, :LANES] = jnp.zeros((8, LANES), f32)
    ref[:, count - LANES :] = jnp.zeros((8, LANES), f32)


def decode_scale(code):
    return jnp.exp2(code.astype(jnp.int32).astype(f32) * (1.0 / 256)) * (1.0 / CODE_STEPS)


def scale_code(largest):
    level = jnp.floor(jnp.log(jnp.maximum(largest, 1e-30)) * (256 * 1.4426950408889634)) + 1.0
    return level


def to_i16(values):
    return jnp.round(values).astype(jnp.int32).astype(i16)


def wide(tile, width):
    return jnp.concatenate([tile] * (width // LANES), axis=1)


def folded(block, join):
    parts = [block[:, i : i + LANES] for i in range(0, block.shape[1], LANES)]
    while len(parts) > 1:
        parts = [join(a, b) for a, b in zip(parts[::2], parts[1::2])]
    return parts[0]


def folded_max(block):
    return folded(jnp.abs(block), jnp.maximum)


def encode(source, largest, targets, width):
    count = source.shape[1]
    code = scale_code(largest).astype(jnp.int32).astype(i16)
    for target in targets:
        target[:, count : count + LANES] = code
    inverse = wide(1.0 / decode_scale(code), width)

    def step(c, none):
        values = to_i16(source[:, cols(c, width)] * inverse)
        for target in targets:
            target[:, cols(c, width)] = values
        return none

    lax.fori_loop(0, count // width, step, 0)


def field_copies(sources, kept, arrived, stage, span):
    at = pl.ds(stage * span, span)
    whole = lambda ref: (slice(None),) * (len(ref.shape) - 1) + (at,)
    return [
        pltpu.make_async_copy(source.at[whole(source)], target.at[whole(target)], arrived.at[stage, place])
        for place, (source, target) in enumerate(zip(sources, kept))
    ]


def edge_kernel(state_far, adjoint_far, edge, state, adjoint, arrived, *, width, stages):
    ids = row_ids(width)
    span = edge.shape[1] // stages
    copies = functools.partial(
        field_copies, (state_far, adjoint_far), (state, adjoint), arrived, span=span
    )
    for stage in range(stages):
        for copy in copies(stage):
            copy.start()

    for stage in range(stages):
        for copy in copies(stage):
            copy.wait()

        def step(c, none):
            at = cols(stage * (span // width) + c, width)
            first = state[0, 0, :, at].astype(f32)
            rows = [state[1, 0, :, at], adjoint[0, 0, :, at], adjoint[1, 0, :, at]]
            for place, row in enumerate(rows):
                first = jnp.where(ids == place + 1, pltpu.roll(row.astype(f32), place + 1, 0), first)
            edge[:, at] = first[:4].astype(jnp.bfloat16)
            return none

        lax.fori_loop(0, span // width, step, 0)


def code_kernel(design_far, code_far, design, code, arrived, left, *, width, stages):
    span = design.shape[1] // stages

    def load(stage):
        at = pl.ds(stage * span, span)
        return pltpu.make_async_copy(design_far.at[:, at], design.at[:, at], arrived.at[stage])

    def save(stage):
        at = pl.ds(stage * span, span)
        return pltpu.make_async_copy(code.at[:, at], code_far.at[:, at], left.at[stage])

    for stage in range(stages):
        load(stage).start()
    for stage in range(stages):
        load(stage).wait()

        def step(c, none):
            at = cols(stage * (span // width) + c, width)
            code[:, at] = to_i16(design[:, at] * DESIGN_STEPS)
            return none

        lax.fori_loop(0, span // width, step, 0)
        save(stage).start()
    for stage in range(stages):
        save(stage).wait()


def element_kernel(
    omega_sq,
    assign,
    state_far,
    adjoint_far,
    edge_far,
    elastic_far,
    inertia_far,
    state,
    adjoint,
    edge,
    elastic,
    inertia,
    arrived,
    left,
    *,
    width,
    stages,
):
    omega = omega_sq[assign[0]]
    ids = row_ids(width)
    span = elastic.shape[1] // stages
    count = span // width
    copies = functools.partial(
        field_copies, (state_far, adjoint_far, edge_far), (state, adjoint, edge), arrived, span=span
    )
    for stage in reversed(range(stages)):
        for copy in copies(stage):
            copy.start()

    def shifted(block, carry):
        return moved(jnp.concatenate([block, carry], axis=1), 1)[:, :width]

    def step(stage, c, carries):
        at = cols((stage + 1) * count - 1 - c, width)
        edges = edge[:, at].astype(f32)
        fields = [state[0, 0, :, at], state[1, 0, :, at], adjoint[0, 0, :, at], adjoint[1, 0, :, at]]
        kept = []
        parts = []
        for place, field in enumerate(fields):
            here = field.astype(f32)
            row = jnp.broadcast_to(edges[place : place + 1], here.shape)
            below = jnp.where(ids == 7, row, pltpu.roll(here, 7, 0))
            plus = here + below
            minus = here - below
            kept += [plus[:, :LANES], minus[:, :LANES]]
            plus_next = shifted(plus, carries[2 * place])
            minus_next = shifted(minus, carries[2 * place + 1])
            parts.append((plus + plus_next, plus - plus_next, minus + minus_next, minus - minus_next))
        sr, si, ar, ai = parts
        same = [ar[k] * sr[k] - ai[k] * si[k] for k in range(4)]
        cross = [ar[k] * si[k] + ai[k] * sr[k] for k in range(1, 4)]
        same_mixed = same[1] + same[2]
        cross_mixed = cross[0] + cross[1]
        stiff = 1.5 * (same_mixed - LOSS * cross_mixed) + (same[3] - LOSS * cross[2])
        mass = 2.25 * same[0] + 0.75 * same_mixed + 0.25 * same[3]
        elastic[:, at] = stiff * (EXPONENT * (1.0 - SOFT_FLOOR) / 6.0)
        inertia[:, at] = mass * (omega * (1.0 / 36.0))
        return tuple(kept)

    def results(stage):
        at = pl.ds(stage * span, span)
        return [
            pltpu.make_async_copy(source.at[:, at], target.at[:, at], left.at[stage, place])
            for place, (source, target) in enumerate(((elastic, elastic_far), (inertia, inertia_far)))
        ]

    carries = (jnp.zeros((8, LANES), f32),) * 8
    for stage in reversed(range(stages)):
        for copy in copies(stage):
            copy.wait()
        carries = lax.fori_loop(0, count, functools.partial(step, stage), carries, unroll=2)
        for copy in results(stage):
            copy.start()
    for stage in reversed(range(stages)):
        for copy in results(stage):
            copy.wait()


def tap_sums(before, after):
    near = jnp.maximum(RADIUS - before, 0)
    far = jnp.maximum(RADIUS - after, 0)
    missing = near * (near + 1) + far * (far + 1)
    return float((RADIUS + 1) ** 2) - 0.5 * missing.astype(f32)


def partial_kernel(top, *refs, stages, whole_rows):
    sources, out_far, kept = refs[:6], refs[6], refs[7:13]
    rowed, spread, blocks, out, arrived, left = refs[13:]
    design, above, below, passive, elastic, inertia = kept
    peers = out.shape[0]
    piece = design.shape[1] // peers
    narrow = 2048
    span = design.shape[1] // stages

    def early(stage):
        at = pl.ds(stage * span, span)
        return [
            pltpu.make_async_copy(sources[k].at[:, at], kept[k].at[:, at], arrived.at[stage, k])
            for k in range(3)
        ]

    late = [pltpu.make_async_copy(sources[k], kept[k], arrived.at[0, k]) for k in range(3, 6)]
    for stage in range(stages):
        for copy in early(stage):
            copy.start()
    for copy in late:
        copy.start()
    clear_ends(rowed)
    clear_ends(spread)

    def filter_rows(c, none):
        at = cols(c, narrow)
        upper = above[:, at].astype(jnp.int32).astype(f32) * (1.0 / DESIGN_STEPS)
        lower = below[:, at].astype(jnp.int32).astype(f32) * (1.0 / DESIGN_STEPS)
        rowed[:, inner_cols(c, narrow)] = row_filter(upper, design[:, at], lower)
        return none

    for stage in range(stages):
        for copy in early(stage):
            copy.wait()
        first = stage * (span // narrow)
        lax.fori_loop(first, first + span // narrow, filter_rows, 0)
    for copy in late:
        copy.wait()

    row = top[0] + row_ids(LANES)
    lane = lax.broadcasted_iota(jnp.int32, (8, LANES), 1)
    full = float((RADIUS + 1) ** 2)
    inside = 1.0 / (full * tap_sums(row, whole_rows - 1 - row))
    left_end = full / tap_sums(lane, RADIUS)
    right_end = full / tap_sums(RADIUS, LANES - 1 - lane)

    def scale(c, none):
        at = cols(c, piece)
        first = inside * jnp.where(c == 0, left_end, 1.0)
        last = inside * jnp.where(c == peers - 1, right_end, 1.0)
        weights = jnp.concatenate([first] + [inside] * (piece // LANES - 2) + [last], axis=1)
        tilde = col_filter(rowed[:, padded_cols(c, piece)])[:, LANES : LANES + piece] * weights
        steep = jnp.tanh(SHARPNESS * (tilde - THRESHOLD))
        solid = passive[:, at] > 0
        density = jnp.where(solid, 1.0, (TANH_HALF + steep) * (0.5 / TANH_HALF))
        slope = jnp.where(solid, 0.0, (1.0 - steep * steep) * (SHARPNESS * 0.5 / TANH_HALF))
        block = (density * density * elastic[:, at] - inertia[:, at]) * (slope * weights)
        spread[:, inner_cols(c, piece)] = block
        return none

    lax.fori_loop(0, peers, scale, 0)

    def send(peer, none):
        block = col_filter(spread[:, padded_cols(peer, piece)])[:, LANES : LANES + piece]
        blocks[...] = block
        encode(blocks, folded_max(block), [out.at[peer]], narrow)
        pltpu.make_async_copy(out.at[peer], out_far.at[peer], left.at[peer]).start()
        return none

    lax.fori_loop(0, peers, send, 0)
    for peer in range(peers):
        pltpu.make_async_copy(out.at[peer], out_far.at[peer], left.at[peer]).wait()


def sum_kernel(coded, out, *, width):
    peers, piece = coded.shape[0], out.shape[1]
    scales = [wide(decode_scale(coded[peer, :, piece:]), width) for peer in range(peers)]

    def step(c, none):
        at = cols(c, width)
        total = None
        for peer in range(peers):
            term = coded[peer, :, at].astype(jnp.int32).astype(f32) * scales[peer]
            total = term if total is None else total + term
        out[:, at] = total
        return none

    lax.fori_loop(0, piece // width, step, 0)


def back_kernel(above, here, below, out, blocks, *, width):
    piece = here.shape[1]
    zeros = jnp.zeros((8, LANES), f32)

    def step(c, carry):
        largest, squares = carry
        at = cols(c, width)
        block = row_filter(above[:, at], here[:, at], below[:, at])
        blocks[:, at] = block
        return jnp.maximum(largest, folded_max(block)), squares + folded(block * block, jnp.add)

    largest, squares = lax.fori_loop(0, piece // width, step, (zeros, zeros))
    encode(blocks, largest, [out.at[peer] for peer in range(out.shape[0])], width)
    code = scale_code(squares).astype(jnp.int32).astype(i16)
    values = to_i16(squares / decode_scale(code))
    for peer in range(out.shape[0]):
        out[peer, :, piece + LANES : piece + 2 * LANES] = code
        out[peer, :, piece + 2 * LANES :] = values


def squares_kernel(coded, squares):
    piece = coded.shape[2] - 3 * LANES
    total = jnp.zeros((8, LANES), f32)
    for peer in range(coded.shape[0]):
        values = coded[peer, :, piece + 2 * LANES :].astype(jnp.int32).astype(f32)
        total = total + values * decode_scale(coded[peer, :, piece + LANES : piece + 2 * LANES])
    squares[...] = jnp.broadcast_to(total[None], squares.shape)


def result_kernel(coded, squares, out_far, out, left, *, width, elements):
    peers = coded.shape[0]
    piece = out.shape[1] // peers
    mean = jnp.sum(jnp.sum(squares[...], axis=0), keepdims=True) * (1.0 / elements) + EPSILON
    root = lax.rsqrt(mean)
    root = root * (1.5 - 0.5 * mean * root * root)

    def finished(peer):
        at = pl.ds(peer * piece, piece)
        return pltpu.make_async_copy(out.at[:, at], out_far.at[:, at], left.at[peer])

    for peer in range(peers):
        scale = wide(decode_scale(coded[peer, :, piece : piece + LANES]) * root, width)

        def step(c, none):
            block = coded[peer, :, cols(c, width)].astype(jnp.int32).astype(f32) * scale
            out[:, cols(peer * (piece // width) + c, width)] = block
            return none

        lax.fori_loop(0, piece // width, step, 0)
        finished(peer).start()
    for peer in range(peers):
        finished(peer).wait()


def layer(design, passive, state, adjoint, omega_sq, assign):
    slab_rows, width = design.shape
    rows = lax.axis_size("rows")
    peers = lax.axis_size("freq")
    whole_rows = slab_rows * rows
    piece = width // peers
    up = [(i, i + 1) for i in range(rows - 1)]
    down = [(target, source) for source, target in up]
    smem = pl.BlockSpec(memory_space=pltpu.SMEM)

    in_place = pl.BlockSpec(memory_space=pltpu.HBM)
    stages = 4
    field_scratch = [
        pltpu.VMEM(state.shape, state.dtype),
        pltpu.VMEM(adjoint.shape, adjoint.dtype),
        pltpu.SemaphoreType.DMA((stages, 2)),
    ]
    edge = pl.pallas_call(
        functools.partial(edge_kernel, width=2048, stages=stages),
        out_shape=jax.ShapeDtypeStruct((4, width), jnp.bfloat16),
        in_specs=[in_place, in_place],
        out_specs=vmem(1)[0],
        scratch_shapes=field_scratch,
        compiler_params=params(63),
        cost_estimate=cost(8 * slab_rows * width, 4 * 1024 * 1024),
        name="edge",
    )(state, adjoint)
    edge_below = lax.ppermute(edge, "rows", down)
    code = pl.pallas_call(
        functools.partial(code_kernel, width=2048, stages=stages),
        out_shape=jax.ShapeDtypeStruct((slab_rows, width), i16),
        in_specs=[in_place],
        out_specs=in_place,
        scratch_shapes=[
            pltpu.VMEM((slab_rows, width), f32),
            pltpu.VMEM((slab_rows, width), i16),
            pltpu.SemaphoreType.DMA((stages,)),
            pltpu.SemaphoreType.DMA((stages,)),
        ],
        compiler_params=params(63),
        name="code",
    )(design)
    code_below = lax.ppermute(code, "rows", down)
    code_above = lax.ppermute(code, "rows", up)

    top = (lax.axis_index("rows") * slab_rows).astype(jnp.int32).reshape(1)

    slab = jax.ShapeDtypeStruct((slab_rows, width), f32)
    elastic, inertia = pl.pallas_call(
        functools.partial(element_kernel, width=2048, stages=stages),
        out_shape=[slab, slab],
        in_specs=[smem, smem] + [in_place] * 3,
        out_specs=[in_place, in_place],
        scratch_shapes=field_scratch[:2]
        + [pltpu.VMEM(edge.shape, edge.dtype)]
        + [pltpu.VMEM((slab_rows, width), f32)] * 2
        + [pltpu.SemaphoreType.DMA((stages, 3)), pltpu.SemaphoreType.DMA((stages, 2))],
        compiler_params=params(63),
        cost_estimate=cost(80 * slab_rows * width, 8 * 1024 * 1024),
        name="element",
    )(omega_sq, assign, state, adjoint, edge_below)

    coded = jax.ShapeDtypeStruct((peers, slab_rows, piece + LANES), i16)
    operands = (design, code_above, code_below, passive, elastic, inertia)
    sent = pl.pallas_call(
        functools.partial(partial_kernel, stages=stages, whole_rows=whole_rows),
        out_shape=coded,
        in_specs=[smem] + [in_place] * len(operands),
        out_specs=in_place,
        scratch_shapes=[pltpu.VMEM(operand.shape, operand.dtype) for operand in operands]
        + [
            pltpu.VMEM((slab_rows, width + 2 * LANES), f32),
            pltpu.VMEM((slab_rows, width + 2 * LANES), f32),
            pltpu.VMEM((slab_rows, piece), f32),
            pltpu.VMEM(coded.shape, coded.dtype),
            pltpu.SemaphoreType.DMA((stages, len(operands))),
            pltpu.SemaphoreType.DMA((peers,)),
        ],
        compiler_params=params(63),
        cost_estimate=cost(150 * slab_rows * width, 14 * 1024 * 1024),
        name="partial",
    )(top, *operands)

    received = lax.all_to_all(sent, "freq", 0, 0, tiled=True)

    spread = pl.pallas_call(
        functools.partial(sum_kernel, width=1024),
        out_shape=jax.ShapeDtypeStruct((slab_rows, piece), f32),
        in_specs=vmem(1),
        out_specs=vmem(1)[0],
        compiler_params=params(8),
        name="total",
    )(received)
    spread_below = lax.ppermute(spread, "rows", down)
    spread_above = lax.ppermute(spread, "rows", up)

    wide_coded = jax.ShapeDtypeStruct((peers, slab_rows, piece + 3 * LANES), i16)
    result = pl.pallas_call(
        functools.partial(back_kernel, width=1024),
        out_shape=wide_coded,
        in_specs=vmem(3),
        out_specs=vmem(1)[0],
        scratch_shapes=[pltpu.VMEM((slab_rows, piece), f32)],
        compiler_params=params(8),
        name="back",
    )(spread_above, spread, spread_below)

    pieces = lax.all_to_all(result, "freq", 0, 0, tiled=True)

    squares = pl.pallas_call(
        squares_kernel,
        out_shape=jax.ShapeDtypeStruct((rows, 8, LANES), f32),
        in_specs=vmem(1),
        out_specs=vmem(1)[0],
        compiler_params=params(8),
        name="squares",
    )(pieces)
    squares = lax.all_to_all(squares, "rows", 0, 0, tiled=True)

    return pl.pallas_call(
        functools.partial(result_kernel, width=2048, elements=float(whole_rows * width)),
        out_shape=slab,
        in_specs=vmem(2),
        out_specs=in_place,
        scratch_shapes=[pltpu.VMEM((slab_rows, width), f32), pltpu.SemaphoreType.DMA((peers,))],
        compiler_params=params(16),
        name="result",
    )(pieces, squares)


def solution(mesh):
    return jax.shard_map(
        layer,
        mesh=mesh,
        in_specs=(
            P("rows", None),
            P("rows", None),
            P(None, "freq", "rows", None),
            P(None, "freq", "rows", None),
            P(),
            P("freq"),
        ),
        out_specs=P("rows", None),
        check_vma=False,
    )
```

```python
import functools

import jax
import jax.numpy as jnp
from jax import lax
from jax.experimental import pallas as pl
from jax.experimental.pallas import tpu as pltpu
from jax.sharding import PartitionSpec as P


RADIUS = 8
LANES = 128
SHARPNESS = 8.0
THRESHOLD = 0.5
EXPONENT = 3.0
SOFT_FLOOR = 0.001
LOSS = 0.2
EPSILON = 1e-06
TANH_HALF = 0.999329299739067
DESIGN_STEPS = 32767.0
CODE_STEPS = 32700.0
SUM_STAGES = ((8, 16), (32, 64), (128, 1), (2, 4))

f32 = jnp.float32
i16 = jnp.int16


def params(megabytes):
    return pltpu.CompilerParams(vmem_limit_bytes=megabytes * 1024 * 1024)


def vmem(count):
    return [pl.BlockSpec(memory_space=pltpu.VMEM)] * count


def cost(flops, moved):
    return pl.CostEstimate(flops=flops, bytes_accessed=moved, transcendentals=0)


def cols(index, width):
    return pl.ds(pl.multiple_of(index * width, width), width)


def row_ids(width):
    return lax.broadcasted_iota(jnp.int32, (8, width), 0)


def rows_up(block, count, ids):
    return jnp.where(ids < 8 - count, pltpu.roll(block, 8 - count, 0), 0.0)


def rows_down(block, count, ids):
    return jnp.where(ids >= count, pltpu.roll(block, count, 0), 0.0)


def row_filter(above, here, below):
    ids = row_ids(here.shape[1])
    upper = above - here
    lower = below - here
    for _ in range(2):
        for count in (1, 2, 4):
            upper = upper + rows_up(upper, count, ids)
            lower = lower + rows_down(lower, count, ids)
    total = here
    for count in (1, 2, 4):
        total = total + pltpu.roll(total, count, 0)
    return upper + lower + here + 10.0 * total


def moved(block, count):
    width = block.shape[1]
    return pltpu.roll(block, (width - count) % width, 1)


def col_filter(block):
    for step in (1, 3):
        near = moved(block, step) + moved(block, -step)
        far = moved(block, 2 * step) + moved(block, -2 * step)
        block = 3.0 * block + 2.0 * near + far
    return block


def padded_cols(index, width):
    return pl.ds(pl.multiple_of(index * width, LANES), width + 2 * LANES)


def inner_cols(index, width):
    return pl.ds(pl.multiple_of(index * width + LANES, LANES), width)


def clear_ends(ref):
    count = ref.shape[1]
    ref[:, :LANES] = jnp.zeros((8, LANES), f32)
    ref[:, count - LANES :] = jnp.zeros((8, LANES), f32)


def decode_scale(code):
    return jnp.exp2(code.astype(jnp.int32).astype(f32) * (1.0 / 256)) * (1.0 / CODE_STEPS)


def scale_code(largest):
    level = jnp.floor(jnp.log(jnp.maximum(largest, 1e-30)) * (256 * 1.4426950408889634)) + 1.0
    return level


def to_i16(values):
    return jnp.round(values).astype(jnp.int32).astype(i16)


def wide(tile, width):
    return jnp.concatenate([tile] * (width // LANES), axis=1)


def folded(block, join):
    parts = [block[:, i : i + LANES] for i in range(0, block.shape[1], LANES)]
    while len(parts) > 1:
        parts = [join(a, b) for a, b in zip(parts[::2], parts[1::2])]
    return parts[0]


def folded_max(block):
    return folded(jnp.abs(block), jnp.maximum)


def encode(source, largest, targets, width):
    count = source.shape[1]
    code = scale_code(largest).astype(jnp.int32).astype(i16)
    for target in targets:
        target[:, count : count + LANES] = code
    inverse = wide(1.0 / decode_scale(code), width)

    def step(c, none):
        values = to_i16(source[:, cols(c, width)] * inverse)
        for target in targets:
            target[:, cols(c, width)] = values
        return none

    lax.fori_loop(0, count // width, step, 0)


def field_copies(sources, kept, arrived, stage, span):
    at = pl.ds(stage * span, span)
    whole = lambda ref: (slice(None),) * (len(ref.shape) - 1) + (at,)
    return [
        pltpu.make_async_copy(source.at[whole(source)], target.at[whole(target)], arrived.at[stage, place])
        for place, (source, target) in enumerate(zip(sources, kept))
    ]


def edge_kernel(state_far, adjoint_far, edge, state, adjoint, arrived, *, width, stages):
    ids = row_ids(width)
    span = edge.shape[1] // stages
    copies = functools.partial(
        field_copies, (state_far, adjoint_far), (state, adjoint), arrived, span=span
    )
    for stage in range(stages):
        for copy in copies(stage):
            copy.start()

    for stage in range(stages):
        for copy in copies(stage):
            copy.wait()

        def step(c, none):
            at = cols(stage * (span // width) + c, width)
            first = state[0, 0, :, at].astype(f32)
            rows = [state[1, 0, :, at], adjoint[0, 0, :, at], adjoint[1, 0, :, at]]
            for place, row in enumerate(rows):
                first = jnp.where(ids == place + 1, pltpu.roll(row.astype(f32), place + 1, 0), first)
            edge[:, at] = first[:4].astype(jnp.bfloat16)
            return none

        lax.fori_loop(0, span // width, step, 0)


def code_kernel(design_far, code_far, design, code, arrived, left, *, width, stages):
    span = design.shape[1] // stages

    def load(stage):
        at = pl.ds(stage * span, span)
        return pltpu.make_async_copy(design_far.at[:, at], design.at[:, at], arrived.at[stage])

    def save(stage):
        at = pl.ds(stage * span, span)
        return pltpu.make_async_copy(code.at[:, at], code_far.at[:, at], left.at[stage])

    for stage in range(stages):
        load(stage).start()
    for stage in range(stages):
        load(stage).wait()

        def step(c, none):
            at = cols(stage * (span // width) + c, width)
            code[:, at] = to_i16(design[:, at] * DESIGN_STEPS)
            return none

        lax.fori_loop(0, span // width, step, 0)
        save(stage).start()
    for stage in range(stages):
        save(stage).wait()


def element_kernel(
    omega_sq,
    assign,
    state_far,
    adjoint_far,
    edge_far,
    elastic_far,
    inertia_far,
    state,
    adjoint,
    edge,
    elastic,
    inertia,
    arrived,
    left,
    *,
    width,
    stages,
):
    omega = omega_sq[assign[0]]
    ids = row_ids(width)
    span = elastic.shape[1] // stages
    count = span // width
    copies = functools.partial(
        field_copies, (state_far, adjoint_far, edge_far), (state, adjoint, edge), arrived, span=span
    )
    for stage in reversed(range(stages)):
        for copy in copies(stage):
            copy.start()

    def shifted(block, carry):
        return moved(jnp.concatenate([block, carry], axis=1), 1)[:, :width]

    def step(stage, c, carries):
        at = cols((stage + 1) * count - 1 - c, width)
        edges = edge[:, at].astype(f32)
        fields = [state[0, 0, :, at], state[1, 0, :, at], adjoint[0, 0, :, at], adjoint[1, 0, :, at]]
        kept = []
        parts = []
        for place, field in enumerate(fields):
            here = field.astype(f32)
            row = jnp.broadcast_to(edges[place : place + 1], here.shape)
            below = jnp.where(ids == 7, row, pltpu.roll(here, 7, 0))
            plus = here + below
            minus = here - below
            kept += [plus[:, :LANES], minus[:, :LANES]]
            plus_next = shifted(plus, carries[2 * place])
            minus_next = shifted(minus, carries[2 * place + 1])
            parts.append((plus + plus_next, plus - plus_next, minus + minus_next, minus - minus_next))
        sr, si, ar, ai = parts
        same = [ar[k] * sr[k] - ai[k] * si[k] for k in range(4)]
        cross = [ar[k] * si[k] + ai[k] * sr[k] for k in range(1, 4)]
        same_mixed = same[1] + same[2]
        cross_mixed = cross[0] + cross[1]
        stiff = 1.5 * (same_mixed - LOSS * cross_mixed) + (same[3] - LOSS * cross[2])
        mass = 2.25 * same[0] + 0.75 * same_mixed + 0.25 * same[3]
        elastic[:, at] = stiff * (EXPONENT * (1.0 - SOFT_FLOOR) / 6.0)
        inertia[:, at] = mass * (omega * (1.0 / 36.0))
        return tuple(kept)

    def results(stage):
        at = pl.ds(stage * span, span)
        return [
            pltpu.make_async_copy(source.at[:, at], target.at[:, at], left.at[stage, place])
            for place, (source, target) in enumerate(((elastic, elastic_far), (inertia, inertia_far)))
        ]

    carries = (jnp.zeros((8, LANES), f32),) * 8
    for stage in reversed(range(stages)):
        for copy in copies(stage):
            copy.wait()
        carries = lax.fori_loop(0, count, functools.partial(step, stage), carries, unroll=2)
        for copy in results(stage):
            copy.start()
    for stage in reversed(range(stages)):
        for copy in results(stage):
            copy.wait()


def tap_sums(before, after):
    near = jnp.maximum(RADIUS - before, 0)
    far = jnp.maximum(RADIUS - after, 0)
    missing = near * (near + 1) + far * (far + 1)
    return float((RADIUS + 1) ** 2) - 0.5 * missing.astype(f32)


def partial_kernel(top, *refs, stages, whole_rows):
    sources, out_far, kept = refs[:6], refs[6], refs[7:13]
    rowed, spread, blocks, out, arrived, left = refs[13:]
    design, above, below, passive, elastic, inertia = kept
    peers = out.shape[0]
    piece = design.shape[1] // peers
    narrow = 2048
    span = design.shape[1] // stages

    def early(stage):
        at = pl.ds(stage * span, span)
        return [
            pltpu.make_async_copy(sources[k].at[:, at], kept[k].at[:, at], arrived.at[stage, k])
            for k in range(3)
        ]

    late = [pltpu.make_async_copy(sources[k], kept[k], arrived.at[0, k]) for k in range(3, 6)]
    for stage in range(stages):
        for copy in early(stage):
            copy.start()
    for copy in late:
        copy.start()
    clear_ends(rowed)
    clear_ends(spread)

    def filter_rows(c, none):
        at = cols(c, narrow)
        upper = above[:, at].astype(jnp.int32).astype(f32) * (1.0 / DESIGN_STEPS)
        lower = below[:, at].astype(jnp.int32).astype(f32) * (1.0 / DESIGN_STEPS)
        rowed[:, inner_cols(c, narrow)] = row_filter(upper, design[:, at], lower)
        return none

    for stage in range(stages):
        for copy in early(stage):
            copy.wait()
        first = stage * (span // narrow)
        lax.fori_loop(first, first + span // narrow, filter_rows, 0)
    for copy in late:
        copy.wait()

    row = top[0] + row_ids(LANES)
    lane = lax.broadcasted_iota(jnp.int32, (8, LANES), 1)
    full = float((RADIUS + 1) ** 2)
    inside = 1.0 / (full * tap_sums(row, whole_rows - 1 - row))
    left_end = full / tap_sums(lane, RADIUS)
    right_end = full / tap_sums(RADIUS, LANES - 1 - lane)

    def scale(c, none):
        at = cols(c, piece)
        first = inside * jnp.where(c == 0, left_end, 1.0)
        last = inside * jnp.where(c == peers - 1, right_end, 1.0)
        weights = jnp.concatenate([first] + [inside] * (piece // LANES - 2) + [last], axis=1)
        tilde = col_filter(rowed[:, padded_cols(c, piece)])[:, LANES : LANES + piece] * weights
        steep = jnp.tanh(SHARPNESS * (tilde - THRESHOLD))
        solid = passive[:, at] > 0
        density = jnp.where(solid, 1.0, (TANH_HALF + steep) * (0.5 / TANH_HALF))
        slope = jnp.where(solid, 0.0, (1.0 - steep * steep) * (SHARPNESS * 0.5 / TANH_HALF))
        block = (density * density * elastic[:, at] - inertia[:, at]) * (slope * weights)
        spread[:, inner_cols(c, piece)] = block
        return none

    lax.fori_loop(0, peers, scale, 0)

    def send(peer, none):
        block = col_filter(spread[:, padded_cols(peer, piece)])[:, LANES : LANES + piece]
        blocks[...] = block
        encode(blocks, folded_max(block), [out.at[peer]], narrow)
        pltpu.make_async_copy(out.at[peer], out_far.at[peer], left.at[peer]).start()
        return none

    lax.fori_loop(0, peers, send, 0)
    for peer in range(peers):
        pltpu.make_async_copy(out.at[peer], out_far.at[peer], left.at[peer]).wait()


def sum_kernel(coded, out, *, width):
    peers, piece = coded.shape[0], out.shape[1]
    scales = [wide(decode_scale(coded[peer, :, piece:]), width) for peer in range(peers)]

    def step(c, none):
        at = cols(c, width)
        total = None
        for peer in range(peers):
            term = coded[peer, :, at].astype(jnp.int32).astype(f32) * scales[peer]
            total = term if total is None else total + term
        out[:, at] = total
        return none

    lax.fori_loop(0, piece // width, step, 0)


def back_kernel(above, here, below, out, shared, blocks, *, width):
    piece = here.shape[1]
    zeros = jnp.zeros((8, LANES), f32)

    def step(c, carry):
        largest, squares = carry
        at = cols(c, width)
        block = row_filter(above[:, at], here[:, at], below[:, at])
        blocks[:, at] = block
        return jnp.maximum(largest, folded_max(block)), squares + folded(block * block, jnp.add)

    largest, squares = lax.fori_loop(0, piece // width, step, (zeros, zeros))
    encode(blocks, largest, [out.at[peer] for peer in range(out.shape[0])], width)
    shared[...] = squares


def fold_kernel(own, first, second, both, total):
    total[...] = (own[...] + first[...]) + (second[...] + both[...])


def result_kernel(coded, squares, out_far, out, left, *, width, elements):
    peers = coded.shape[0]
    piece = out.shape[1] // peers
    mean = jnp.sum(squares[...], keepdims=True) * (1.0 / elements) + EPSILON
    root = lax.rsqrt(mean)
    root = root * (1.5 - 0.5 * mean * root * root)

    def finished(peer):
        at = pl.ds(peer * piece, piece)
        return pltpu.make_async_copy(out.at[:, at], out_far.at[:, at], left.at[peer])

    for peer in range(peers):
        scale = wide(decode_scale(coded[peer, :, piece:]) * root, width)

        def step(c, none):
            block = coded[peer, :, cols(c, width)].astype(jnp.int32).astype(f32) * scale
            out[:, cols(peer * (piece // width) + c, width)] = block
            return none

        lax.fori_loop(0, piece // width, step, 0)
        finished(peer).start()
    for peer in range(peers):
        finished(peer).wait()


def layer(design, passive, state, adjoint, omega_sq, assign):
    slab_rows, width = design.shape
    rows = lax.axis_size("rows")
    peers = lax.axis_size("freq")
    whole_rows = slab_rows * rows
    piece = width // peers
    up = [(i, i + 1) for i in range(rows - 1)]
    down = [(target, source) for source, target in up]
    smem = pl.BlockSpec(memory_space=pltpu.SMEM)

    in_place = pl.BlockSpec(memory_space=pltpu.HBM)
    stages = 4
    field_scratch = [
        pltpu.VMEM(state.shape, state.dtype),
        pltpu.VMEM(adjoint.shape, adjoint.dtype),
        pltpu.SemaphoreType.DMA((stages, 2)),
    ]
    edge = pl.pallas_call(
        functools.partial(edge_kernel, width=2048, stages=stages),
        out_shape=jax.ShapeDtypeStruct((4, width), jnp.bfloat16),
        in_specs=[in_place, in_place],
        out_specs=vmem(1)[0],
        scratch_shapes=field_scratch,
        compiler_params=params(63),
        cost_estimate=cost(8 * slab_rows * width, 4 * 1024 * 1024),
        name="edge",
    )(state, adjoint)
    edge_below = lax.ppermute(edge, "rows", down)
    code = pl.pallas_call(
        functools.partial(code_kernel, width=2048, stages=stages),
        out_shape=jax.ShapeDtypeStruct((slab_rows, width), i16),
        in_specs=[in_place],
        out_specs=in_place,
        scratch_shapes=[
            pltpu.VMEM((slab_rows, width), f32),
            pltpu.VMEM((slab_rows, width), i16),
            pltpu.SemaphoreType.DMA((stages,)),
            pltpu.SemaphoreType.DMA((stages,)),
        ],
        compiler_params=params(63),
        name="code",
    )(design)
    code_below = lax.ppermute(code, "rows", down)
    code_above = lax.ppermute(code, "rows", up)

    top = (lax.axis_index("rows") * slab_rows).astype(jnp.int32).reshape(1)

    slab = jax.ShapeDtypeStruct((slab_rows, width), f32)
    elastic, inertia = pl.pallas_call(
        functools.partial(element_kernel, width=2048, stages=stages),
        out_shape=[slab, slab],
        in_specs=[smem, smem] + [in_place] * 3,
        out_specs=[in_place, in_place],
        scratch_shapes=field_scratch[:2]
        + [pltpu.VMEM(edge.shape, edge.dtype)]
        + [pltpu.VMEM((slab_rows, width), f32)] * 2
        + [pltpu.SemaphoreType.DMA((stages, 3)), pltpu.SemaphoreType.DMA((stages, 2))],
        compiler_params=params(63),
        cost_estimate=cost(80 * slab_rows * width, 8 * 1024 * 1024),
        name="element",
    )(omega_sq, assign, state, adjoint, edge_below)

    coded = jax.ShapeDtypeStruct((peers, slab_rows, piece + LANES), i16)
    operands = (design, code_above, code_below, passive, elastic, inertia)
    sent = pl.pallas_call(
        functools.partial(partial_kernel, stages=stages, whole_rows=whole_rows),
        out_shape=coded,
        in_specs=[smem] + [in_place] * len(operands),
        out_specs=in_place,
        scratch_shapes=[pltpu.VMEM(operand.shape, operand.dtype) for operand in operands]
        + [
            pltpu.VMEM((slab_rows, width + 2 * LANES), f32),
            pltpu.VMEM((slab_rows, width + 2 * LANES), f32),
            pltpu.VMEM((slab_rows, piece), f32),
            pltpu.VMEM(coded.shape, coded.dtype),
            pltpu.SemaphoreType.DMA((stages, len(operands))),
            pltpu.SemaphoreType.DMA((peers,)),
        ],
        compiler_params=params(63),
        cost_estimate=cost(150 * slab_rows * width, 14 * 1024 * 1024),
        name="partial",
    )(top, *operands)

    received = lax.all_to_all(sent, "freq", 0, 0, tiled=True)

    spread = pl.pallas_call(
        functools.partial(sum_kernel, width=1024),
        out_shape=jax.ShapeDtypeStruct((slab_rows, piece), f32),
        in_specs=vmem(1),
        out_specs=vmem(1)[0],
        compiler_params=params(8),
        name="total",
    )(received)
    spread_below = lax.ppermute(spread, "rows", down)
    spread_above = lax.ppermute(spread, "rows", up)

    tile = jax.ShapeDtypeStruct((8, LANES), f32)
    result, squares = pl.pallas_call(
        functools.partial(back_kernel, width=1024),
        out_shape=[coded, tile],
        in_specs=vmem(3),
        out_specs=vmem(2),
        scratch_shapes=[pltpu.VMEM((slab_rows, piece), f32)],
        compiler_params=params(8),
        name="back",
    )(spread_above, spread, spread_below)

    pieces = lax.all_to_all(result, "freq", 0, 0, tiled=True)

    everyone = ("rows", "freq")
    for first, second in SUM_STAGES:
        heard = [
            lax.ppermute(squares, everyone, [(i, i ^ mask) for i in range(rows * peers)])
            for mask in (first, second, first | second)
        ]
        squares = pl.pallas_call(
            fold_kernel,
            out_shape=tile,
            in_specs=vmem(4),
            out_specs=vmem(1)[0],
            compiler_params=params(4),
            cost_estimate=cost(1 << 20, 1 << 18),
        )(squares, *heard)

    return pl.pallas_call(
        functools.partial(result_kernel, width=2048, elements=float(whole_rows * width)),
        out_shape=slab,
        in_specs=vmem(2),
        out_specs=in_place,
        scratch_shapes=[pltpu.VMEM((slab_rows, width), f32), pltpu.SemaphoreType.DMA((peers,))],
        compiler_params=params(16),
        name="result",
    )(pieces, squares)


def solution(mesh):
    return jax.shard_map(
        layer,
        mesh=mesh,
        in_specs=(
            P("rows", None),
            P("rows", None),
            P(None, "freq", "rows", None),
            P(None, "freq", "rows", None),
            P(),
            P("freq"),
        ),
        out_specs=P("rows", None),
        check_vma=False,
    )
```

```python
import functools

import jax
import jax.numpy as jnp
from jax import lax
from jax.experimental import pallas as pl
from jax.experimental.pallas import tpu as pltpu
from jax.sharding import PartitionSpec as P


RADIUS = 8
LANES = 128
SHARPNESS = 8.0
THRESHOLD = 0.5
EXPONENT = 3.0
SOFT_FLOOR = 0.001
LOSS = 0.2
EPSILON = 1e-06
TANH_HALF = 0.999329299739067
DESIGN_STEPS = 32767.0
CODE_STEPS = 32700.0

f32 = jnp.float32
i16 = jnp.int16


def params(megabytes):
    return pltpu.CompilerParams(vmem_limit_bytes=megabytes * 1024 * 1024)


def vmem(count):
    return [pl.BlockSpec(memory_space=pltpu.VMEM)] * count


def cost(flops, moved):
    return pl.CostEstimate(flops=flops, bytes_accessed=moved, transcendentals=0)


def cols(index, width):
    return pl.ds(pl.multiple_of(index * width, width), width)


def row_ids(width):
    return lax.broadcasted_iota(jnp.int32, (8, width), 0)


def rows_up(block, count, ids):
    return jnp.where(ids < 8 - count, pltpu.roll(block, 8 - count, 0), 0.0)


def rows_down(block, count, ids):
    return jnp.where(ids >= count, pltpu.roll(block, count, 0), 0.0)


def row_filter(above, here, below):
    ids = row_ids(here.shape[1])
    upper = above - here
    lower = below - here
    for _ in range(2):
        for count in (1, 2, 4):
            upper = upper + rows_up(upper, count, ids)
            lower = lower + rows_down(lower, count, ids)
    total = here
    for count in (1, 2, 4):
        total = total + pltpu.roll(total, count, 0)
    return upper + lower + here + 10.0 * total


def moved(block, count):
    width = block.shape[1]
    return pltpu.roll(block, (width - count) % width, 1)


def band():
    shape = (3 * LANES, LANES)
    source = lax.broadcasted_iota(jnp.int32, shape, 0) - LANES
    target = lax.broadcasted_iota(jnp.int32, shape, 1)
    taps = jnp.maximum(RADIUS + 1 - jnp.abs(source - target), 0)
    return taps.astype(f32).astype(jnp.bfloat16)


def col_filter(window, taps):
    count = window.shape[1] // LANES - 2
    half = count // 2
    tiles = [window[:, i * LANES : (i + 1) * LANES] for i in range(count + 2)]
    stacked = jnp.concatenate(
        [tiles[i + side] for i in range(half + 2) for side in (0, half)], axis=0
    )
    coarse = stacked.astype(jnp.bfloat16)
    fine = (stacked - coarse.astype(f32)).astype(jnp.bfloat16)
    left, here, right = (slice(start, start + 16 * half) for start in (0, 16, 32))

    def product(first, second, weights):
        return jnp.dot(
            jnp.concatenate([first, second], axis=1), weights, preferred_element_type=f32
        )

    near, far = taps[: 2 * LANES], taps[2 * LANES :]
    total = product(coarse[left], coarse[here], near) + product(fine[left], fine[here], near)
    total = total + product(coarse[right], fine[right], jnp.concatenate([far, far], axis=0))
    halves = [
        [total[16 * i + 8 * side : 16 * i + 8 * side + 8] for i in range(half)] for side in (0, 1)
    ]
    return jnp.concatenate(halves[0] + halves[1], axis=1)


def padded_cols(index, width):
    return pl.ds(pl.multiple_of(index * width, LANES), width + 2 * LANES)


def inner_cols(index, width):
    return pl.ds(pl.multiple_of(index * width + LANES, LANES), width)


def clear_ends(ref):
    count = ref.shape[1]
    ref[:, :LANES] = jnp.zeros((8, LANES), f32)
    ref[:, count - LANES :] = jnp.zeros((8, LANES), f32)


def decode_scale(code):
    return jnp.exp2(code.astype(jnp.int32).astype(f32) * (1.0 / 256)) * (1.0 / CODE_STEPS)


def scale_code(largest):
    level = jnp.floor(jnp.log(jnp.maximum(largest, 1e-30)) * (256 * 1.4426950408889634)) + 1.0
    return level


def to_i16(values):
    return jnp.round(values).astype(jnp.int32).astype(i16)


def wide(tile, width):
    return jnp.concatenate([tile] * (width // LANES), axis=1)


def folded(block, join):
    parts = [block[:, i : i + LANES] for i in range(0, block.shape[1], LANES)]
    while len(parts) > 1:
        parts = [join(a, b) for a, b in zip(parts[::2], parts[1::2])]
    return parts[0]


def folded_max(block):
    return folded(jnp.abs(block), jnp.maximum)


def encode(source, largest, targets, width):
    count = source.shape[1]
    code = scale_code(largest).astype(jnp.int32).astype(i16)
    for target in targets:
        target[:, count : count + LANES] = code
    inverse = wide(1.0 / decode_scale(code), width)

    def step(c, none):
        values = to_i16(source[:, cols(c, width)] * inverse)
        for target in targets:
            target[:, cols(c, width)] = values
        return none

    lax.fori_loop(0, count // width, step, 0)


def field_copies(sources, kept, arrived, stage, span):
    at = pl.ds(stage * span, span)
    whole = lambda ref: (slice(None),) * (len(ref.shape) - 1) + (at,)
    return [
        pltpu.make_async_copy(source.at[whole(source)], target.at[whole(target)], arrived.at[stage, place])
        for place, (source, target) in enumerate(zip(sources, kept))
    ]


def edge_kernel(state_far, adjoint_far, edge, state, adjoint, arrived, *, width, stages):
    ids = row_ids(width)
    span = edge.shape[1] // stages
    copies = functools.partial(
        field_copies, (state_far, adjoint_far), (state, adjoint), arrived, span=span
    )
    for stage in range(stages):
        for copy in copies(stage):
            copy.start()

    for stage in range(stages):
        for copy in copies(stage):
            copy.wait()

        def step(c, none):
            at = cols(stage * (span // width) + c, width)
            first = state[0, 0, :, at].astype(f32)
            rows = [state[1, 0, :, at], adjoint[0, 0, :, at], adjoint[1, 0, :, at]]
            for place, row in enumerate(rows):
                first = jnp.where(ids == place + 1, pltpu.roll(row.astype(f32), place + 1, 0), first)
            edge[:, at] = first[:4].astype(jnp.bfloat16)
            return none

        lax.fori_loop(0, span // width, step, 0)


def code_kernel(design_far, code_far, design, code, arrived, left, *, width, stages):
    span = design.shape[1] // stages

    def load(stage):
        at = pl.ds(stage * span, span)
        return pltpu.make_async_copy(design_far.at[:, at], design.at[:, at], arrived.at[stage])

    def save(stage):
        at = pl.ds(stage * span, span)
        return pltpu.make_async_copy(code.at[:, at], code_far.at[:, at], left.at[stage])

    for stage in range(stages):
        load(stage).start()
    for stage in range(stages):
        load(stage).wait()

        def step(c, none):
            at = cols(stage * (span // width) + c, width)
            code[:, at] = to_i16(design[:, at] * DESIGN_STEPS)
            return none

        lax.fori_loop(0, span // width, step, 0)
        save(stage).start()
    for stage in range(stages):
        save(stage).wait()


def element_kernel(
    omega_sq,
    assign,
    state_far,
    adjoint_far,
    edge_far,
    elastic_far,
    inertia_far,
    state,
    adjoint,
    edge,
    elastic,
    inertia,
    arrived,
    left,
    *,
    width,
    stages,
):
    omega = omega_sq[assign[0]]
    ids = row_ids(width)
    span = elastic.shape[1] // stages
    count = span // width
    copies = functools.partial(
        field_copies, (state_far, adjoint_far, edge_far), (state, adjoint, edge), arrived, span=span
    )
    for stage in reversed(range(stages)):
        for copy in copies(stage):
            copy.start()

    def shifted(block, carry):
        return moved(jnp.concatenate([block, carry], axis=1), 1)[:, :width]

    def step(stage, c, carries):
        at = cols((stage + 1) * count - 1 - c, width)
        edges = edge[:, at].astype(f32)
        fields = [state[0, 0, :, at], state[1, 0, :, at], adjoint[0, 0, :, at], adjoint[1, 0, :, at]]
        kept = []
        parts = []
        for place, field in enumerate(fields):
            here = field.astype(f32)
            row = jnp.broadcast_to(edges[place : place + 1], here.shape)
            below = jnp.where(ids == 7, row, pltpu.roll(here, 7, 0))
            plus = here + below
            minus = here - below
            kept += [plus[:, :LANES], minus[:, :LANES]]
            plus_next = shifted(plus, carries[2 * place])
            minus_next = shifted(minus, carries[2 * place + 1])
            parts.append((plus + plus_next, plus - plus_next, minus + minus_next, minus - minus_next))
        sr, si, ar, ai = parts
        same = [ar[k] * sr[k] - ai[k] * si[k] for k in range(4)]
        cross = [ar[k] * si[k] + ai[k] * sr[k] for k in range(1, 4)]
        same_mixed = same[1] + same[2]
        cross_mixed = cross[0] + cross[1]
        stiff = 1.5 * (same_mixed - LOSS * cross_mixed) + (same[3] - LOSS * cross[2])
        mass = 2.25 * same[0] + 0.75 * same_mixed + 0.25 * same[3]
        elastic[:, at] = stiff * (EXPONENT * (1.0 - SOFT_FLOOR) / 6.0)
        inertia[:, at] = mass * (omega * (1.0 / 36.0))
        return tuple(kept)

    def results(stage):
        at = pl.ds(stage * span, span)
        return [
            pltpu.make_async_copy(source.at[:, at], target.at[:, at], left.at[stage, place])
            for place, (source, target) in enumerate(((elastic, elastic_far), (inertia, inertia_far)))
        ]

    carries = (jnp.zeros((8, LANES), f32),) * 8
    for stage in reversed(range(stages)):
        for copy in copies(stage):
            copy.wait()
        carries = lax.fori_loop(0, count, functools.partial(step, stage), carries, unroll=2)
        for copy in results(stage):
            copy.start()
    for stage in reversed(range(stages)):
        for copy in results(stage):
            copy.wait()


def tap_sums(before, after):
    near = jnp.maximum(RADIUS - before, 0)
    far = jnp.maximum(RADIUS - after, 0)
    missing = near * (near + 1) + far * (far + 1)
    return float((RADIUS + 1) ** 2) - 0.5 * missing.astype(f32)


def partial_kernel(top, *refs, stages, whole_rows):
    sources, out_far, kept = refs[:6], refs[6], refs[7:13]
    rowed, spread, blocks, out, arrived, left = refs[13:]
    design, above, below, passive, elastic, inertia = kept
    peers = out.shape[0]
    piece = design.shape[1] // peers
    narrow = 2048
    span = design.shape[1] // stages

    def early(stage):
        at = pl.ds(stage * span, span)
        return [
            pltpu.make_async_copy(sources[k].at[:, at], kept[k].at[:, at], arrived.at[stage, k])
            for k in range(3)
        ]

    late = [pltpu.make_async_copy(sources[k], kept[k], arrived.at[0, k]) for k in range(3, 6)]
    for stage in range(stages):
        for copy in early(stage):
            copy.start()
    for copy in late:
        copy.start()
    clear_ends(rowed)
    clear_ends(spread)

    def filter_rows(c, none):
        at = cols(c, narrow)
        upper = above[:, at].astype(jnp.int32).astype(f32) * (1.0 / DESIGN_STEPS)
        lower = below[:, at].astype(jnp.int32).astype(f32) * (1.0 / DESIGN_STEPS)
        rowed[:, inner_cols(c, narrow)] = row_filter(upper, design[:, at], lower)
        return none

    for stage in range(stages):
        for copy in early(stage):
            copy.wait()
        first = stage * (span // narrow)
        lax.fori_loop(first, first + span // narrow, filter_rows, 0)
    for copy in late:
        copy.wait()

    taps = band()
    row = top[0] + row_ids(LANES)
    lane = lax.broadcasted_iota(jnp.int32, (8, LANES), 1)
    full = float((RADIUS + 1) ** 2)
    inside = 1.0 / (full * tap_sums(row, whole_rows - 1 - row))
    left_end = full / tap_sums(lane, RADIUS)
    right_end = full / tap_sums(RADIUS, LANES - 1 - lane)

    def scale(c, none):
        at = cols(c, piece)
        first = inside * jnp.where(c == 0, left_end, 1.0)
        last = inside * jnp.where(c == peers - 1, right_end, 1.0)
        weights = jnp.concatenate([first] + [inside] * (piece // LANES - 2) + [last], axis=1)
        tilde = col_filter(rowed[:, padded_cols(c, piece)], taps) * weights
        steep = jnp.tanh(SHARPNESS * (tilde - THRESHOLD))
        solid = passive[:, at] > 0
        density = jnp.where(solid, 1.0, (TANH_HALF + steep) * (0.5 / TANH_HALF))
        slope = jnp.where(solid, 0.0, (1.0 - steep * steep) * (SHARPNESS * 0.5 / TANH_HALF))
        block = (density * density * elastic[:, at] - inertia[:, at]) * (slope * weights)
        spread[:, inner_cols(c, piece)] = block
        return none

    lax.fori_loop(0, peers, scale, 0)

    def send(peer, none):
        block = col_filter(spread[:, padded_cols(peer, piece)], taps)
        blocks[...] = block
        encode(blocks, folded_max(block), [out.at[peer]], narrow)
        pltpu.make_async_copy(out.at[peer], out_far.at[peer], left.at[peer]).start()
        return none

    lax.fori_loop(0, peers, send, 0)
    for peer in range(peers):
        pltpu.make_async_copy(out.at[peer], out_far.at[peer], left.at[peer]).wait()


def sum_kernel(coded, out, *, width):
    peers, piece = coded.shape[0], out.shape[1]
    scales = [wide(decode_scale(coded[peer, :, piece:]), width) for peer in range(peers)]

    def step(c, none):
        at = cols(c, width)
        total = None
        for peer in range(peers):
            term = coded[peer, :, at].astype(jnp.int32).astype(f32) * scales[peer]
            total = term if total is None else total + term
        out[:, at] = total
        return none

    lax.fori_loop(0, piece // width, step, 0)


def back_kernel(above, here, below, out, blocks, *, width):
    piece = here.shape[1]
    zeros = jnp.zeros((8, LANES), f32)

    def step(c, carry):
        largest, squares = carry
        at = cols(c, width)
        block = row_filter(above[:, at], here[:, at], below[:, at])
        blocks[:, at] = block
        return jnp.maximum(largest, folded_max(block)), squares + folded(block * block, jnp.add)

    largest, squares = lax.fori_loop(0, piece // width, step, (zeros, zeros))
    encode(blocks, largest, [out.at[peer] for peer in range(out.shape[0])], width)
    code = scale_code(squares).astype(jnp.int32).astype(i16)
    values = to_i16(squares / decode_scale(code))
    for peer in range(out.shape[0]):
        out[peer, :, piece + LANES : piece + 2 * LANES] = code
        out[peer, :, piece + 2 * LANES :] = values


def squares_kernel(coded, squares):
    piece = coded.shape[2] - 3 * LANES
    total = jnp.zeros((8, LANES), f32)
    for peer in range(coded.shape[0]):
        values = coded[peer, :, piece + 2 * LANES :].astype(jnp.int32).astype(f32)
        total = total + values * decode_scale(coded[peer, :, piece + LANES : piece + 2 * LANES])
    squares[...] = jnp.broadcast_to(total[None], squares.shape)


def result_kernel(coded, squares, out_far, out, left, *, width, elements):
    peers = coded.shape[0]
    piece = out.shape[1] // peers
    mean = jnp.sum(jnp.sum(squares[...], axis=0), keepdims=True) * (1.0 / elements) + EPSILON
    root = lax.rsqrt(mean)
    root = root * (1.5 - 0.5 * mean * root * root)

    def finished(peer):
        at = pl.ds(peer * piece, piece)
        return pltpu.make_async_copy(out.at[:, at], out_far.at[:, at], left.at[peer])

    for peer in range(peers):
        scale = wide(decode_scale(coded[peer, :, piece : piece + LANES]) * root, width)

        def step(c, none):
            block = coded[peer, :, cols(c, width)].astype(jnp.int32).astype(f32) * scale
            out[:, cols(peer * (piece // width) + c, width)] = block
            return none

        lax.fori_loop(0, piece // width, step, 0)
        finished(peer).start()
    for peer in range(peers):
        finished(peer).wait()


def layer(design, passive, state, adjoint, omega_sq, assign):
    slab_rows, width = design.shape
    rows = lax.axis_size("rows")
    peers = lax.axis_size("freq")
    whole_rows = slab_rows * rows
    piece = width // peers
    up = [(i, i + 1) for i in range(rows - 1)]
    down = [(target, source) for source, target in up]
    smem = pl.BlockSpec(memory_space=pltpu.SMEM)

    in_place = pl.BlockSpec(memory_space=pltpu.HBM)
    stages = 4
    field_scratch = [
        pltpu.VMEM(state.shape, state.dtype),
        pltpu.VMEM(adjoint.shape, adjoint.dtype),
        pltpu.SemaphoreType.DMA((stages, 2)),
    ]
    edge = pl.pallas_call(
        functools.partial(edge_kernel, width=2048, stages=stages),
        out_shape=jax.ShapeDtypeStruct((4, width), jnp.bfloat16),
        in_specs=[in_place, in_place],
        out_specs=vmem(1)[0],
        scratch_shapes=field_scratch,
        compiler_params=params(63),
        cost_estimate=cost(8 * slab_rows * width, 4 * 1024 * 1024),
        name="edge",
    )(state, adjoint)
    edge_below = lax.ppermute(edge, "rows", down)
    code = pl.pallas_call(
        functools.partial(code_kernel, width=2048, stages=stages),
        out_shape=jax.ShapeDtypeStruct((slab_rows, width), i16),
        in_specs=[in_place],
        out_specs=in_place,
        scratch_shapes=[
            pltpu.VMEM((slab_rows, width), f32),
            pltpu.VMEM((slab_rows, width), i16),
            pltpu.SemaphoreType.DMA((stages,)),
            pltpu.SemaphoreType.DMA((stages,)),
        ],
        compiler_params=params(63),
        name="code",
    )(design)
    code_below = lax.ppermute(code, "rows", down)
    code_above = lax.ppermute(code, "rows", up)

    top = (lax.axis_index("rows") * slab_rows).astype(jnp.int32).reshape(1)

    slab = jax.ShapeDtypeStruct((slab_rows, width), f32)
    elastic, inertia = pl.pallas_call(
        functools.partial(element_kernel, width=2048, stages=stages),
        out_shape=[slab, slab],
        in_specs=[smem, smem] + [in_place] * 3,
        out_specs=[in_place, in_place],
        scratch_shapes=field_scratch[:2]
        + [pltpu.VMEM(edge.shape, edge.dtype)]
        + [pltpu.VMEM((slab_rows, width), f32)] * 2
        + [pltpu.SemaphoreType.DMA((stages, 3)), pltpu.SemaphoreType.DMA((stages, 2))],
        compiler_params=params(63),
        cost_estimate=cost(80 * slab_rows * width, 8 * 1024 * 1024),
        name="element",
    )(omega_sq, assign, state, adjoint, edge_below)

    coded = jax.ShapeDtypeStruct((peers, slab_rows, piece + LANES), i16)
    operands = (design, code_above, code_below, passive, elastic, inertia)
    sent = pl.pallas_call(
        functools.partial(partial_kernel, stages=stages, whole_rows=whole_rows),
        out_shape=coded,
        in_specs=[smem] + [in_place] * len(operands),
        out_specs=in_place,
        scratch_shapes=[pltpu.VMEM(operand.shape, operand.dtype) for operand in operands]
        + [
            pltpu.VMEM((slab_rows, width + 2 * LANES), f32),
            pltpu.VMEM((slab_rows, width + 2 * LANES), f32),
            pltpu.VMEM((slab_rows, piece), f32),
            pltpu.VMEM(coded.shape, coded.dtype),
            pltpu.SemaphoreType.DMA((stages, len(operands))),
            pltpu.SemaphoreType.DMA((peers,)),
        ],
        compiler_params=params(63),
        cost_estimate=cost(150 * slab_rows * width, 14 * 1024 * 1024),
        name="partial",
    )(top, *operands)

    received = lax.all_to_all(sent, "freq", 0, 0, tiled=True)

    spread = pl.pallas_call(
        functools.partial(sum_kernel, width=1024),
        out_shape=jax.ShapeDtypeStruct((slab_rows, piece), f32),
        in_specs=vmem(1),
        out_specs=vmem(1)[0],
        compiler_params=params(8),
        name="total",
    )(received)
    spread_below = lax.ppermute(spread, "rows", down)
    spread_above = lax.ppermute(spread, "rows", up)

    wide_coded = jax.ShapeDtypeStruct((peers, slab_rows, piece + 3 * LANES), i16)
    result = pl.pallas_call(
        functools.partial(back_kernel, width=1024),
        out_shape=wide_coded,
        in_specs=vmem(3),
        out_specs=vmem(1)[0],
        scratch_shapes=[pltpu.VMEM((slab_rows, piece), f32)],
        compiler_params=params(8),
        name="back",
    )(spread_above, spread, spread_below)

    pieces = lax.all_to_all(result, "freq", 0, 0, tiled=True)

    squares = pl.pallas_call(
        squares_kernel,
        out_shape=jax.ShapeDtypeStruct((rows, 8, LANES), f32),
        in_specs=vmem(1),
        out_specs=vmem(1)[0],
        compiler_params=params(8),
        name="squares",
    )(pieces)
    squares = lax.all_to_all(squares, "rows", 0, 0, tiled=True)

    return pl.pallas_call(
        functools.partial(result_kernel, width=2048, elements=float(whole_rows * width)),
        out_shape=slab,
        in_specs=vmem(2),
        out_specs=in_place,
        scratch_shapes=[pltpu.VMEM((slab_rows, width), f32), pltpu.SemaphoreType.DMA((peers,))],
        compiler_params=params(16),
        name="result",
    )(pieces, squares)


def solution(mesh):
    return jax.shard_map(
        layer,
        mesh=mesh,
        in_specs=(
            P("rows", None),
            P("rows", None),
            P(None, "freq", "rows", None),
            P(None, "freq", "rows", None),
            P(),
            P("freq"),
        ),
        out_specs=P("rows", None),
        check_vma=False,
    )
```

```python
import functools

import jax
import jax.numpy as jnp
from jax import lax
from jax.experimental import pallas as pl
from jax.experimental.pallas import tpu as pltpu
from jax.sharding import PartitionSpec as P


RADIUS = 8
LANES = 128
SHARPNESS = 8.0
THRESHOLD = 0.5
EXPONENT = 3.0
SOFT_FLOOR = 0.001
LOSS = 0.2
EPSILON = 1e-06
TANH_HALF = 0.999329299739067
DESIGN_STEPS = 32767.0
CODE_STEPS = 32700.0

f32 = jnp.float32
i16 = jnp.int16


def params(megabytes):
    return pltpu.CompilerParams(vmem_limit_bytes=megabytes * 1024 * 1024)


def vmem(count):
    return [pl.BlockSpec(memory_space=pltpu.VMEM)] * count


def cost(flops, moved):
    return pl.CostEstimate(flops=flops, bytes_accessed=moved, transcendentals=0)


def cols(index, width):
    return pl.ds(pl.multiple_of(index * width, width), width)


def row_ids(width):
    return lax.broadcasted_iota(jnp.int32, (8, width), 0)


def rows_up(block, count, ids):
    return jnp.where(ids < 8 - count, pltpu.roll(block, 8 - count, 0), 0.0)


def rows_down(block, count, ids):
    return jnp.where(ids >= count, pltpu.roll(block, count, 0), 0.0)


def row_filter(above, here, below):
    ids = row_ids(here.shape[1])
    upper = above - here
    lower = below - here
    for _ in range(2):
        for count in (1, 2, 4):
            upper = upper + rows_up(upper, count, ids)
            lower = lower + rows_down(lower, count, ids)
    total = here
    for count in (1, 2, 4):
        total = total + pltpu.roll(total, count, 0)
    return upper + lower + here + 10.0 * total


def moved(block, count):
    width = block.shape[1]
    return pltpu.roll(block, (width - count) % width, 1)


def band():
    shape = (3 * LANES, LANES)
    source = lax.broadcasted_iota(jnp.int32, shape, 0) - LANES
    target = lax.broadcasted_iota(jnp.int32, shape, 1)
    taps = jnp.maximum(RADIUS + 1 - jnp.abs(source - target), 0)
    return taps.astype(f32).astype(jnp.bfloat16)


def col_filter(window, taps):
    count = window.shape[1] // LANES - 2
    half = count // 2
    tiles = [window[:, i * LANES : (i + 1) * LANES] for i in range(count + 2)]
    stacked = jnp.concatenate(
        [tiles[i + side] for i in range(half + 2) for side in (0, half)], axis=0
    )
    coarse = stacked.astype(jnp.bfloat16)
    fine = (stacked - coarse.astype(f32)).astype(jnp.bfloat16)
    left, here, right = (slice(start, start + 16 * half) for start in (0, 16, 32))

    def product(first, second, weights):
        return jnp.dot(
            jnp.concatenate([first, second], axis=1), weights, preferred_element_type=f32
        )

    near, far = taps[: 2 * LANES], taps[2 * LANES :]
    total = product(coarse[left], coarse[here], near) + product(fine[left], fine[here], near)
    total = total + product(coarse[right], fine[right], jnp.concatenate([far, far], axis=0))
    halves = [
        [total[16 * i + 8 * side : 16 * i + 8 * side + 8] for i in range(half)] for side in (0, 1)
    ]
    return jnp.concatenate(halves[0] + halves[1], axis=1)


def padded_cols(index, width):
    return pl.ds(pl.multiple_of(index * width, LANES), width + 2 * LANES)


def inner_cols(index, width):
    return pl.ds(pl.multiple_of(index * width + LANES, LANES), width)


def clear_ends(ref):
    count = ref.shape[1]
    ref[:, :LANES] = jnp.zeros((8, LANES), f32)
    ref[:, count - LANES :] = jnp.zeros((8, LANES), f32)


def decode_scale(code):
    return jnp.exp2(code.astype(jnp.int32).astype(f32) * (1.0 / 256)) * (1.0 / CODE_STEPS)


def scale_code(largest):
    level = jnp.floor(jnp.log(jnp.maximum(largest, 1e-30)) * (256 * 1.4426950408889634)) + 1.0
    return level


def to_i16(values):
    return jnp.round(values).astype(jnp.int32).astype(i16)


def wide(tile, width):
    return jnp.concatenate([tile] * (width // LANES), axis=1)


def folded(block, join):
    parts = [block[:, i : i + LANES] for i in range(0, block.shape[1], LANES)]
    while len(parts) > 1:
        parts = [join(a, b) for a, b in zip(parts[::2], parts[1::2])]
    return parts[0]


def folded_max(block):
    return folded(jnp.abs(block), jnp.maximum)


def encode(source, largest, targets, width):
    count = source.shape[1]
    code = scale_code(largest).astype(jnp.int32).astype(i16)
    for target in targets:
        target[:, count : count + LANES] = code
    inverse = wide(1.0 / decode_scale(code), width)

    def step(c, none):
        values = to_i16(source[:, cols(c, width)] * inverse)
        for target in targets:
            target[:, cols(c, width)] = values
        return none

    lax.fori_loop(0, count // width, step, 0)


def field_copies(sources, kept, arrived, stage, span):
    at = pl.ds(stage * span, span)
    whole = lambda ref: (slice(None),) * (len(ref.shape) - 1) + (at,)
    return [
        pltpu.make_async_copy(source.at[whole(source)], target.at[whole(target)], arrived.at[stage, place])
        for place, (source, target) in enumerate(zip(sources, kept))
    ]


def prepare_kernel(
    state_far,
    adjoint_far,
    design_far,
    edge,
    code_far,
    state,
    adjoint,
    design,
    code,
    arrived,
    design_arrived,
    left,
    *,
    width,
    stages,
):
    ids = row_ids(width)
    span = edge.shape[1] // stages
    steps = span // width
    copies = functools.partial(
        field_copies, (state_far, adjoint_far), (state, adjoint), arrived, span=span
    )

    def load(stage):
        at = pl.ds(stage * span, span)
        return pltpu.make_async_copy(design_far.at[:, at], design.at[:, at], design_arrived.at[stage])

    def save(stage):
        at = pl.ds(stage * span, span)
        return pltpu.make_async_copy(code.at[:, at], code_far.at[:, at], left.at[stage])

    for stage in range(stages):
        load(stage).start()
    for stage in range(stages):
        for copy in copies(stage):
            copy.start()

    for stage in range(stages):
        load(stage).wait()

        def encode_rows(c, none):
            at = cols(stage * steps + c, width)
            code[:, at] = to_i16(design[:, at] * DESIGN_STEPS)
            return none

        lax.fori_loop(0, steps, encode_rows, 0)
        save(stage).start()

    for stage in range(stages):
        for copy in copies(stage):
            copy.wait()

        def pick_rows(c, none):
            at = cols(stage * steps + c, width)
            first = state[0, 0, :, at].astype(f32)
            rows = [state[1, 0, :, at], adjoint[0, 0, :, at], adjoint[1, 0, :, at]]
            for place, row in enumerate(rows):
                first = jnp.where(ids == place + 1, pltpu.roll(row.astype(f32), place + 1, 0), first)
            edge[:, at] = first[:4].astype(jnp.bfloat16)
            return none

        lax.fori_loop(0, steps, pick_rows, 0)
    for stage in range(stages):
        save(stage).wait()


def element_kernel(
    omega_sq,
    assign,
    state_far,
    adjoint_far,
    edge_far,
    elastic_far,
    inertia_far,
    state,
    adjoint,
    edge,
    elastic,
    inertia,
    arrived,
    left,
    *,
    width,
    stages,
):
    omega = omega_sq[assign[0]]
    ids = row_ids(width)
    span = elastic.shape[1] // stages
    count = span // width
    copies = functools.partial(
        field_copies, (state_far, adjoint_far, edge_far), (state, adjoint, edge), arrived, span=span
    )
    for stage in reversed(range(stages)):
        for copy in copies(stage):
            copy.start()

    def shifted(block, carry):
        return moved(jnp.concatenate([block, carry], axis=1), 1)[:, :width]

    def step(stage, c, carries):
        at = cols((stage + 1) * count - 1 - c, width)
        edges = edge[:, at].astype(f32)
        fields = [state[0, 0, :, at], state[1, 0, :, at], adjoint[0, 0, :, at], adjoint[1, 0, :, at]]
        kept = []
        parts = []
        for place, field in enumerate(fields):
            here = field.astype(f32)
            row = jnp.broadcast_to(edges[place : place + 1], here.shape)
            below = jnp.where(ids == 7, row, pltpu.roll(here, 7, 0))
            plus = here + below
            minus = here - below
            kept += [plus[:, :LANES], minus[:, :LANES]]
            plus_next = shifted(plus, carries[2 * place])
            minus_next = shifted(minus, carries[2 * place + 1])
            parts.append((plus + plus_next, plus - plus_next, minus + minus_next, minus - minus_next))
        sr, si, ar, ai = parts
        same = [ar[k] * sr[k] - ai[k] * si[k] for k in range(4)]
        cross = [ar[k] * si[k] + ai[k] * sr[k] for k in range(1, 4)]
        same_mixed = same[1] + same[2]
        cross_mixed = cross[0] + cross[1]
        stiff = 1.5 * (same_mixed - LOSS * cross_mixed) + (same[3] - LOSS * cross[2])
        mass = 2.25 * same[0] + 0.75 * same_mixed + 0.25 * same[3]
        elastic[:, at] = stiff * (EXPONENT * (1.0 - SOFT_FLOOR) / 6.0)
        inertia[:, at] = mass * (omega * (1.0 / 36.0))
        return tuple(kept)

    def results(stage):
        at = pl.ds(stage * span, span)
        return [
            pltpu.make_async_copy(source.at[:, at], target.at[:, at], left.at[stage, place])
            for place, (source, target) in enumerate(((elastic, elastic_far), (inertia, inertia_far)))
        ]

    carries = (jnp.zeros((8, LANES), f32),) * 8
    for stage in reversed(range(stages)):
        for copy in copies(stage):
            copy.wait()
        carries = lax.fori_loop(0, count, functools.partial(step, stage), carries, unroll=2)
        for copy in results(stage):
            copy.start()
    for stage in reversed(range(stages)):
        for copy in results(stage):
            copy.wait()


def tap_sums(before, after):
    near = jnp.maximum(RADIUS - before, 0)
    far = jnp.maximum(RADIUS - after, 0)
    missing = near * (near + 1) + far * (far + 1)
    return float((RADIUS + 1) ** 2) - 0.5 * missing.astype(f32)


def partial_kernel(top, *refs, stages, whole_rows):
    sources, out_far, kept = refs[:6], refs[6], refs[7:13]
    rowed, spread, blocks, out, arrived, left = refs[13:]
    design, above, below, passive, elastic, inertia = kept
    peers = out.shape[0]
    piece = design.shape[1] // peers
    narrow = 2048
    span = design.shape[1] // stages

    def early(stage):
        at = pl.ds(stage * span, span)
        return [
            pltpu.make_async_copy(sources[k].at[:, at], kept[k].at[:, at], arrived.at[stage, k])
            for k in range(3)
        ]

    late = [pltpu.make_async_copy(sources[k], kept[k], arrived.at[0, k]) for k in range(3, 6)]
    for stage in range(stages):
        for copy in early(stage):
            copy.start()
    for copy in late:
        copy.start()
    clear_ends(rowed)
    clear_ends(spread)

    def filter_rows(c, none):
        at = cols(c, narrow)
        upper = above[:, at].astype(jnp.int32).astype(f32) * (1.0 / DESIGN_STEPS)
        lower = below[:, at].astype(jnp.int32).astype(f32) * (1.0 / DESIGN_STEPS)
        rowed[:, inner_cols(c, narrow)] = row_filter(upper, design[:, at], lower)
        return none

    for stage in range(stages):
        for copy in early(stage):
            copy.wait()
        first = stage * (span // narrow)
        lax.fori_loop(first, first + span // narrow, filter_rows, 0)
    for copy in late:
        copy.wait()

    taps = band()
    row = top[0] + row_ids(LANES)
    lane = lax.broadcasted_iota(jnp.int32, (8, LANES), 1)
    full = float((RADIUS + 1) ** 2)
    inside = 1.0 / (full * tap_sums(row, whole_rows - 1 - row))
    left_end = full / tap_sums(lane, RADIUS)
    right_end = full / tap_sums(RADIUS, LANES - 1 - lane)

    def scale(c, none):
        at = cols(c, piece)
        first = inside * jnp.where(c == 0, left_end, 1.0)
        last = inside * jnp.where(c == peers - 1, right_end, 1.0)
        weights = jnp.concatenate([first] + [inside] * (piece // LANES - 2) + [last], axis=1)
        tilde = col_filter(rowed[:, padded_cols(c, piece)], taps) * weights
        steep = jnp.tanh(SHARPNESS * (tilde - THRESHOLD))
        solid = passive[:, at] > 0
        density = jnp.where(solid, 1.0, (TANH_HALF + steep) * (0.5 / TANH_HALF))
        slope = jnp.where(solid, 0.0, (1.0 - steep * steep) * (SHARPNESS * 0.5 / TANH_HALF))
        block = (density * density * elastic[:, at] - inertia[:, at]) * (slope * weights)
        spread[:, inner_cols(c, piece)] = block
        return none

    lax.fori_loop(0, peers, scale, 0)

    def send(peer, none):
        block = col_filter(spread[:, padded_cols(peer, piece)], taps)
        blocks[...] = block
        encode(blocks, folded_max(block), [out.at[peer]], narrow)
        pltpu.make_async_copy(out.at[peer], out_far.at[peer], left.at[peer]).start()
        return none

    lax.fori_loop(0, peers, send, 0)
    for peer in range(peers):
        pltpu.make_async_copy(out.at[peer], out_far.at[peer], left.at[peer]).wait()


def sum_kernel(coded, out, *, width):
    peers, piece = coded.shape[0], out.shape[1]
    scales = [wide(decode_scale(coded[peer, :, piece:]), width) for peer in range(peers)]

    def step(c, none):
        at = cols(c, width)
        total = None
        for peer in range(peers):
            term = coded[peer, :, at].astype(jnp.int32).astype(f32) * scales[peer]
            total = term if total is None else total + term
        out[:, at] = total
        return none

    lax.fori_loop(0, piece // width, step, 0)


def back_kernel(above, here, below, out, blocks, *, width):
    piece = here.shape[1]
    zeros = jnp.zeros((8, LANES), f32)

    def step(c, carry):
        largest, squares = carry
        at = cols(c, width)
        block = row_filter(above[:, at], here[:, at], below[:, at])
        blocks[:, at] = block
        return jnp.maximum(largest, folded_max(block)), squares + folded(block * block, jnp.add)

    largest, squares = lax.fori_loop(0, piece // width, step, (zeros, zeros))
    encode(blocks, largest, [out.at[peer] for peer in range(out.shape[0])], width)
    code = scale_code(squares).astype(jnp.int32).astype(i16)
    values = to_i16(squares / decode_scale(code))
    for peer in range(out.shape[0]):
        out[peer, :, piece + LANES : piece + 2 * LANES] = code
        out[peer, :, piece + 2 * LANES :] = values


def squares_kernel(coded, squares):
    piece = coded.shape[2] - 3 * LANES
    total = jnp.zeros((8, LANES), f32)
    for peer in range(coded.shape[0]):
        values = coded[peer, :, piece + 2 * LANES :].astype(jnp.int32).astype(f32)
        total = total + values * decode_scale(coded[peer, :, piece + LANES : piece + 2 * LANES])
    squares[...] = jnp.broadcast_to(total[None], squares.shape)


def result_kernel(coded, squares, out_far, out, left, *, width, elements):
    peers = coded.shape[0]
    piece = out.shape[1] // peers
    mean = jnp.sum(jnp.sum(squares[...], axis=0), keepdims=True) * (1.0 / elements) + EPSILON
    root = lax.rsqrt(mean)
    root = root * (1.5 - 0.5 * mean * root * root)

    def finished(peer):
        at = pl.ds(peer * piece, piece)
        return pltpu.make_async_copy(out.at[:, at], out_far.at[:, at], left.at[peer])

    for peer in range(peers):
        scale = wide(decode_scale(coded[peer, :, piece : piece + LANES]) * root, width)

        def step(c, none):
            block = coded[peer, :, cols(c, width)].astype(jnp.int32).astype(f32) * scale
            out[:, cols(peer * (piece // width) + c, width)] = block
            return none

        lax.fori_loop(0, piece // width, step, 0)
        finished(peer).start()
    for peer in range(peers):
        finished(peer).wait()


def layer(design, passive, state, adjoint, omega_sq, assign):
    slab_rows, width = design.shape
    rows = lax.axis_size("rows")
    peers = lax.axis_size("freq")
    whole_rows = slab_rows * rows
    piece = width // peers
    up = [(i, i + 1) for i in range(rows - 1)]
    down = [(target, source) for source, target in up]
    smem = pl.BlockSpec(memory_space=pltpu.SMEM)

    in_place = pl.BlockSpec(memory_space=pltpu.HBM)
    stages = 4
    element_stages = 8
    field_scratch = [
        pltpu.VMEM(state.shape, state.dtype),
        pltpu.VMEM(adjoint.shape, adjoint.dtype),
        pltpu.SemaphoreType.DMA((stages, 2)),
    ]
    design_scratch = [
        pltpu.VMEM((slab_rows, width), f32),
        pltpu.VMEM((slab_rows, width), i16),
    ]
    edge, code = pl.pallas_call(
        functools.partial(prepare_kernel, width=2048, stages=stages),
        out_shape=[
            jax.ShapeDtypeStruct((4, width), jnp.bfloat16),
            jax.ShapeDtypeStruct((slab_rows, width), i16),
        ],
        in_specs=[in_place] * 3,
        out_specs=vmem(1) + [in_place],
        scratch_shapes=field_scratch[:2]
        + design_scratch
        + [field_scratch[2]]
        + [pltpu.SemaphoreType.DMA((stages,))] * 2,
        compiler_params=params(63),
        cost_estimate=cost(8 * slab_rows * width, 7 * 1024 * 1024),
        name="prepare",
    )(state, adjoint, design)
    edge_below = lax.ppermute(edge, "rows", down)
    code_below = lax.ppermute(code, "rows", down)
    code_above = lax.ppermute(code, "rows", up)

    top = (lax.axis_index("rows") * slab_rows).astype(jnp.int32).reshape(1)

    slab = jax.ShapeDtypeStruct((slab_rows, width), f32)
    elastic, inertia = pl.pallas_call(
        functools.partial(element_kernel, width=2048, stages=element_stages),
        out_shape=[slab, slab],
        in_specs=[smem, smem] + [in_place] * 3,
        out_specs=[in_place, in_place],
        scratch_shapes=field_scratch[:2]
        + [pltpu.VMEM(edge.shape, edge.dtype)]
        + [pltpu.VMEM((slab_rows, width), f32)] * 2
        + [pltpu.SemaphoreType.DMA((element_stages, count)) for count in (3, 2)],
        compiler_params=params(53),
        cost_estimate=cost(80 * slab_rows * width, 8 * 1024 * 1024),
        name="element",
    )(omega_sq, assign, state, adjoint, edge_below)

    coded = jax.ShapeDtypeStruct((peers, slab_rows, piece + LANES), i16)
    operands = (design, code_above, code_below, passive, elastic, inertia)
    sent = pl.pallas_call(
        functools.partial(partial_kernel, stages=stages, whole_rows=whole_rows),
        out_shape=coded,
        in_specs=[smem] + [in_place] * len(operands),
        out_specs=in_place,
        scratch_shapes=[pltpu.VMEM(operand.shape, operand.dtype) for operand in operands]
        + [
            pltpu.VMEM((slab_rows, width + 2 * LANES), f32),
            pltpu.VMEM((slab_rows, width + 2 * LANES), f32),
            pltpu.VMEM((slab_rows, piece), f32),
            pltpu.VMEM(coded.shape, coded.dtype),
            pltpu.SemaphoreType.DMA((stages, len(operands))),
            pltpu.SemaphoreType.DMA((peers,)),
        ],
        compiler_params=params(63),
        cost_estimate=cost(150 * slab_rows * width, 14 * 1024 * 1024),
        name="partial",
    )(top, *operands)

    received = lax.all_to_all(sent, "freq", 0, 0, tiled=True)

    spread = pl.pallas_call(
        functools.partial(sum_kernel, width=1024),
        out_shape=jax.ShapeDtypeStruct((slab_rows, piece), f32),
        in_specs=vmem(1),
        out_specs=vmem(1)[0],
        compiler_params=params(8),
        name="total",
    )(received)
    spread_below = lax.ppermute(spread, "rows", down)
    spread_above = lax.ppermute(spread, "rows", up)

    wide_coded = jax.ShapeDtypeStruct((peers, slab_rows, piece + 3 * LANES), i16)
    result = pl.pallas_call(
        functools.partial(back_kernel, width=1024),
        out_shape=wide_coded,
        in_specs=vmem(3),
        out_specs=vmem(1)[0],
        scratch_shapes=[pltpu.VMEM((slab_rows, piece), f32)],
        compiler_params=params(8),
        name="back",
    )(spread_above, spread, spread_below)

    pieces = lax.all_to_all(result, "freq", 0, 0, tiled=True)

    squares = pl.pallas_call(
        squares_kernel,
        out_shape=jax.ShapeDtypeStruct((rows, 8, LANES), f32),
        in_specs=vmem(1),
        out_specs=vmem(1)[0],
        compiler_params=params(8),
        name="squares",
    )(pieces)
    squares = lax.all_to_all(squares, "rows", 0, 0, tiled=True)

    return pl.pallas_call(
        functools.partial(result_kernel, width=2048, elements=float(whole_rows * width)),
        out_shape=slab,
        in_specs=vmem(2),
        out_specs=in_place,
        scratch_shapes=[pltpu.VMEM((slab_rows, width), f32), pltpu.SemaphoreType.DMA((peers,))],
        compiler_params=params(16),
        name="result",
    )(pieces, squares)


def solution(mesh):
    return jax.shard_map(
        layer,
        mesh=mesh,
        in_specs=(
            P("rows", None),
            P("rows", None),
            P(None, "freq", "rows", None),
            P(None, "freq", "rows", None),
            P(),
            P("freq"),
        ),
        out_specs=P("rows", None),
        check_vma=False,
    )
```

```python
import functools

import jax
import jax.numpy as jnp
from jax import lax
from jax.experimental import pallas as pl
from jax.experimental.pallas import tpu as pltpu
from jax.sharding import PartitionSpec as P


RADIUS = 8
LANES = 128
SHARPNESS = 8.0
THRESHOLD = 0.5
EXPONENT = 3.0
SOFT_FLOOR = 0.001
LOSS = 0.2
EPSILON = 1e-06
TANH_HALF = 0.999329299739067
DESIGN_STEPS = 32767.0
CODE_STEPS = 32700.0

f32 = jnp.float32
i16 = jnp.int16


def params(megabytes):
    return pltpu.CompilerParams(vmem_limit_bytes=megabytes * 1024 * 1024)


def vmem(count):
    return [pl.BlockSpec(memory_space=pltpu.VMEM)] * count


def cost(flops, moved):
    return pl.CostEstimate(flops=flops, bytes_accessed=moved, transcendentals=0)


def cols(index, width):
    return pl.ds(pl.multiple_of(index * width, width), width)


def row_ids(width):
    return lax.broadcasted_iota(jnp.int32, (8, width), 0)


def rows_up(block, count, ids):
    return jnp.where(ids < 8 - count, pltpu.roll(block, 8 - count, 0), 0.0)


def rows_down(block, count, ids):
    return jnp.where(ids >= count, pltpu.roll(block, count, 0), 0.0)


def row_filter(above, here, below):
    ids = row_ids(here.shape[1])
    upper = above - here
    lower = below - here
    for _ in range(2):
        for count in (1, 2, 4):
            upper = upper + rows_up(upper, count, ids)
            lower = lower + rows_down(lower, count, ids)
    total = here
    for count in (1, 2, 4):
        total = total + pltpu.roll(total, count, 0)
    return upper + lower + here + 10.0 * total


def moved(block, count):
    width = block.shape[1]
    return pltpu.roll(block, (width - count) % width, 1)


def band():
    shape = (3 * LANES, LANES)
    source = lax.broadcasted_iota(jnp.int32, shape, 0) - LANES
    target = lax.broadcasted_iota(jnp.int32, shape, 1)
    taps = jnp.maximum(RADIUS + 1 - jnp.abs(source - target), 0)
    return taps.astype(f32).astype(jnp.bfloat16)


def col_filter(window, taps):
    count = window.shape[1] // LANES - 2
    half = count // 2
    tiles = [window[:, i * LANES : (i + 1) * LANES] for i in range(count + 2)]
    stacked = jnp.concatenate(
        [tiles[i + side] for i in range(half + 2) for side in (0, half)], axis=0
    )
    coarse = stacked.astype(jnp.bfloat16)
    fine = (stacked - coarse.astype(f32)).astype(jnp.bfloat16)
    left, here, right = (slice(start, start + 16 * half) for start in (0, 16, 32))

    def product(first, second, weights):
        return jnp.dot(
            jnp.concatenate([first, second], axis=1), weights, preferred_element_type=f32
        )

    near, far = taps[: 2 * LANES], taps[2 * LANES :]
    total = product(coarse[left], coarse[here], near) + product(fine[left], fine[here], near)
    total = total + product(coarse[right], fine[right], jnp.concatenate([far, far], axis=0))
    halves = [
        [total[16 * i + 8 * side : 16 * i + 8 * side + 8] for i in range(half)] for side in (0, 1)
    ]
    return jnp.concatenate(halves[0] + halves[1], axis=1)


def padded_cols(index, width):
    return pl.ds(pl.multiple_of(index * width, LANES), width + 2 * LANES)


def inner_cols(index, width):
    return pl.ds(pl.multiple_of(index * width + LANES, LANES), width)


def clear_ends(ref):
    count = ref.shape[1]
    ref[:, :LANES] = jnp.zeros((8, LANES), f32)
    ref[:, count - LANES :] = jnp.zeros((8, LANES), f32)


def decode_scale(code):
    return jnp.exp2(code.astype(jnp.int32).astype(f32) * (1.0 / 256)) * (1.0 / CODE_STEPS)


def scale_code(largest):
    level = jnp.floor(jnp.log(jnp.maximum(largest, 1e-30)) * (256 * 1.4426950408889634)) + 1.0
    return level


def to_i16(values):
    return jnp.round(values).astype(jnp.int32).astype(i16)


def wide(tile, width):
    return jnp.concatenate([tile] * (width // LANES), axis=1)


def folded(block, join):
    parts = [block[:, i : i + LANES] for i in range(0, block.shape[1], LANES)]
    while len(parts) > 1:
        parts = [join(a, b) for a, b in zip(parts[::2], parts[1::2])]
    return parts[0]


def folded_max(block):
    return folded(jnp.abs(block), jnp.maximum)


def encode(source, largest, targets, width):
    count = source.shape[1]
    code = scale_code(largest).astype(jnp.int32).astype(i16)
    for target in targets:
        target[:, count : count + LANES] = code
    inverse = wide(1.0 / decode_scale(code), width)

    def step(c, none):
        values = to_i16(source[:, cols(c, width)] * inverse)
        for target in targets:
            target[:, cols(c, width)] = values
        return none

    lax.fori_loop(0, count // width, step, 0)


def field_copies(sources, kept, arrived, stage, span):
    at = pl.ds(stage * span, span)
    whole = lambda ref: (slice(None),) * (len(ref.shape) - 1) + (at,)
    return [
        pltpu.make_async_copy(source.at[whole(source)], target.at[whole(target)], arrived.at[stage, place])
        for place, (source, target) in enumerate(zip(sources, kept))
    ]


def prepare_kernel(
    state_far,
    adjoint_far,
    design_far,
    edge,
    code_far,
    state,
    adjoint,
    design,
    code,
    arrived,
    design_arrived,
    left,
    *,
    width,
    stages,
):
    span = edge.shape[1] // stages
    steps = span // width
    sent = lax.broadcasted_iota(jnp.int32, (4, width), 0)

    def copies(stage):
        at = pl.ds(stage * span, span)
        return [
            pltpu.make_async_copy(source.at[:, :, 0:2, at], target.at[:, :, :, at], arrived.at[stage, place])
            for place, (source, target) in enumerate(((state_far, state), (adjoint_far, adjoint)))
        ]

    def load(stage):
        at = pl.ds(stage * span, span)
        return pltpu.make_async_copy(design_far.at[:, at], design.at[:, at], design_arrived.at[stage])

    def save(stage):
        at = pl.ds(stage * span, span)
        return pltpu.make_async_copy(code.at[:, at], code_far.at[:, at], left.at[stage])

    for stage in range(stages):
        for copy in copies(stage):
            copy.start()
    for stage in range(stages):
        load(stage).start()

    for stage in range(stages):
        for copy in copies(stage):
            copy.wait()

        def pick_rows(c, none):
            at = cols(stage * steps + c, width)
            fields = [state[0, 0, :, at], state[1, 0, :, at], adjoint[0, 0, :, at], adjoint[1, 0, :, at]]
            picked = jnp.zeros((4, width), f32)
            for place, field in enumerate(fields):
                row = jnp.broadcast_to(field.astype(f32)[:1], picked.shape)
                picked = jnp.where(sent == place, row, picked)
            edge[:, at] = picked.astype(jnp.bfloat16)
            return none

        lax.fori_loop(0, steps, pick_rows, 0)

    for stage in range(stages):
        load(stage).wait()

        def encode_rows(c, none):
            at = cols(stage * steps + c, width)
            code[:, at] = to_i16(design[:, at] * DESIGN_STEPS)
            return none

        lax.fori_loop(0, steps, encode_rows, 0)
        save(stage).start()
    for stage in range(stages):
        save(stage).wait()


def element_kernel(
    omega_sq,
    assign,
    state_far,
    adjoint_far,
    edge_far,
    elastic_far,
    inertia_far,
    state,
    adjoint,
    edge,
    elastic,
    inertia,
    arrived,
    left,
    *,
    width,
    stages,
):
    omega = omega_sq[assign[0]]
    ids = row_ids(width)
    span = elastic.shape[1] // stages
    count = span // width
    copies = functools.partial(
        field_copies, (state_far, adjoint_far, edge_far), (state, adjoint, edge), arrived, span=span
    )
    for stage in reversed(range(stages)):
        for copy in copies(stage):
            copy.start()

    def shifted(block, carry):
        return moved(jnp.concatenate([block, carry], axis=1), 1)[:, :width]

    def step(stage, c, carries):
        at = cols((stage + 1) * count - 1 - c, width)
        edges = edge[:, at].astype(f32)
        fields = [state[0, 0, :, at], state[1, 0, :, at], adjoint[0, 0, :, at], adjoint[1, 0, :, at]]
        kept = []
        parts = []
        for place, field in enumerate(fields):
            here = field.astype(f32)
            row = jnp.broadcast_to(edges[place : place + 1], here.shape)
            below = jnp.where(ids == 7, row, pltpu.roll(here, 7, 0))
            plus = here + below
            minus = here - below
            kept += [plus[:, :LANES], minus[:, :LANES]]
            plus_next = shifted(plus, carries[2 * place])
            minus_next = shifted(minus, carries[2 * place + 1])
            parts.append((plus + plus_next, plus - plus_next, minus + minus_next, minus - minus_next))
        sr, si, ar, ai = parts
        same = [ar[k] * sr[k] - ai[k] * si[k] for k in range(4)]
        cross = [ar[k] * si[k] + ai[k] * sr[k] for k in range(1, 4)]
        same_mixed = same[1] + same[2]
        cross_mixed = cross[0] + cross[1]
        stiff = 1.5 * (same_mixed - LOSS * cross_mixed) + (same[3] - LOSS * cross[2])
        mass = 2.25 * same[0] + 0.75 * same_mixed + 0.25 * same[3]
        elastic[:, at] = stiff * (EXPONENT * (1.0 - SOFT_FLOOR) / 6.0)
        inertia[:, at] = mass * (omega * (1.0 / 36.0))
        return tuple(kept)

    def results(stage):
        at = pl.ds(stage * span, span)
        return [
            pltpu.make_async_copy(source.at[:, at], target.at[:, at], left.at[stage, place])
            for place, (source, target) in enumerate(((elastic, elastic_far), (inertia, inertia_far)))
        ]

    carries = (jnp.zeros((8, LANES), f32),) * 8
    for stage in reversed(range(stages)):
        for copy in copies(stage):
            copy.wait()
        carries = lax.fori_loop(0, count, functools.partial(step, stage), carries, unroll=2)
        for copy in results(stage):
            copy.start()
    for stage in reversed(range(stages)):
        for copy in results(stage):
            copy.wait()


def tap_sums(before, after):
    near = jnp.maximum(RADIUS - before, 0)
    far = jnp.maximum(RADIUS - after, 0)
    missing = near * (near + 1) + far * (far + 1)
    return float((RADIUS + 1) ** 2) - 0.5 * missing.astype(f32)


def partial_kernel(top, *refs, stages, whole_rows):
    sources, out_far, kept = refs[:6], refs[6], refs[7:13]
    rowed, spread, blocks, out, arrived, left = refs[13:]
    design, above, below, passive, elastic, inertia = kept
    peers = out.shape[0]
    piece = design.shape[1] // peers
    narrow = 2048
    span = design.shape[1] // stages

    def early(stage):
        at = pl.ds(stage * span, span)
        return [
            pltpu.make_async_copy(sources[k].at[:, at], kept[k].at[:, at], arrived.at[stage, k])
            for k in range(3)
        ]

    late = [pltpu.make_async_copy(sources[k], kept[k], arrived.at[0, k]) for k in range(3, 6)]
    for stage in range(stages):
        for copy in early(stage):
            copy.start()
    for copy in late:
        copy.start()
    clear_ends(rowed)
    clear_ends(spread)

    def filter_rows(c, none):
        at = cols(c, narrow)
        upper = above[:, at].astype(jnp.int32).astype(f32) * (1.0 / DESIGN_STEPS)
        lower = below[:, at].astype(jnp.int32).astype(f32) * (1.0 / DESIGN_STEPS)
        rowed[:, inner_cols(c, narrow)] = row_filter(upper, design[:, at], lower)
        return none

    for stage in range(stages):
        for copy in early(stage):
            copy.wait()
        first = stage * (span // narrow)
        lax.fori_loop(first, first + span // narrow, filter_rows, 0)
    for copy in late:
        copy.wait()

    taps = band()
    row = top[0] + row_ids(LANES)
    lane = lax.broadcasted_iota(jnp.int32, (8, LANES), 1)
    full = float((RADIUS + 1) ** 2)
    inside = 1.0 / (full * tap_sums(row, whole_rows - 1 - row))
    left_end = full / tap_sums(lane, RADIUS)
    right_end = full / tap_sums(RADIUS, LANES - 1 - lane)

    def scale(c, none):
        at = cols(c, piece)
        first = inside * jnp.where(c == 0, left_end, 1.0)
        last = inside * jnp.where(c == peers - 1, right_end, 1.0)
        weights = jnp.concatenate([first] + [inside] * (piece // LANES - 2) + [last], axis=1)
        tilde = col_filter(rowed[:, padded_cols(c, piece)], taps) * weights
        steep = jnp.tanh(SHARPNESS * (tilde - THRESHOLD))
        solid = passive[:, at] > 0
        density = jnp.where(solid, 1.0, (TANH_HALF + steep) * (0.5 / TANH_HALF))
        slope = jnp.where(solid, 0.0, (1.0 - steep * steep) * (SHARPNESS * 0.5 / TANH_HALF))
        block = (density * density * elastic[:, at] - inertia[:, at]) * (slope * weights)
        spread[:, inner_cols(c, piece)] = block
        return none

    lax.fori_loop(0, peers, scale, 0)

    def send(peer, none):
        block = col_filter(spread[:, padded_cols(peer, piece)], taps)
        blocks[...] = block
        encode(blocks, folded_max(block), [out.at[peer]], narrow)
        pltpu.make_async_copy(out.at[peer], out_far.at[peer], left.at[peer]).start()
        return none

    lax.fori_loop(0, peers, send, 0)
    for peer in range(peers):
        pltpu.make_async_copy(out.at[peer], out_far.at[peer], left.at[peer]).wait()


def sum_kernel(coded, out, *, width):
    peers, piece = coded.shape[0], out.shape[1]
    scales = [wide(decode_scale(coded[peer, :, piece:]), width) for peer in range(peers)]

    def step(c, none):
        at = cols(c, width)
        total = None
        for peer in range(peers):
            term = coded[peer, :, at].astype(jnp.int32).astype(f32) * scales[peer]
            total = term if total is None else total + term
        out[:, at] = total
        return none

    lax.fori_loop(0, piece // width, step, 0)


def back_kernel(above, here, below, out, blocks, *, width):
    piece = here.shape[1]
    zeros = jnp.zeros((8, LANES), f32)

    def step(c, carry):
        largest, squares = carry
        at = cols(c, width)
        block = row_filter(above[:, at], here[:, at], below[:, at])
        blocks[:, at] = block
        return jnp.maximum(largest, folded_max(block)), squares + folded(block * block, jnp.add)

    largest, squares = lax.fori_loop(0, piece // width, step, (zeros, zeros))
    encode(blocks, largest, [out.at[peer] for peer in range(out.shape[0])], width)
    code = scale_code(squares).astype(jnp.int32).astype(i16)
    values = to_i16(squares / decode_scale(code))
    for peer in range(out.shape[0]):
        out[peer, :, piece + LANES : piece + 2 * LANES] = code
        out[peer, :, piece + 2 * LANES :] = values


def squares_kernel(coded, squares):
    piece = coded.shape[2] - 3 * LANES
    total = jnp.zeros((8, LANES), f32)
    for peer in range(coded.shape[0]):
        values = coded[peer, :, piece + 2 * LANES :].astype(jnp.int32).astype(f32)
        total = total + values * decode_scale(coded[peer, :, piece + LANES : piece + 2 * LANES])
    squares[...] = jnp.broadcast_to(total[None], squares.shape)


def result_kernel(coded, squares, out_far, out, left, *, width, elements):
    peers = coded.shape[0]
    piece = out.shape[1] // peers
    mean = jnp.sum(jnp.sum(squares[...], axis=0), keepdims=True) * (1.0 / elements) + EPSILON
    root = lax.rsqrt(mean)
    root = root * (1.5 - 0.5 * mean * root * root)

    def finished(peer):
        at = pl.ds(peer * piece, piece)
        return pltpu.make_async_copy(out.at[:, at], out_far.at[:, at], left.at[peer])

    for peer in range(peers):
        scale = wide(decode_scale(coded[peer, :, piece : piece + LANES]) * root, width)

        def step(c, none):
            block = coded[peer, :, cols(c, width)].astype(jnp.int32).astype(f32) * scale
            out[:, cols(peer * (piece // width) + c, width)] = block
            return none

        lax.fori_loop(0, piece // width, step, 0)
        finished(peer).start()
    for peer in range(peers):
        finished(peer).wait()


def layer(design, passive, state, adjoint, omega_sq, assign):
    slab_rows, width = design.shape
    rows = lax.axis_size("rows")
    peers = lax.axis_size("freq")
    whole_rows = slab_rows * rows
    piece = width // peers
    up = [(i, i + 1) for i in range(rows - 1)]
    down = [(target, source) for source, target in up]
    smem = pl.BlockSpec(memory_space=pltpu.SMEM)

    in_place = pl.BlockSpec(memory_space=pltpu.HBM)
    stages = 4
    element_stages = 8
    field_scratch = [
        pltpu.VMEM(state.shape, state.dtype),
        pltpu.VMEM(adjoint.shape, adjoint.dtype),
        pltpu.SemaphoreType.DMA((stages, 2)),
    ]
    design_scratch = [
        pltpu.VMEM((slab_rows, width), f32),
        pltpu.VMEM((slab_rows, width), i16),
    ]
    edge, code = pl.pallas_call(
        functools.partial(prepare_kernel, width=2048, stages=stages),
        out_shape=[
            jax.ShapeDtypeStruct((4, width), jnp.bfloat16),
            jax.ShapeDtypeStruct((slab_rows, width), i16),
        ],
        in_specs=[in_place] * 3,
        out_specs=vmem(1) + [in_place],
        scratch_shapes=[
            pltpu.VMEM((2, 1, 2, width), state.dtype),
            pltpu.VMEM((2, 1, 2, width), adjoint.dtype),
        ]
        + design_scratch
        + [field_scratch[2]]
        + [pltpu.SemaphoreType.DMA((stages,))] * 2,
        compiler_params=params(63),
        cost_estimate=cost(8 * slab_rows * width, 7 * 1024 * 1024),
        name="prepare",
    )(state, adjoint, design)
    edge_below = lax.ppermute(edge, "rows", down)
    code_above = lax.ppermute(code, "rows", up)
    code_below = lax.ppermute(code, "rows", down)

    top = (lax.axis_index("rows") * slab_rows).astype(jnp.int32).reshape(1)

    slab = jax.ShapeDtypeStruct((slab_rows, width), f32)
    elastic, inertia = pl.pallas_call(
        functools.partial(element_kernel, width=2048, stages=element_stages),
        out_shape=[slab, slab],
        in_specs=[smem, smem] + [in_place] * 3,
        out_specs=[in_place, in_place],
        scratch_shapes=field_scratch[:2]
        + [pltpu.VMEM(edge.shape, edge.dtype)]
        + [pltpu.VMEM((slab_rows, width), f32)] * 2
        + [pltpu.SemaphoreType.DMA((element_stages, count)) for count in (3, 2)],
        compiler_params=params(53),
        cost_estimate=cost(80 * slab_rows * width, 8 * 1024 * 1024),
        name="element",
    )(omega_sq, assign, state, adjoint, edge_below)

    coded = jax.ShapeDtypeStruct((peers, slab_rows, piece + LANES), i16)
    operands = (design, code_above, code_below, passive, elastic, inertia)
    sent = pl.pallas_call(
        functools.partial(partial_kernel, stages=stages, whole_rows=whole_rows),
        out_shape=coded,
        in_specs=[smem] + [in_place] * len(operands),
        out_specs=in_place,
        scratch_shapes=[pltpu.VMEM(operand.shape, operand.dtype) for operand in operands]
        + [
            pltpu.VMEM((slab_rows, width + 2 * LANES), f32),
            pltpu.VMEM((slab_rows, width + 2 * LANES), f32),
            pltpu.VMEM((slab_rows, piece), f32),
            pltpu.VMEM(coded.shape, coded.dtype),
            pltpu.SemaphoreType.DMA((stages, len(operands))),
            pltpu.SemaphoreType.DMA((peers,)),
        ],
        compiler_params=params(63),
        cost_estimate=cost(150 * slab_rows * width, 14 * 1024 * 1024),
        name="partial",
    )(top, *operands)

    received = lax.all_to_all(sent, "freq", 0, 0, tiled=True)

    spread = pl.pallas_call(
        functools.partial(sum_kernel, width=1024),
        out_shape=jax.ShapeDtypeStruct((slab_rows, piece), f32),
        in_specs=vmem(1),
        out_specs=vmem(1)[0],
        compiler_params=params(8),
        name="total",
    )(received)
    spread_below = lax.ppermute(spread, "rows", down)
    spread_above = lax.ppermute(spread, "rows", up)

    wide_coded = jax.ShapeDtypeStruct((peers, slab_rows, piece + 3 * LANES), i16)
    result = pl.pallas_call(
        functools.partial(back_kernel, width=1024),
        out_shape=wide_coded,
        in_specs=vmem(3),
        out_specs=vmem(1)[0],
        scratch_shapes=[pltpu.VMEM((slab_rows, piece), f32)],
        compiler_params=params(8),
        name="back",
    )(spread_above, spread, spread_below)

    pieces = lax.all_to_all(result, "freq", 0, 0, tiled=True)

    squares = pl.pallas_call(
        squares_kernel,
        out_shape=jax.ShapeDtypeStruct((rows, 8, LANES), f32),
        in_specs=vmem(1),
        out_specs=vmem(1)[0],
        compiler_params=params(8),
        name="squares",
    )(pieces)
    squares = lax.all_to_all(squares, "rows", 0, 0, tiled=True)

    return pl.pallas_call(
        functools.partial(result_kernel, width=2048, elements=float(whole_rows * width)),
        out_shape=slab,
        in_specs=vmem(2),
        out_specs=in_place,
        scratch_shapes=[pltpu.VMEM((slab_rows, width), f32), pltpu.SemaphoreType.DMA((peers,))],
        compiler_params=params(16),
        name="result",
    )(pieces, squares)


def solution(mesh):
    return jax.shard_map(
        layer,
        mesh=mesh,
        in_specs=(
            P("rows", None),
            P("rows", None),
            P(None, "freq", "rows", None),
            P(None, "freq", "rows", None),
            P(),
            P("freq"),
        ),
        out_specs=P("rows", None),
        check_vma=False,
    )
```

```python
import functools

import jax
import jax.numpy as jnp
from jax import lax
from jax.experimental import pallas as pl
from jax.experimental.pallas import tpu as pltpu
from jax.sharding import PartitionSpec as P


RADIUS = 8
LANES = 128
SHARPNESS = 8.0
THRESHOLD = 0.5
EXPONENT = 3.0
SOFT_FLOOR = 0.001
LOSS = 0.2
EPSILON = 1e-06
TANH_HALF = 0.999329299739067
DESIGN_STEPS = 32767.0
CODE_STEPS = 32700.0

f32 = jnp.float32
i16 = jnp.int16


def params(megabytes):
    return pltpu.CompilerParams(vmem_limit_bytes=megabytes * 1024 * 1024)


def vmem(count):
    return [pl.BlockSpec(memory_space=pltpu.VMEM)] * count


def cost(flops, moved):
    return pl.CostEstimate(flops=flops, bytes_accessed=moved, transcendentals=0)


def cols(index, width):
    return pl.ds(pl.multiple_of(index * width, width), width)


def row_ids(width):
    return lax.broadcasted_iota(jnp.int32, (8, width), 0)


def rows_up(block, count, ids):
    return jnp.where(ids < 8 - count, pltpu.roll(block, 8 - count, 0), 0.0)


def rows_down(block, count, ids):
    return jnp.where(ids >= count, pltpu.roll(block, count, 0), 0.0)


def row_filter(above, here, below):
    ids = row_ids(here.shape[1])
    upper = above - here
    lower = below - here
    for _ in range(2):
        for count in (1, 2, 4):
            upper = upper + rows_up(upper, count, ids)
            lower = lower + rows_down(lower, count, ids)
    total = here
    for count in (1, 2, 4):
        total = total + pltpu.roll(total, count, 0)
    return upper + lower + here + 10.0 * total


def moved(block, count):
    width = block.shape[1]
    return pltpu.roll(block, (width - count) % width, 1)


def band():
    shape = (3 * LANES, LANES)
    source = lax.broadcasted_iota(jnp.int32, shape, 0) - LANES
    target = lax.broadcasted_iota(jnp.int32, shape, 1)
    taps = jnp.maximum(RADIUS + 1 - jnp.abs(source - target), 0)
    return taps.astype(f32).astype(jnp.bfloat16)


def col_filter(window, taps):
    count = window.shape[1] // LANES - 2
    half = count // 2
    tiles = [window[:, i * LANES : (i + 1) * LANES] for i in range(count + 2)]
    stacked = jnp.concatenate(
        [tiles[i + side] for i in range(half + 2) for side in (0, half)], axis=0
    )
    coarse = stacked.astype(jnp.bfloat16)
    fine = (stacked - coarse.astype(f32)).astype(jnp.bfloat16)
    left, here, right = (slice(start, start + 16 * half) for start in (0, 16, 32))

    def product(first, second, weights):
        return jnp.dot(
            jnp.concatenate([first, second], axis=1), weights, preferred_element_type=f32
        )

    near, far = taps[: 2 * LANES], taps[2 * LANES :]
    total = product(coarse[left], coarse[here], near) + product(fine[left], fine[here], near)
    total = total + product(coarse[right], fine[right], jnp.concatenate([far, far], axis=0))
    halves = [
        [total[16 * i + 8 * side : 16 * i + 8 * side + 8] for i in range(half)] for side in (0, 1)
    ]
    return jnp.concatenate(halves[0] + halves[1], axis=1)


def padded_cols(index, width):
    return pl.ds(pl.multiple_of(index * width, LANES), width + 2 * LANES)


def inner_cols(index, width):
    return pl.ds(pl.multiple_of(index * width + LANES, LANES), width)


def clear_ends(ref):
    count = ref.shape[1]
    ref[:, :LANES] = jnp.zeros((8, LANES), f32)
    ref[:, count - LANES :] = jnp.zeros((8, LANES), f32)


def decode_scale(code):
    return jnp.exp2(code.astype(jnp.int32).astype(f32) * (1.0 / 256)) * (1.0 / CODE_STEPS)


def scale_code(largest):
    level = jnp.floor(jnp.log(jnp.maximum(largest, 1e-30)) * (256 * 1.4426950408889634)) + 1.0
    return level


def to_i16(values):
    return jnp.round(values).astype(jnp.int32).astype(i16)


def wide(tile, width):
    return jnp.concatenate([tile] * (width // LANES), axis=1)


def folded(block, join):
    parts = [block[:, i : i + LANES] for i in range(0, block.shape[1], LANES)]
    while len(parts) > 1:
        parts = [join(a, b) for a, b in zip(parts[::2], parts[1::2])]
    return parts[0]


def folded_max(block):
    return folded(jnp.abs(block), jnp.maximum)


def encode(source, largest, targets, width):
    count = source.shape[1]
    code = scale_code(largest).astype(jnp.int32).astype(i16)
    for target in targets:
        target[:, count : count + LANES] = code
    inverse = wide(1.0 / decode_scale(code), width)

    def step(c, none):
        values = to_i16(source[:, cols(c, width)] * inverse)
        for target in targets:
            target[:, cols(c, width)] = values
        return none

    lax.fori_loop(0, count // width, step, 0)


def field_copies(sources, kept, arrived, stage, span):
    at = pl.ds(stage * span, span)
    whole = lambda ref: (slice(None),) * (len(ref.shape) - 1) + (at,)
    return [
        pltpu.make_async_copy(source.at[whole(source)], target.at[whole(target)], arrived.at[stage, place])
        for place, (source, target) in enumerate(zip(sources, kept))
    ]


def edge_kernel(state_far, adjoint_far, edge, state, adjoint, arrived, *, width, stages):
    span = edge.shape[1] // stages
    steps = span // width
    sent = lax.broadcasted_iota(jnp.int32, (4, width), 0)

    def copies(stage):
        at = pl.ds(stage * span, span)
        return [
            pltpu.make_async_copy(source.at[:, :, 0:2, at], target.at[:, :, :, at], arrived.at[stage, place])
            for place, (source, target) in enumerate(((state_far, state), (adjoint_far, adjoint)))
        ]

    for stage in range(stages):
        for copy in copies(stage):
            copy.start()
    for stage in range(stages):
        for copy in copies(stage):
            copy.wait()

        def pick_rows(c, none):
            at = cols(stage * steps + c, width)
            fields = [state[0, 0, :, at], state[1, 0, :, at], adjoint[0, 0, :, at], adjoint[1, 0, :, at]]
            picked = jnp.zeros((4, width), f32)
            for place, field in enumerate(fields):
                row = jnp.broadcast_to(field.astype(f32)[:1], picked.shape)
                picked = jnp.where(sent == place, row, picked)
            edge[:, at] = picked.astype(jnp.bfloat16)
            return none

        lax.fori_loop(0, steps, pick_rows, 0)


def code_kernel(design_far, code_far, design, code, arrived, left, *, width, stages):
    span = design.shape[1] // stages
    steps = span // width

    def load(stage):
        at = pl.ds(stage * span, span)
        return pltpu.make_async_copy(design_far.at[:, at], design.at[:, at], arrived.at[stage])

    def save(stage):
        at = pl.ds(stage * span, span)
        return pltpu.make_async_copy(code.at[:, at], code_far.at[:, at], left.at[stage])

    for stage in range(stages):
        load(stage).start()
    for stage in range(stages):
        load(stage).wait()

        def encode_rows(c, none):
            at = cols(stage * steps + c, width)
            code[:, at] = to_i16(design[:, at] * DESIGN_STEPS)
            return none

        lax.fori_loop(0, steps, encode_rows, 0)
        save(stage).start()
    for stage in range(stages):
        save(stage).wait()


def element_kernel(
    omega_sq,
    assign,
    state_far,
    adjoint_far,
    edge_far,
    elastic_far,
    inertia_far,
    state,
    adjoint,
    edge,
    elastic,
    inertia,
    arrived,
    left,
    *,
    width,
    stages,
):
    omega = omega_sq[assign[0]]
    ids = row_ids(width)
    span = elastic.shape[1] // stages
    count = span // width
    copies = functools.partial(
        field_copies, (state_far, adjoint_far, edge_far), (state, adjoint, edge), arrived, span=span
    )
    for stage in reversed(range(stages)):
        for copy in copies(stage):
            copy.start()

    def shifted(block, carry):
        return moved(jnp.concatenate([block, carry], axis=1), 1)[:, :width]

    def step(stage, c, carries):
        at = cols((stage + 1) * count - 1 - c, width)
        edges = edge[:, at].astype(f32)
        fields = [state[0, 0, :, at], state[1, 0, :, at], adjoint[0, 0, :, at], adjoint[1, 0, :, at]]
        kept = []
        parts = []
        for place, field in enumerate(fields):
            here = field.astype(f32)
            row = jnp.broadcast_to(edges[place : place + 1], here.shape)
            below = jnp.where(ids == 7, row, pltpu.roll(here, 7, 0))
            plus = here + below
            minus = here - below
            kept += [plus[:, :LANES], minus[:, :LANES]]
            plus_next = shifted(plus, carries[2 * place])
            minus_next = shifted(minus, carries[2 * place + 1])
            parts.append((plus + plus_next, plus - plus_next, minus + minus_next, minus - minus_next))
        sr, si, ar, ai = parts
        same = [ar[k] * sr[k] - ai[k] * si[k] for k in range(4)]
        cross = [ar[k] * si[k] + ai[k] * sr[k] for k in range(1, 4)]
        same_mixed = same[1] + same[2]
        cross_mixed = cross[0] + cross[1]
        stiff = 1.5 * (same_mixed - LOSS * cross_mixed) + (same[3] - LOSS * cross[2])
        mass = 2.25 * same[0] + 0.75 * same_mixed + 0.25 * same[3]
        elastic[:, at] = stiff * (EXPONENT * (1.0 - SOFT_FLOOR) / 6.0)
        inertia[:, at] = mass * (omega * (1.0 / 36.0))
        return tuple(kept)

    def results(stage):
        at = pl.ds(stage * span, span)
        return [
            pltpu.make_async_copy(source.at[:, at], target.at[:, at], left.at[stage, place])
            for place, (source, target) in enumerate(((elastic, elastic_far), (inertia, inertia_far)))
        ]

    carries = (jnp.zeros((8, LANES), f32),) * 8
    for stage in reversed(range(stages)):
        for copy in copies(stage):
            copy.wait()
        carries = lax.fori_loop(0, count, functools.partial(step, stage), carries, unroll=2)
        for copy in results(stage):
            copy.start()
    for stage in reversed(range(stages)):
        for copy in results(stage):
            copy.wait()


def tap_sums(before, after):
    near = jnp.maximum(RADIUS - before, 0)
    far = jnp.maximum(RADIUS - after, 0)
    missing = near * (near + 1) + far * (far + 1)
    return float((RADIUS + 1) ** 2) - 0.5 * missing.astype(f32)


def partial_kernel(top, *refs, stages, whole_rows):
    sources, out_far, kept = refs[:6], refs[6], refs[7:13]
    rowed, spread, blocks, out, arrived, left = refs[13:]
    design, above, below, passive, elastic, inertia = kept
    peers = out.shape[0]
    piece = design.shape[1] // peers
    narrow = 2048
    span = design.shape[1] // stages

    def early(stage):
        at = pl.ds(stage * span, span)
        return [
            pltpu.make_async_copy(sources[k].at[:, at], kept[k].at[:, at], arrived.at[stage, k])
            for k in range(3)
        ]

    late = [pltpu.make_async_copy(sources[k], kept[k], arrived.at[0, k]) for k in range(3, 6)]
    for stage in range(stages):
        for copy in early(stage):
            copy.start()
    for copy in late:
        copy.start()
    clear_ends(rowed)
    clear_ends(spread)

    def filter_rows(c, none):
        at = cols(c, narrow)
        upper = above[:, at].astype(jnp.int32).astype(f32) * (1.0 / DESIGN_STEPS)
        lower = below[:, at].astype(jnp.int32).astype(f32) * (1.0 / DESIGN_STEPS)
        rowed[:, inner_cols(c, narrow)] = row_filter(upper, design[:, at], lower)
        return none

    for stage in range(stages):
        for copy in early(stage):
            copy.wait()
        first = stage * (span // narrow)
        lax.fori_loop(first, first + span // narrow, filter_rows, 0)
    for copy in late:
        copy.wait()

    taps = band()
    row = top[0] + row_ids(LANES)
    lane = lax.broadcasted_iota(jnp.int32, (8, LANES), 1)
    full = float((RADIUS + 1) ** 2)
    inside = 1.0 / (full * tap_sums(row, whole_rows - 1 - row))
    left_end = full / tap_sums(lane, RADIUS)
    right_end = full / tap_sums(RADIUS, LANES - 1 - lane)

    def scale(c, none):
        at = cols(c, piece)
        first = inside * jnp.where(c == 0, left_end, 1.0)
        last = inside * jnp.where(c == peers - 1, right_end, 1.0)
        weights = jnp.concatenate([first] + [inside] * (piece // LANES - 2) + [last], axis=1)
        tilde = col_filter(rowed[:, padded_cols(c, piece)], taps) * weights
        steep = jnp.tanh(SHARPNESS * (tilde - THRESHOLD))
        solid = passive[:, at] > 0
        density = jnp.where(solid, 1.0, (TANH_HALF + steep) * (0.5 / TANH_HALF))
        slope = jnp.where(solid, 0.0, (1.0 - steep * steep) * (SHARPNESS * 0.5 / TANH_HALF))
        block = (density * density * elastic[:, at] - inertia[:, at]) * (slope * weights)
        spread[:, inner_cols(c, piece)] = block
        return none

    lax.fori_loop(0, peers, scale, 0)

    def send(peer, none):
        block = col_filter(spread[:, padded_cols(peer, piece)], taps)
        blocks[...] = block
        encode(blocks, folded_max(block), [out.at[peer]], narrow)
        pltpu.make_async_copy(out.at[peer], out_far.at[peer], left.at[peer]).start()
        return none

    lax.fori_loop(0, peers, send, 0)
    for peer in range(peers):
        pltpu.make_async_copy(out.at[peer], out_far.at[peer], left.at[peer]).wait()


def sum_kernel(coded, out, sent, *, width):
    peers, piece = coded.shape[0], out.shape[1]
    scales = [wide(decode_scale(coded[peer, :, piece:]), width) for peer in range(peers)]

    def step(c, largest):
        at = cols(c, width)
        total = None
        for peer in range(peers):
            term = coded[peer, :, at].astype(jnp.int32).astype(f32) * scales[peer]
            total = term if total is None else total + term
        out[:, at] = total
        return jnp.maximum(largest, folded_max(total))

    largest = lax.fori_loop(0, piece // width, step, jnp.zeros((8, LANES), f32))
    encode(out, largest, [sent], width)


def back_kernel(above, here, below, out, blocks, *, width):
    piece = here.shape[1]
    zeros = jnp.zeros((8, LANES), f32)
    above_scale, below_scale = (
        wide(decode_scale(ref[:, piece:]), width) for ref in (above, below)
    )

    def step(c, carry):
        largest, squares = carry
        at = cols(c, width)
        upper = above[:, at].astype(jnp.int32).astype(f32) * above_scale
        lower = below[:, at].astype(jnp.int32).astype(f32) * below_scale
        block = row_filter(upper, here[:, at], lower)
        blocks[:, at] = block
        return jnp.maximum(largest, folded_max(block)), squares + folded(block * block, jnp.add)

    largest, squares = lax.fori_loop(0, piece // width, step, (zeros, zeros))
    encode(blocks, largest, [out.at[peer] for peer in range(out.shape[0])], width)
    code = scale_code(squares).astype(jnp.int32).astype(i16)
    values = to_i16(squares / decode_scale(code))
    for peer in range(out.shape[0]):
        out[peer, :, piece + LANES : piece + 2 * LANES] = code
        out[peer, :, piece + 2 * LANES :] = values


def squares_kernel(coded, squares):
    piece = coded.shape[2] - 3 * LANES
    total = jnp.zeros((8, LANES), f32)
    for peer in range(coded.shape[0]):
        values = coded[peer, :, piece + 2 * LANES :].astype(jnp.int32).astype(f32)
        total = total + values * decode_scale(coded[peer, :, piece + LANES : piece + 2 * LANES])
    squares[...] = jnp.broadcast_to(total[None], squares.shape)


def result_kernel(coded, squares, out_far, out, left, *, width, elements):
    peers = coded.shape[0]
    piece = out.shape[1] // peers
    mean = jnp.sum(jnp.sum(squares[...], axis=0), keepdims=True) * (1.0 / elements) + EPSILON
    root = lax.rsqrt(mean)
    root = root * (1.5 - 0.5 * mean * root * root)

    def finished(peer):
        at = pl.ds(peer * piece, piece)
        return pltpu.make_async_copy(out.at[:, at], out_far.at[:, at], left.at[peer])

    for peer in range(peers):
        scale = wide(decode_scale(coded[peer, :, piece : piece + LANES]) * root, width)

        def step(c, none):
            block = coded[peer, :, cols(c, width)].astype(jnp.int32).astype(f32) * scale
            out[:, cols(peer * (piece // width) + c, width)] = block
            return none

        lax.fori_loop(0, piece // width, step, 0)
        finished(peer).start()
    for peer in range(peers):
        finished(peer).wait()


def layer(design, passive, state, adjoint, omega_sq, assign):
    slab_rows, width = design.shape
    rows = lax.axis_size("rows")
    peers = lax.axis_size("freq")
    whole_rows = slab_rows * rows
    piece = width // peers
    up = [(i, i + 1) for i in range(rows - 1)]
    down = [(target, source) for source, target in up]
    smem = pl.BlockSpec(memory_space=pltpu.SMEM)

    in_place = pl.BlockSpec(memory_space=pltpu.HBM)
    stages = 4
    element_stages = 8
    field_scratch = [
        pltpu.VMEM(state.shape, state.dtype),
        pltpu.VMEM(adjoint.shape, adjoint.dtype),
        pltpu.SemaphoreType.DMA((stages, 2)),
    ]
    edge = pl.pallas_call(
        functools.partial(edge_kernel, width=2048, stages=stages),
        out_shape=jax.ShapeDtypeStruct((4, width), jnp.bfloat16),
        in_specs=[in_place] * 2,
        out_specs=vmem(1)[0],
        scratch_shapes=[
            pltpu.VMEM((2, 1, 2, width), state.dtype),
            pltpu.VMEM((2, 1, 2, width), adjoint.dtype),
            field_scratch[2],
        ],
        compiler_params=params(63),
        cost_estimate=cost(4 * slab_rows * width, 2 * 1024 * 1024),
        name="edge",
    )(state, adjoint)
    edge_below = lax.ppermute(edge, "rows", down)
    code = pl.pallas_call(
        functools.partial(code_kernel, width=2048, stages=stages),
        out_shape=jax.ShapeDtypeStruct((slab_rows, width), i16),
        in_specs=[in_place],
        out_specs=in_place,
        scratch_shapes=[
            pltpu.VMEM((slab_rows, width), f32),
            pltpu.VMEM((slab_rows, width), i16),
        ]
        + [pltpu.SemaphoreType.DMA((stages,))] * 2,
        compiler_params=params(63),
        name="code",
    )(design)
    code_above = lax.ppermute(code, "rows", up)
    code_below = lax.ppermute(code, "rows", down)

    top = (lax.axis_index("rows") * slab_rows).astype(jnp.int32).reshape(1)

    slab = jax.ShapeDtypeStruct((slab_rows, width), f32)
    elastic, inertia = pl.pallas_call(
        functools.partial(element_kernel, width=2048, stages=element_stages),
        out_shape=[slab, slab],
        in_specs=[smem, smem] + [in_place] * 3,
        out_specs=[in_place, in_place],
        scratch_shapes=field_scratch[:2]
        + [pltpu.VMEM(edge.shape, edge.dtype)]
        + [pltpu.VMEM((slab_rows, width), f32)] * 2
        + [pltpu.SemaphoreType.DMA((element_stages, count)) for count in (3, 2)],
        compiler_params=params(53),
        cost_estimate=cost(80 * slab_rows * width, 8 * 1024 * 1024),
        name="element",
    )(omega_sq, assign, state, adjoint, edge_below)

    coded = jax.ShapeDtypeStruct((peers, slab_rows, piece + LANES), i16)
    operands = (design, code_above, code_below, passive, elastic, inertia)
    sent = pl.pallas_call(
        functools.partial(partial_kernel, stages=stages, whole_rows=whole_rows),
        out_shape=coded,
        in_specs=[smem] + [in_place] * len(operands),
        out_specs=in_place,
        scratch_shapes=[pltpu.VMEM(operand.shape, operand.dtype) for operand in operands]
        + [
            pltpu.VMEM((slab_rows, width + 2 * LANES), f32),
            pltpu.VMEM((slab_rows, width + 2 * LANES), f32),
            pltpu.VMEM((slab_rows, piece), f32),
            pltpu.VMEM(coded.shape, coded.dtype),
            pltpu.SemaphoreType.DMA((stages, len(operands))),
            pltpu.SemaphoreType.DMA((peers,)),
        ],
        compiler_params=params(63),
        cost_estimate=cost(150 * slab_rows * width, 14 * 1024 * 1024),
        name="partial",
    )(top, *operands)

    received = lax.all_to_all(sent, "freq", 0, 0, tiled=True)

    spread, sent = pl.pallas_call(
        functools.partial(sum_kernel, width=1024),
        out_shape=[
            jax.ShapeDtypeStruct((slab_rows, piece), f32),
            jax.ShapeDtypeStruct((slab_rows, piece + LANES), i16),
        ],
        in_specs=vmem(1),
        out_specs=vmem(2),
        compiler_params=params(8),
        name="total",
    )(received)
    spread_below = lax.ppermute(sent, "rows", down)
    spread_above = lax.ppermute(sent, "rows", up)

    wide_coded = jax.ShapeDtypeStruct((peers, slab_rows, piece + 3 * LANES), i16)
    result = pl.pallas_call(
        functools.partial(back_kernel, width=1024),
        out_shape=wide_coded,
        in_specs=vmem(3),
        out_specs=vmem(1)[0],
        scratch_shapes=[pltpu.VMEM((slab_rows, piece), f32)],
        compiler_params=params(8),
        name="back",
    )(spread_above, spread, spread_below)

    pieces = lax.all_to_all(result, "freq", 0, 0, tiled=True)

    squares = pl.pallas_call(
        squares_kernel,
        out_shape=jax.ShapeDtypeStruct((rows, 8, LANES), f32),
        in_specs=vmem(1),
        out_specs=vmem(1)[0],
        compiler_params=params(8),
        name="squares",
    )(pieces)
    squares = lax.all_to_all(squares, "rows", 0, 0, tiled=True)

    return pl.pallas_call(
        functools.partial(result_kernel, width=2048, elements=float(whole_rows * width)),
        out_shape=slab,
        in_specs=vmem(2),
        out_specs=in_place,
        scratch_shapes=[pltpu.VMEM((slab_rows, width), f32), pltpu.SemaphoreType.DMA((peers,))],
        compiler_params=params(16),
        name="result",
    )(pieces, squares)


def solution(mesh):
    return jax.shard_map(
        layer,
        mesh=mesh,
        in_specs=(
            P("rows", None),
            P("rows", None),
            P(None, "freq", "rows", None),
            P(None, "freq", "rows", None),
            P(),
            P("freq"),
        ),
        out_specs=P("rows", None),
        check_vma=False,
    )
```

```python
import functools

import jax
import jax.numpy as jnp
from jax import lax
from jax.experimental import pallas as pl
from jax.experimental.pallas import tpu as pltpu
from jax.sharding import PartitionSpec as P


RADIUS = 8
LANES = 128
SHARPNESS = 8.0
THRESHOLD = 0.5
EXPONENT = 3.0
SOFT_FLOOR = 0.001
LOSS = 0.2
EPSILON = 1e-06
TANH_HALF = 0.999329299739067
DESIGN_STEPS = 32767.0
CODE_STEPS = 32700.0

f32 = jnp.float32
i16 = jnp.int16


def params(megabytes):
    return pltpu.CompilerParams(vmem_limit_bytes=megabytes * 1024 * 1024)


def vmem(count):
    return [pl.BlockSpec(memory_space=pltpu.VMEM)] * count


def cost(flops, moved):
    return pl.CostEstimate(flops=flops, bytes_accessed=moved, transcendentals=0)


def cols(index, width):
    return pl.ds(pl.multiple_of(index * width, width), width)


def row_ids(width):
    return lax.broadcasted_iota(jnp.int32, (8, width), 0)


def rows_up(block, count, ids):
    return jnp.where(ids < 8 - count, pltpu.roll(block, 8 - count, 0), 0.0)


def rows_down(block, count, ids):
    return jnp.where(ids >= count, pltpu.roll(block, count, 0), 0.0)


def row_filter(above, here, below):
    ids = row_ids(here.shape[1])
    upper = above - here
    lower = below - here
    for _ in range(2):
        for count in (1, 2, 4):
            upper = upper + rows_up(upper, count, ids)
            lower = lower + rows_down(lower, count, ids)
    total = here
    for count in (1, 2, 4):
        total = total + pltpu.roll(total, count, 0)
    return upper + lower + here + 10.0 * total


def moved(block, count):
    width = block.shape[1]
    return pltpu.roll(block, (width - count) % width, 1)


def band():
    shape = (3 * LANES, LANES)
    source = lax.broadcasted_iota(jnp.int32, shape, 0) - LANES
    target = lax.broadcasted_iota(jnp.int32, shape, 1)
    taps = jnp.maximum(RADIUS + 1 - jnp.abs(source - target), 0)
    return taps.astype(f32).astype(jnp.bfloat16)


def col_filter(window, taps):
    count = window.shape[1] // LANES - 2
    half = count // 2
    tiles = [window[:, i * LANES : (i + 1) * LANES] for i in range(count + 2)]
    stacked = jnp.concatenate(
        [tiles[i + side] for i in range(half + 2) for side in (0, half)], axis=0
    )
    coarse = stacked.astype(jnp.bfloat16)
    fine = (stacked - coarse.astype(f32)).astype(jnp.bfloat16)
    left, here, right = (slice(start, start + 16 * half) for start in (0, 16, 32))

    def product(first, second, weights):
        return jnp.dot(
            jnp.concatenate([first, second], axis=1), weights, preferred_element_type=f32
        )

    near, far = taps[: 2 * LANES], taps[2 * LANES :]
    total = product(coarse[left], coarse[here], near) + product(fine[left], fine[here], near)
    total = total + product(coarse[right], fine[right], jnp.concatenate([far, far], axis=0))
    halves = [
        [total[16 * i + 8 * side : 16 * i + 8 * side + 8] for i in range(half)] for side in (0, 1)
    ]
    return jnp.concatenate(halves[0] + halves[1], axis=1)


def padded_cols(index, width):
    return pl.ds(pl.multiple_of(index * width, LANES), width + 2 * LANES)


def inner_cols(index, width):
    return pl.ds(pl.multiple_of(index * width + LANES, LANES), width)


def clear_ends(ref):
    count = ref.shape[1]
    ref[:, :LANES] = jnp.zeros((8, LANES), f32)
    ref[:, count - LANES :] = jnp.zeros((8, LANES), f32)


def decode_scale(code):
    return jnp.exp2(code.astype(jnp.int32).astype(f32) * (1.0 / 256)) * (1.0 / CODE_STEPS)


def scale_code(largest):
    level = jnp.floor(jnp.log(jnp.maximum(largest, 1e-30)) * (256 * 1.4426950408889634)) + 1.0
    return level


def to_i16(values):
    return jnp.round(values).astype(jnp.int32).astype(i16)


def wide(tile, width):
    return jnp.concatenate([tile] * (width // LANES), axis=1)


def folded(block, join):
    parts = [block[:, i : i + LANES] for i in range(0, block.shape[1], LANES)]
    while len(parts) > 1:
        parts = [join(a, b) for a, b in zip(parts[::2], parts[1::2])]
    return parts[0]


def folded_max(block):
    return folded(jnp.abs(block), jnp.maximum)


def encode(source, largest, targets, width):
    count = source.shape[1]
    code = scale_code(largest).astype(jnp.int32).astype(i16)
    for target in targets:
        target[:, count : count + LANES] = code
    inverse = wide(1.0 / decode_scale(code), width)

    def step(c, none):
        values = to_i16(source[:, cols(c, width)] * inverse)
        for target in targets:
            target[:, cols(c, width)] = values
        return none

    lax.fori_loop(0, count // width, step, 0)


def field_copies(sources, kept, arrived, stage, span):
    at = pl.ds(stage * span, span)
    whole = lambda ref: (slice(None),) * (len(ref.shape) - 1) + (at,)
    return [
        pltpu.make_async_copy(source.at[whole(source)], target.at[whole(target)], arrived.at[stage, place])
        for place, (source, target) in enumerate(zip(sources, kept))
    ]


def prepare_kernel(
    state_far,
    adjoint_far,
    design_far,
    edge,
    code_far,
    state,
    adjoint,
    design,
    code,
    arrived,
    design_arrived,
    left,
    *,
    width,
    stages,
):
    ids = row_ids(width)
    span = edge.shape[1] // stages
    steps = span // width
    copies = functools.partial(
        field_copies, (state_far, adjoint_far), (state, adjoint), arrived, span=span
    )

    def load(stage):
        at = pl.ds(stage * span, span)
        return pltpu.make_async_copy(design_far.at[:, at], design.at[:, at], design_arrived.at[stage])

    def save(stage):
        at = pl.ds(stage * span, span)
        return pltpu.make_async_copy(code.at[:, at], code_far.at[:, at], left.at[stage])

    for stage in range(stages):
        load(stage).start()
    for stage in range(stages):
        for copy in copies(stage):
            copy.start()

    for stage in range(stages):
        load(stage).wait()

        def encode_rows(c, none):
            at = cols(stage * steps + c, width)
            code[:, at] = to_i16(design[:, at] * DESIGN_STEPS)
            return none

        lax.fori_loop(0, steps, encode_rows, 0)
        save(stage).start()

    for stage in range(stages):
        for copy in copies(stage):
            copy.wait()

        def pick_rows(c, none):
            at = cols(stage * steps + c, width)
            first = state[0, 0, :, at].astype(f32)
            rows = [state[1, 0, :, at], adjoint[0, 0, :, at], adjoint[1, 0, :, at]]
            for place, row in enumerate(rows):
                first = jnp.where(ids == place + 1, pltpu.roll(row.astype(f32), place + 1, 0), first)
            edge[:, at] = first[:4].astype(jnp.bfloat16)
            return none

        lax.fori_loop(0, steps, pick_rows, 0)
    for stage in range(stages):
        save(stage).wait()


def element_kernel(
    omega_sq,
    assign,
    state_far,
    adjoint_far,
    edge_far,
    elastic_far,
    inertia_far,
    state,
    adjoint,
    edge,
    elastic,
    inertia,
    arrived,
    left,
    *,
    width,
    stages,
):
    omega = omega_sq[assign[0]]
    ids = row_ids(width)
    span = elastic.shape[1] // stages
    count = span // width
    copies = functools.partial(
        field_copies, (state_far, adjoint_far, edge_far), (state, adjoint, edge), arrived, span=span
    )
    for stage in reversed(range(stages)):
        for copy in copies(stage):
            copy.start()

    def shifted(block, carry):
        return moved(jnp.concatenate([block, carry], axis=1), 1)[:, :width]

    def step(stage, c, carries):
        at = cols((stage + 1) * count - 1 - c, width)
        edges = edge[:, at].astype(f32)
        fields = [state[0, 0, :, at], state[1, 0, :, at], adjoint[0, 0, :, at], adjoint[1, 0, :, at]]
        kept = []
        parts = []
        for place, field in enumerate(fields):
            here = field.astype(f32)
            row = jnp.broadcast_to(edges[place : place + 1], here.shape)
            below = jnp.where(ids == 7, row, pltpu.roll(here, 7, 0))
            plus = here + below
            minus = here - below
            kept += [plus[:, :LANES], minus[:, :LANES]]
            plus_next = shifted(plus, carries[2 * place])
            minus_next = shifted(minus, carries[2 * place + 1])
            parts.append((plus + plus_next, plus - plus_next, minus + minus_next, minus - minus_next))
        sr, si, ar, ai = parts
        same = [ar[k] * sr[k] - ai[k] * si[k] for k in range(4)]
        cross = [ar[k] * si[k] + ai[k] * sr[k] for k in range(1, 4)]
        same_mixed = same[1] + same[2]
        cross_mixed = cross[0] + cross[1]
        stiff = 1.5 * (same_mixed - LOSS * cross_mixed) + (same[3] - LOSS * cross[2])
        mass = 2.25 * same[0] + 0.75 * same_mixed + 0.25 * same[3]
        elastic[:, at] = stiff * (EXPONENT * (1.0 - SOFT_FLOOR) / 6.0)
        inertia[:, at] = mass * (omega * (1.0 / 36.0))
        return tuple(kept)

    def results(stage):
        at = pl.ds(stage * span, span)
        return [
            pltpu.make_async_copy(source.at[:, at], target.at[:, at], left.at[stage, place])
            for place, (source, target) in enumerate(((elastic, elastic_far), (inertia, inertia_far)))
        ]

    carries = (jnp.zeros((8, LANES), f32),) * 8
    for stage in reversed(range(stages)):
        for copy in copies(stage):
            copy.wait()
        carries = lax.fori_loop(0, count, functools.partial(step, stage), carries, unroll=2)
        for copy in results(stage):
            copy.start()
    for stage in reversed(range(stages)):
        for copy in results(stage):
            copy.wait()


def tap_sums(before, after):
    near = jnp.maximum(RADIUS - before, 0)
    far = jnp.maximum(RADIUS - after, 0)
    missing = near * (near + 1) + far * (far + 1)
    return float((RADIUS + 1) ** 2) - 0.5 * missing.astype(f32)


def partial_kernel(top, *refs, stages, whole_rows):
    sources, out_far, kept = refs[:6], refs[6], refs[7:13]
    rowed, spread, blocks, out, arrived, left = refs[13:]
    design, above, below, passive, elastic, inertia = kept
    peers = out.shape[0]
    piece = design.shape[1] // peers
    narrow = 2048
    span = design.shape[1] // stages

    def early(stage):
        at = pl.ds(stage * span, span)
        return [
            pltpu.make_async_copy(sources[k].at[:, at], kept[k].at[:, at], arrived.at[stage, k])
            for k in range(3)
        ]

    def late(stage):
        at = cols(stage, span)
        return [
            pltpu.make_async_copy(sources[k].at[:, at], kept[k].at[:, at], arrived.at[stage, k])
            for k in range(3, 6)
        ]

    for stage in range(stages):
        for copy in early(stage):
            copy.start()
    for stage in range(stages):
        for copy in late(stage):
            copy.start()
    clear_ends(rowed)
    clear_ends(spread)

    def filter_rows(c, none):
        at = cols(c, narrow)
        upper = above[:, at].astype(jnp.int32).astype(f32) * (1.0 / DESIGN_STEPS)
        lower = below[:, at].astype(jnp.int32).astype(f32) * (1.0 / DESIGN_STEPS)
        rowed[:, inner_cols(c, narrow)] = row_filter(upper, design[:, at], lower)
        return none

    for stage in range(stages):
        for copy in early(stage):
            copy.wait()
        first = stage * (span // narrow)
        lax.fori_loop(first, first + span // narrow, filter_rows, 0)

    taps = band()
    row = top[0] + row_ids(LANES)
    lane = lax.broadcasted_iota(jnp.int32, (8, LANES), 1)
    full = float((RADIUS + 1) ** 2)
    inside = 1.0 / (full * tap_sums(row, whole_rows - 1 - row))
    left_end = full / tap_sums(lane, RADIUS)
    right_end = full / tap_sums(RADIUS, LANES - 1 - lane)

    def scale(c, none):
        at = cols(c, piece)
        for copy in late(c):
            copy.wait()
        first = inside * jnp.where(c == 0, left_end, 1.0)
        last = inside * jnp.where(c == peers - 1, right_end, 1.0)
        weights = jnp.concatenate([first] + [inside] * (piece // LANES - 2) + [last], axis=1)
        tilde = col_filter(rowed[:, padded_cols(c, piece)], taps) * weights
        steep = jnp.tanh(SHARPNESS * (tilde - THRESHOLD))
        solid = passive[:, at] > 0
        density = jnp.where(solid, 1.0, (TANH_HALF + steep) * (0.5 / TANH_HALF))
        slope = jnp.where(solid, 0.0, (1.0 - steep * steep) * (SHARPNESS * 0.5 / TANH_HALF))
        block = (density * density * elastic[:, at] - inertia[:, at]) * (slope * weights)
        spread[:, inner_cols(c, piece)] = block
        return none

    lax.fori_loop(0, peers, scale, 0)

    def send(peer, none):
        block = col_filter(spread[:, padded_cols(peer, piece)], taps)
        blocks[...] = block
        encode(blocks, folded_max(block), [out.at[peer]], narrow)
        pltpu.make_async_copy(out.at[peer], out_far.at[peer], left.at[peer]).start()
        return none

    lax.fori_loop(0, peers, send, 0)
    for peer in range(peers):
        pltpu.make_async_copy(out.at[peer], out_far.at[peer], left.at[peer]).wait()


def sum_kernel(coded, out, sent, *, width):
    peers, piece = coded.shape[0], out.shape[1]
    scales = [wide(decode_scale(coded[peer, :, piece:]), width) for peer in range(peers)]

    def step(c, largest):
        at = cols(c, width)
        total = None
        for peer in range(peers):
            term = coded[peer, :, at].astype(jnp.int32).astype(f32) * scales[peer]
            total = term if total is None else total + term
        out[:, at] = total
        return jnp.maximum(largest, folded_max(total))

    largest = lax.fori_loop(0, piece // width, step, jnp.zeros((8, LANES), f32))
    encode(out, largest, [sent], width)


def back_kernel(above, here, below, out, blocks, *, width):
    piece = here.shape[1]
    zeros = jnp.zeros((8, LANES), f32)
    above_scale, below_scale = (
        wide(decode_scale(ref[:, piece:]), width) for ref in (above, below)
    )

    def step(c, carry):
        largest, squares = carry
        at = cols(c, width)
        upper = above[:, at].astype(jnp.int32).astype(f32) * above_scale
        lower = below[:, at].astype(jnp.int32).astype(f32) * below_scale
        block = row_filter(upper, here[:, at], lower)
        blocks[:, at] = block
        return jnp.maximum(largest, folded_max(block)), squares + folded(block * block, jnp.add)

    largest, squares = lax.fori_loop(0, piece // width, step, (zeros, zeros))
    encode(blocks, largest, [out.at[peer] for peer in range(out.shape[0])], width)
    code = scale_code(squares).astype(jnp.int32).astype(i16)
    values = to_i16(squares / decode_scale(code))
    for peer in range(out.shape[0]):
        out[peer, :, piece + LANES : piece + 2 * LANES] = code
        out[peer, :, piece + 2 * LANES :] = values


def squares_kernel(coded, squares):
    piece = coded.shape[2] - 3 * LANES
    total = jnp.zeros((8, LANES), f32)
    for peer in range(coded.shape[0]):
        values = coded[peer, :, piece + 2 * LANES :].astype(jnp.int32).astype(f32)
        total = total + values * decode_scale(coded[peer, :, piece + LANES : piece + 2 * LANES])
    squares[...] = jnp.broadcast_to(total[None], squares.shape)


def result_kernel(coded, squares, out_far, out, left, *, width, elements):
    peers = coded.shape[0]
    piece = out.shape[1] // peers
    mean = jnp.sum(jnp.sum(squares[...], axis=0), keepdims=True) * (1.0 / elements) + EPSILON
    root = lax.rsqrt(mean)
    root = root * (1.5 - 0.5 * mean * root * root)

    def finished(peer):
        at = pl.ds(peer * piece, piece)
        return pltpu.make_async_copy(out.at[:, at], out_far.at[:, at], left.at[peer])

    for peer in range(peers):
        scale = wide(decode_scale(coded[peer, :, piece : piece + LANES]) * root, width)

        def step(c, none):
            block = coded[peer, :, cols(c, width)].astype(jnp.int32).astype(f32) * scale
            out[:, cols(peer * (piece // width) + c, width)] = block
            return none

        lax.fori_loop(0, piece // width, step, 0)
        finished(peer).start()
    for peer in range(peers):
        finished(peer).wait()


def layer(design, passive, state, adjoint, omega_sq, assign):
    slab_rows, width = design.shape
    rows = lax.axis_size("rows")
    peers = lax.axis_size("freq")
    whole_rows = slab_rows * rows
    piece = width // peers
    up = [(i, i + 1) for i in range(rows - 1)]
    down = [(target, source) for source, target in up]
    smem = pl.BlockSpec(memory_space=pltpu.SMEM)

    in_place = pl.BlockSpec(memory_space=pltpu.HBM)
    stages = 4
    element_stages = 8
    field_scratch = [
        pltpu.VMEM(state.shape, state.dtype),
        pltpu.VMEM(adjoint.shape, adjoint.dtype),
        pltpu.SemaphoreType.DMA((stages, 2)),
    ]
    design_scratch = [
        pltpu.VMEM((slab_rows, width), f32),
        pltpu.VMEM((slab_rows, width), i16),
    ]
    edge, code = pl.pallas_call(
        functools.partial(prepare_kernel, width=2048, stages=stages),
        out_shape=[
            jax.ShapeDtypeStruct((4, width), jnp.bfloat16),
            jax.ShapeDtypeStruct((slab_rows, width), i16),
        ],
        in_specs=[in_place] * 3,
        out_specs=vmem(1) + [in_place],
        scratch_shapes=field_scratch[:2]
        + design_scratch
        + [field_scratch[2]]
        + [pltpu.SemaphoreType.DMA((stages,))] * 2,
        compiler_params=params(63),
        cost_estimate=cost(8 * slab_rows * width, 7 * 1024 * 1024),
        name="prepare",
    )(state, adjoint, design)
    edge_below = lax.ppermute(edge, "rows", down)
    code_below = lax.ppermute(code, "rows", down)
    code_above = lax.ppermute(code, "rows", up)

    top = (lax.axis_index("rows") * slab_rows).astype(jnp.int32).reshape(1)

    slab = jax.ShapeDtypeStruct((slab_rows, width), f32)
    elastic, inertia = pl.pallas_call(
        functools.partial(element_kernel, width=2048, stages=element_stages),
        out_shape=[slab, slab],
        in_specs=[smem, smem] + [in_place] * 3,
        out_specs=[in_place, in_place],
        scratch_shapes=field_scratch[:2]
        + [pltpu.VMEM(edge.shape, edge.dtype)]
        + [pltpu.VMEM((slab_rows, width), f32)] * 2
        + [pltpu.SemaphoreType.DMA((element_stages, count)) for count in (3, 2)],
        compiler_params=params(53),
        cost_estimate=cost(80 * slab_rows * width, 8 * 1024 * 1024),
        name="element",
    )(omega_sq, assign, state, adjoint, edge_below)

    coded = jax.ShapeDtypeStruct((peers, slab_rows, piece + LANES), i16)
    operands = (design, code_above, code_below, passive, elastic, inertia)
    sent = pl.pallas_call(
        functools.partial(partial_kernel, stages=peers, whole_rows=whole_rows),
        out_shape=coded,
        in_specs=[smem] + [in_place] * len(operands),
        out_specs=in_place,
        scratch_shapes=[pltpu.VMEM(operand.shape, operand.dtype) for operand in operands]
        + [
            pltpu.VMEM((slab_rows, width + 2 * LANES), f32),
            pltpu.VMEM((slab_rows, width + 2 * LANES), f32),
            pltpu.VMEM((slab_rows, piece), f32),
            pltpu.VMEM(coded.shape, coded.dtype),
            pltpu.SemaphoreType.DMA((peers, len(operands))),
            pltpu.SemaphoreType.DMA((peers,)),
        ],
        compiler_params=params(63),
        cost_estimate=cost(150 * slab_rows * width, 14 * 1024 * 1024),
        name="partial",
    )(top, *operands)

    received = lax.all_to_all(sent, "freq", 0, 0, tiled=True)

    spread, sent = pl.pallas_call(
        functools.partial(sum_kernel, width=1024),
        out_shape=[
            jax.ShapeDtypeStruct((slab_rows, piece), f32),
            jax.ShapeDtypeStruct((slab_rows, piece + LANES), i16),
        ],
        in_specs=vmem(1),
        out_specs=vmem(2),
        compiler_params=params(8),
        name="total",
    )(received)
    spread_below = lax.ppermute(sent, "rows", down)
    spread_above = lax.ppermute(sent, "rows", up)

    wide_coded = jax.ShapeDtypeStruct((peers, slab_rows, piece + 3 * LANES), i16)
    result = pl.pallas_call(
        functools.partial(back_kernel, width=1024),
        out_shape=wide_coded,
        in_specs=vmem(3),
        out_specs=vmem(1)[0],
        scratch_shapes=[pltpu.VMEM((slab_rows, piece), f32)],
        compiler_params=params(8),
        name="back",
    )(spread_above, spread, spread_below)

    pieces = lax.all_to_all(result, "freq", 0, 0, tiled=True)

    squares = pl.pallas_call(
        squares_kernel,
        out_shape=jax.ShapeDtypeStruct((rows, 8, LANES), f32),
        in_specs=vmem(1),
        out_specs=vmem(1)[0],
        compiler_params=params(8),
        name="squares",
    )(pieces)
    squares = lax.all_to_all(squares, "rows", 0, 0, tiled=True)

    return pl.pallas_call(
        functools.partial(result_kernel, width=2048, elements=float(whole_rows * width)),
        out_shape=slab,
        in_specs=vmem(2),
        out_specs=in_place,
        scratch_shapes=[pltpu.VMEM((slab_rows, width), f32), pltpu.SemaphoreType.DMA((peers,))],
        compiler_params=params(16),
        name="result",
    )(pieces, squares)


def solution(mesh):
    return jax.shard_map(
        layer,
        mesh=mesh,
        in_specs=(
            P("rows", None),
            P("rows", None),
            P(None, "freq", "rows", None),
            P(None, "freq", "rows", None),
            P(),
            P("freq"),
        ),
        out_specs=P("rows", None),
        check_vma=False,
    )
```

```python
import functools

import jax
import jax.numpy as jnp
from jax import lax
from jax.experimental import pallas as pl
from jax.experimental.pallas import tpu as pltpu
from jax.sharding import PartitionSpec as P


RADIUS = 8
LANES = 128
SHARPNESS = 8.0
THRESHOLD = 0.5
EXPONENT = 3.0
SOFT_FLOOR = 0.001
LOSS = 0.2
EPSILON = 1e-06
TANH_HALF = 0.999329299739067
DESIGN_STEPS = 32767.0
CODE_STEPS = 32700.0

f32 = jnp.float32
i16 = jnp.int16


def params(megabytes):
    return pltpu.CompilerParams(vmem_limit_bytes=megabytes * 1024 * 1024)


def vmem(count):
    return [pl.BlockSpec(memory_space=pltpu.VMEM)] * count


def cost(flops, moved):
    return pl.CostEstimate(flops=flops, bytes_accessed=moved, transcendentals=0)


def cols(index, width):
    return pl.ds(pl.multiple_of(index * width, width), width)


def row_ids(width):
    return lax.broadcasted_iota(jnp.int32, (8, width), 0)


def rows_up(block, count, ids):
    return jnp.where(ids < 8 - count, pltpu.roll(block, 8 - count, 0), 0.0)


def rows_down(block, count, ids):
    return jnp.where(ids >= count, pltpu.roll(block, count, 0), 0.0)


def row_filter(above, here, below):
    ids = row_ids(here.shape[1])
    upper = above - here
    lower = below - here
    for _ in range(2):
        for count in (1, 2, 4):
            upper = upper + rows_up(upper, count, ids)
            lower = lower + rows_down(lower, count, ids)
    total = here
    for count in (1, 2, 4):
        total = total + pltpu.roll(total, count, 0)
    return upper + lower + here + 10.0 * total


def moved(block, count):
    width = block.shape[1]
    return pltpu.roll(block, (width - count) % width, 1)


def band():
    shape = (3 * LANES, LANES)
    source = lax.broadcasted_iota(jnp.int32, shape, 0) - LANES
    target = lax.broadcasted_iota(jnp.int32, shape, 1)
    taps = jnp.maximum(RADIUS + 1 - jnp.abs(source - target), 0)
    return taps.astype(f32).astype(jnp.bfloat16)


def col_filter(window, taps):
    count = window.shape[1] // LANES - 2
    half = count // 2
    tiles = [window[:, i * LANES : (i + 1) * LANES] for i in range(count + 2)]
    stacked = jnp.concatenate(
        [tiles[i + side] for i in range(half + 2) for side in (0, half)], axis=0
    )
    coarse = stacked.astype(jnp.bfloat16)
    fine = (stacked - coarse.astype(f32)).astype(jnp.bfloat16)
    left, here, right = (slice(start, start + 16 * half) for start in (0, 16, 32))

    def product(first, second, weights):
        return jnp.dot(
            jnp.concatenate([first, second], axis=1), weights, preferred_element_type=f32
        )

    near, far = taps[: 2 * LANES], taps[2 * LANES :]
    total = product(coarse[left], coarse[here], near) + product(fine[left], fine[here], near)
    total = total + product(coarse[right], fine[right], jnp.concatenate([far, far], axis=0))
    halves = [
        [total[16 * i + 8 * side : 16 * i + 8 * side + 8] for i in range(half)] for side in (0, 1)
    ]
    return jnp.concatenate(halves[0] + halves[1], axis=1)


def padded_cols(index, width):
    return pl.ds(pl.multiple_of(index * width, LANES), width + 2 * LANES)


def inner_cols(index, width):
    return pl.ds(pl.multiple_of(index * width + LANES, LANES), width)


def clear_ends(ref):
    count = ref.shape[1]
    ref[:, :LANES] = jnp.zeros((8, LANES), f32)
    ref[:, count - LANES :] = jnp.zeros((8, LANES), f32)


def decode_scale(code):
    return jnp.exp2(code.astype(jnp.int32).astype(f32) * (1.0 / 256)) * (1.0 / CODE_STEPS)


def scale_code(largest):
    level = jnp.floor(jnp.log(jnp.maximum(largest, 1e-30)) * (256 * 1.4426950408889634)) + 1.0
    return level


def to_i16(values):
    return jnp.round(values).astype(jnp.int32).astype(i16)


def wide(tile, width):
    return jnp.concatenate([tile] * (width // LANES), axis=1)


def folded(block, join):
    parts = [block[:, i : i + LANES] for i in range(0, block.shape[1], LANES)]
    while len(parts) > 1:
        parts = [join(a, b) for a, b in zip(parts[::2], parts[1::2])]
    return parts[0]


def folded_max(block):
    return folded(jnp.abs(block), jnp.maximum)


def encode(source, largest, targets, width):
    count = source.shape[1]
    code = scale_code(largest).astype(jnp.int32).astype(i16)
    for target in targets:
        target[:, count : count + LANES] = code
    inverse = wide(1.0 / decode_scale(code), width)

    def step(c, none):
        values = to_i16(source[:, cols(c, width)] * inverse)
        for target in targets:
            target[:, cols(c, width)] = values
        return none

    lax.fori_loop(0, count // width, step, 0)


def field_copies(sources, kept, arrived, stage, span):
    at = pl.ds(stage * span, span)
    whole = lambda ref: (slice(None),) * (len(ref.shape) - 1) + (at,)
    return [
        pltpu.make_async_copy(source.at[whole(source)], target.at[whole(target)], arrived.at[stage, place])
        for place, (source, target) in enumerate(zip(sources, kept))
    ]


def prepare_kernel(
    state_far,
    adjoint_far,
    design_far,
    edge,
    code_far,
    state,
    adjoint,
    design,
    code,
    arrived,
    design_arrived,
    left,
    *,
    width,
    stages,
):
    span = edge.shape[1] // stages
    steps = span // width
    sent = lax.broadcasted_iota(jnp.int32, (4, width), 0)

    def copies(stage):
        at = pl.ds(stage * span, span)
        return [
            pltpu.make_async_copy(source.at[:, :, 0:2, at], target.at[:, :, :, at], arrived.at[stage, place])
            for place, (source, target) in enumerate(((state_far, state), (adjoint_far, adjoint)))
        ]

    def load(stage):
        at = pl.ds(stage * span, span)
        return pltpu.make_async_copy(design_far.at[:, at], design.at[:, at], design_arrived.at[stage])

    def save(stage):
        at = pl.ds(stage * span, span)
        return pltpu.make_async_copy(code.at[:, at], code_far.at[:, at], left.at[stage])

    for stage in range(stages):
        for copy in copies(stage):
            copy.start()
    for stage in range(stages):
        load(stage).start()

    for stage in range(stages):
        for copy in copies(stage):
            copy.wait()

        def pick_rows(c, none):
            at = cols(stage * steps + c, width)
            fields = [state[0, 0, :, at], state[1, 0, :, at], adjoint[0, 0, :, at], adjoint[1, 0, :, at]]
            picked = jnp.zeros((4, width), f32)
            for place, field in enumerate(fields):
                row = jnp.broadcast_to(field.astype(f32)[:1], picked.shape)
                picked = jnp.where(sent == place, row, picked)
            edge[:, at] = picked.astype(jnp.bfloat16)
            return none

        lax.fori_loop(0, steps, pick_rows, 0)

    for stage in range(stages):
        load(stage).wait()

        def encode_rows(c, none):
            at = cols(stage * steps + c, width)
            code[:, at] = to_i16(design[:, at] * DESIGN_STEPS)
            return none

        lax.fori_loop(0, steps, encode_rows, 0)
        save(stage).start()
    for stage in range(stages):
        save(stage).wait()


def element_kernel(
    omega_sq,
    assign,
    state_far,
    adjoint_far,
    edge_far,
    elastic_far,
    inertia_far,
    state,
    adjoint,
    edge,
    elastic,
    inertia,
    arrived,
    left,
    *,
    width,
    stages,
):
    omega = omega_sq[assign[0]]
    ids = row_ids(width)
    span = elastic.shape[1] // stages
    count = span // width
    copies = functools.partial(
        field_copies, (state_far, adjoint_far, edge_far), (state, adjoint, edge), arrived, span=span
    )
    for stage in reversed(range(stages)):
        for copy in copies(stage):
            copy.start()

    def shifted(block, carry):
        return moved(jnp.concatenate([block, carry], axis=1), 1)[:, :width]

    def step(stage, c, carries):
        at = cols((stage + 1) * count - 1 - c, width)
        edges = edge[:, at].astype(f32)
        fields = [state[0, 0, :, at], state[1, 0, :, at], adjoint[0, 0, :, at], adjoint[1, 0, :, at]]
        kept = []
        parts = []
        for place, field in enumerate(fields):
            here = field.astype(f32)
            row = jnp.broadcast_to(edges[place : place + 1], here.shape)
            below = jnp.where(ids == 7, row, pltpu.roll(here, 7, 0))
            plus = here + below
            minus = here - below
            kept += [plus[:, :LANES], minus[:, :LANES]]
            plus_next = shifted(plus, carries[2 * place])
            minus_next = shifted(minus, carries[2 * place + 1])
            parts.append((plus + plus_next, plus - plus_next, minus + minus_next, minus - minus_next))
        sr, si, ar, ai = parts
        same = [ar[k] * sr[k] - ai[k] * si[k] for k in range(4)]
        cross = [ar[k] * si[k] + ai[k] * sr[k] for k in range(1, 4)]
        same_mixed = same[1] + same[2]
        cross_mixed = cross[0] + cross[1]
        stiff = 1.5 * (same_mixed - LOSS * cross_mixed) + (same[3] - LOSS * cross[2])
        mass = 2.25 * same[0] + 0.75 * same_mixed + 0.25 * same[3]
        elastic[:, at] = stiff * (EXPONENT * (1.0 - SOFT_FLOOR) / 6.0)
        inertia[:, at] = mass * (omega * (1.0 / 36.0))
        return tuple(kept)

    def results(stage):
        at = pl.ds(stage * span, span)
        return [
            pltpu.make_async_copy(source.at[:, at], target.at[:, at], left.at[stage, place])
            for place, (source, target) in enumerate(((elastic, elastic_far), (inertia, inertia_far)))
        ]

    carries = (jnp.zeros((8, LANES), f32),) * 8
    for stage in reversed(range(stages)):
        for copy in copies(stage):
            copy.wait()
        carries = lax.fori_loop(0, count, functools.partial(step, stage), carries, unroll=2)
        for copy in results(stage):
            copy.start()
    for stage in reversed(range(stages)):
        for copy in results(stage):
            copy.wait()


def tap_sums(before, after):
    near = jnp.maximum(RADIUS - before, 0)
    far = jnp.maximum(RADIUS - after, 0)
    missing = near * (near + 1) + far * (far + 1)
    return float((RADIUS + 1) ** 2) - 0.5 * missing.astype(f32)


def partial_kernel(top, *refs, stages, whole_rows):
    sources, out_far, kept = refs[:6], refs[6], refs[7:13]
    rowed, spread, blocks, out, arrived, left = refs[13:]
    design, above, below, passive, elastic, inertia = kept
    peers = out.shape[0]
    piece = design.shape[1] // peers
    narrow = 2048
    rows_width = 4096
    span = design.shape[1] // stages

    def early(stage):
        at = pl.ds(stage * span, span)
        return [
            pltpu.make_async_copy(sources[k].at[:, at], kept[k].at[:, at], arrived.at[stage, k])
            for k in range(3)
        ]

    def late(stage):
        at = cols(stage, span)
        return [
            pltpu.make_async_copy(sources[k].at[:, at], kept[k].at[:, at], arrived.at[stage, k])
            for k in range(3, 6)
        ]

    for stage in range(stages):
        for copy in early(stage):
            copy.start()
    for stage in range(stages):
        for copy in late(stage):
            copy.start()
    clear_ends(rowed)
    clear_ends(spread)

    def filter_rows(c, none):
        at = cols(c, rows_width)
        upper = above[:, at].astype(jnp.int32).astype(f32) * (1.0 / DESIGN_STEPS)
        lower = below[:, at].astype(jnp.int32).astype(f32) * (1.0 / DESIGN_STEPS)
        rowed[:, inner_cols(c, rows_width)] = row_filter(upper, design[:, at], lower)
        return none

    for stage in range(stages):
        for copy in early(stage):
            copy.wait()
        first = stage * (span // rows_width)
        lax.fori_loop(first, first + span // rows_width, filter_rows, 0)

    taps = band()
    row = top[0] + row_ids(LANES)
    lane = lax.broadcasted_iota(jnp.int32, (8, LANES), 1)
    full = float((RADIUS + 1) ** 2)
    inside = 1.0 / (full * tap_sums(row, whole_rows - 1 - row))
    left_end = full / tap_sums(lane, RADIUS)
    right_end = full / tap_sums(RADIUS, LANES - 1 - lane)

    def scale(c, none):
        at = cols(c, piece)
        for copy in late(c):
            copy.wait()
        first = inside * jnp.where(c == 0, left_end, 1.0)
        last = inside * jnp.where(c == peers - 1, right_end, 1.0)
        weights = jnp.concatenate([first] + [inside] * (piece // LANES - 2) + [last], axis=1)
        tilde = col_filter(rowed[:, padded_cols(c, piece)], taps) * weights
        steep = jnp.tanh(SHARPNESS * (tilde - THRESHOLD))
        solid = passive[:, at] > 0
        density = jnp.where(solid, 1.0, (TANH_HALF + steep) * (0.5 / TANH_HALF))
        slope = jnp.where(solid, 0.0, (1.0 - steep * steep) * (SHARPNESS * 0.5 / TANH_HALF))
        block = (density * density * elastic[:, at] - inertia[:, at]) * (slope * weights)
        spread[:, inner_cols(c, piece)] = block
        return none

    lax.fori_loop(0, peers, scale, 0)

    def send(peer, none):
        block = col_filter(spread[:, padded_cols(peer, piece)], taps)
        blocks[...] = block
        encode(blocks, folded_max(block), [out.at[peer]], narrow)
        pltpu.make_async_copy(out.at[peer], out_far.at[peer], left.at[peer]).start()
        return none

    lax.fori_loop(0, peers, send, 0)
    for peer in range(peers):
        pltpu.make_async_copy(out.at[peer], out_far.at[peer], left.at[peer]).wait()


def sum_kernel(coded, out, sent, *, width):
    peers, piece = coded.shape[0], out.shape[1]
    scales = [wide(decode_scale(coded[peer, :, piece:]), width) for peer in range(peers)]

    def step(c, largest):
        at = cols(c, width)
        total = None
        for peer in range(peers):
            term = coded[peer, :, at].astype(jnp.int32).astype(f32) * scales[peer]
            total = term if total is None else total + term
        out[:, at] = total
        return jnp.maximum(largest, folded_max(total))

    largest = lax.fori_loop(0, piece // width, step, jnp.zeros((8, LANES), f32))
    encode(out, largest, [sent], width)


def back_kernel(above, here, below, out, blocks, *, width):
    piece = here.shape[1]
    zeros = jnp.zeros((8, LANES), f32)
    above_scale, below_scale = (
        wide(decode_scale(ref[:, piece:]), width) for ref in (above, below)
    )

    def step(c, carry):
        largest, squares = carry
        at = cols(c, width)
        upper = above[:, at].astype(jnp.int32).astype(f32) * above_scale
        lower = below[:, at].astype(jnp.int32).astype(f32) * below_scale
        block = row_filter(upper, here[:, at], lower)
        blocks[:, at] = block
        return jnp.maximum(largest, folded_max(block)), squares + folded(block * block, jnp.add)

    largest, squares = lax.fori_loop(0, piece // width, step, (zeros, zeros))
    encode(blocks, largest, [out.at[peer] for peer in range(out.shape[0])], width)
    code = scale_code(squares).astype(jnp.int32).astype(i16)
    values = to_i16(squares / decode_scale(code))
    for peer in range(out.shape[0]):
        out[peer, :, piece + LANES : piece + 2 * LANES] = code
        out[peer, :, piece + 2 * LANES :] = values


def squares_kernel(coded, squares):
    piece = coded.shape[2] - 3 * LANES
    total = jnp.zeros((8, LANES), f32)
    for peer in range(coded.shape[0]):
        values = coded[peer, :, piece + 2 * LANES :].astype(jnp.int32).astype(f32)
        total = total + values * decode_scale(coded[peer, :, piece + LANES : piece + 2 * LANES])
    squares[...] = jnp.broadcast_to(total[None], squares.shape)


def result_kernel(coded, squares, out_far, out, left, *, width, elements):
    peers = coded.shape[0]
    piece = out.shape[1] // peers
    mean = jnp.sum(jnp.sum(squares[...], axis=0), keepdims=True) * (1.0 / elements) + EPSILON
    root = lax.rsqrt(mean)
    root = root * (1.5 - 0.5 * mean * root * root)

    def finished(peer):
        at = pl.ds(peer * piece, piece)
        return pltpu.make_async_copy(out.at[:, at], out_far.at[:, at], left.at[peer])

    for peer in range(peers):
        scale = wide(decode_scale(coded[peer, :, piece : piece + LANES]) * root, width)

        def step(c, none):
            block = coded[peer, :, cols(c, width)].astype(jnp.int32).astype(f32) * scale
            out[:, cols(peer * (piece // width) + c, width)] = block
            return none

        lax.fori_loop(0, piece // width, step, 0)
        finished(peer).start()
    for peer in range(peers):
        finished(peer).wait()


def layer(design, passive, state, adjoint, omega_sq, assign):
    slab_rows, width = design.shape
    rows = lax.axis_size("rows")
    peers = lax.axis_size("freq")
    whole_rows = slab_rows * rows
    piece = width // peers
    up = [(i, i + 1) for i in range(rows - 1)]
    down = [(target, source) for source, target in up]
    smem = pl.BlockSpec(memory_space=pltpu.SMEM)

    in_place = pl.BlockSpec(memory_space=pltpu.HBM)
    stages = 4
    element_stages = 8
    field_scratch = [
        pltpu.VMEM(state.shape, state.dtype),
        pltpu.VMEM(adjoint.shape, adjoint.dtype),
        pltpu.SemaphoreType.DMA((stages, 2)),
    ]
    design_scratch = [
        pltpu.VMEM((slab_rows, width), f32),
        pltpu.VMEM((slab_rows, width), i16),
    ]
    edge, code = pl.pallas_call(
        functools.partial(prepare_kernel, width=2048, stages=stages),
        out_shape=[
            jax.ShapeDtypeStruct((4, width), jnp.bfloat16),
            jax.ShapeDtypeStruct((slab_rows, width), i16),
        ],
        in_specs=[in_place] * 3,
        out_specs=vmem(1) + [in_place],
        scratch_shapes=[
            pltpu.VMEM((2, 1, 2, width), state.dtype),
            pltpu.VMEM((2, 1, 2, width), adjoint.dtype),
        ]
        + design_scratch
        + [field_scratch[2]]
        + [pltpu.SemaphoreType.DMA((stages,))] * 2,
        compiler_params=params(63),
        cost_estimate=cost(8 * slab_rows * width, 7 * 1024 * 1024),
        name="prepare",
    )(state, adjoint, design)
    edge_below = lax.ppermute(edge, "rows", down)
    code_below = lax.ppermute(code, "rows", down)
    code_above = lax.ppermute(code, "rows", up)

    top = (lax.axis_index("rows") * slab_rows).astype(jnp.int32).reshape(1)

    slab = jax.ShapeDtypeStruct((slab_rows, width), f32)
    elastic, inertia = pl.pallas_call(
        functools.partial(element_kernel, width=2048, stages=element_stages),
        out_shape=[slab, slab],
        in_specs=[smem, smem] + [in_place] * 3,
        out_specs=[in_place, in_place],
        scratch_shapes=field_scratch[:2]
        + [pltpu.VMEM(edge.shape, edge.dtype)]
        + [pltpu.VMEM((slab_rows, width), f32)] * 2
        + [pltpu.SemaphoreType.DMA((element_stages, count)) for count in (3, 2)],
        compiler_params=params(53),
        cost_estimate=cost(80 * slab_rows * width, 8 * 1024 * 1024),
        name="element",
    )(omega_sq, assign, state, adjoint, edge_below)

    coded = jax.ShapeDtypeStruct((peers, slab_rows, piece + LANES), i16)
    operands = (design, code_above, code_below, passive, elastic, inertia)
    sent = pl.pallas_call(
        functools.partial(partial_kernel, stages=peers, whole_rows=whole_rows),
        out_shape=coded,
        in_specs=[smem] + [in_place] * len(operands),
        out_specs=in_place,
        scratch_shapes=[pltpu.VMEM(operand.shape, operand.dtype) for operand in operands]
        + [
            pltpu.VMEM((slab_rows, width + 2 * LANES), f32),
            pltpu.VMEM((slab_rows, width + 2 * LANES), f32),
            pltpu.VMEM((slab_rows, piece), f32),
            pltpu.VMEM(coded.shape, coded.dtype),
            pltpu.SemaphoreType.DMA((peers, len(operands))),
            pltpu.SemaphoreType.DMA((peers,)),
        ],
        compiler_params=params(63),
        cost_estimate=cost(150 * slab_rows * width, 14 * 1024 * 1024),
        name="partial",
    )(top, *operands)

    received = lax.all_to_all(sent, "freq", 0, 0, tiled=True)

    spread, sent = pl.pallas_call(
        functools.partial(sum_kernel, width=1024),
        out_shape=[
            jax.ShapeDtypeStruct((slab_rows, piece), f32),
            jax.ShapeDtypeStruct((slab_rows, piece + LANES), i16),
        ],
        in_specs=vmem(1),
        out_specs=vmem(2),
        compiler_params=params(8),
        name="total",
    )(received)
    spread_below = lax.ppermute(sent, "rows", down)
    spread_above = lax.ppermute(sent, "rows", up)

    wide_coded = jax.ShapeDtypeStruct((peers, slab_rows, piece + 3 * LANES), i16)
    result = pl.pallas_call(
        functools.partial(back_kernel, width=1024),
        out_shape=wide_coded,
        in_specs=vmem(3),
        out_specs=vmem(1)[0],
        scratch_shapes=[pltpu.VMEM((slab_rows, piece), f32)],
        compiler_params=params(8),
        name="back",
    )(spread_above, spread, spread_below)

    pieces = lax.all_to_all(result, "freq", 0, 0, tiled=True)

    squares = pl.pallas_call(
        squares_kernel,
        out_shape=jax.ShapeDtypeStruct((rows, 8, LANES), f32),
        in_specs=vmem(1),
        out_specs=vmem(1)[0],
        compiler_params=params(8),
        name="squares",
    )(pieces)
    squares = lax.all_to_all(squares, "rows", 0, 0, tiled=True)

    return pl.pallas_call(
        functools.partial(result_kernel, width=2048, elements=float(whole_rows * width)),
        out_shape=slab,
        in_specs=vmem(2),
        out_specs=in_place,
        scratch_shapes=[pltpu.VMEM((slab_rows, width), f32), pltpu.SemaphoreType.DMA((peers,))],
        compiler_params=params(16),
        name="result",
    )(pieces, squares)


def solution(mesh):
    return jax.shard_map(
        layer,
        mesh=mesh,
        in_specs=(
            P("rows", None),
            P("rows", None),
            P(None, "freq", "rows", None),
            P(None, "freq", "rows", None),
            P(),
            P("freq"),
        ),
        out_specs=P("rows", None),
        check_vma=False,
    )
```
